128 devices in a mesh: dp: 128 (over z, y, x, core).
Axes of the slice: x: 4, y: 4, z: 4, core: 2. Of those that a mesh axis runs over, the one named last changes fastest.
Arguments:
- x_rows: bfloat16 [131072, 512], P('dp')
- dy_rows: bfloat16 [131072, 512], P('dp')
- w_one: bfloat16 [512, 8192], replicated
- w_two: bfloat16 [8192, 512], replicated
- w_three: bfloat16 [512, 2048], replicated
- w_four: bfloat16 [2048, 512], replicated
- master_one: float32 [512, 8192], P('dp')
- master_two: float32 [8192, 512], P('dp')
- master_three: float32 [512, 2048], P('dp')
- master_four: float32 [2048, 512], P('dp')
- m_one: float32 [512, 8192], P('dp')
- m_two: float32 [8192, 512], P('dp')
- m_three: float32 [512, 2048], P('dp')
- m_four: float32 [2048, 512], P('dp')
- v_one: float32 [512, 8192], P('dp')
- v_two: float32 [8192, 512], P('dp')
- v_three: float32 [512, 2048], P('dp')
- v_four: float32 [2048, 512], P('dp')
- learn_rate: float32 [], replicated
- clip_max: float32 [], replicated
Outputs:
- output 1: bfloat16 [512, 8192], replicated
- output 2: bfloat16 [8192, 512], replicated
- output 3: bfloat16 [512, 2048], replicated
- output 4: bfloat16 [2048, 512], replicated
- output 5: float32 [512, 8192], P('dp')
- output 6: float32 [8192, 512], P('dp')
- output 7: float32 [512, 2048], P('dp')
- output 8: float32 [2048, 512], P('dp')
- output 9: float32 [512, 8192], P('dp')
- output 10: float32 [8192, 512], P('dp')
- output 11: float32 [512, 2048], P('dp')
- output 12: float32 [2048, 512], P('dp')
- output 13: float32 [512, 8192], P('dp')
- output 14: float32 [8192, 512], P('dp')
- output 15: float32 [512, 2048], P('dp')
- output 16: float32 [2048, 512], P('dp')
- output 17: float32 [], replicated
All inputs are finite; a program needn't handle non-finite values.
Results may differ from the reference program's by a relative error of at most 0.0112006.
Values are sent between devices in bfloat16 or wider.
A program may use at most 1 GiB of HBM per device.

```python
import math
import jax
import jax.numpy as jnp
from jax import lax

MODEL_DIM = 512
FF_DIM = 2048
ROWS_DEV = 1024
DP_SIZE = 128
ADAM_STEP = 10
WIDE_DIM = 4 * FF_DIM
BETA_ONE = 0.9
BETA_TWO = 0.95
ADAM_EPS = 1e-8
NORM_EPS = 1e-6
BIAS_ONE = 1.0 - BETA_ONE ** ADAM_STEP
BIAS_TWO = 1.0 - BETA_TWO ** ADAM_STEP
INV_SQRT2 = 0.7071067811865476
INV_SQRT2PI = 0.3989422804014327
STD_ONE = 1.0 / (1.5 * math.sqrt(MODEL_DIM))
STD_TWO = math.sqrt(2.0 / 0.43) / math.sqrt(WIDE_DIM)
STD_THREE = 1.0 / math.sqrt(2.0 * MODEL_DIM)
STD_FOUR = 1.0 / math.sqrt(0.43 * FF_DIM)


def gelu_value(pre_act):
    pre_wide = pre_act.astype(jnp.float32)
    return 0.5 * pre_wide * (1.0 + lax.erf(pre_wide * INV_SQRT2))


def gelu_slope(pre_act):
    pre_wide = pre_act.astype(jnp.float32)
    return 0.5 * (1.0 + lax.erf(pre_wide * INV_SQRT2)) + pre_wide * INV_SQRT2PI * jnp.exp(-0.5 * pre_wide * pre_wide)


def local_grads(x_rows, dy_rows, w_one, w_two, w_three, w_four):
    z_one = jnp.dot(x_rows, w_one, preferred_element_type=jnp.float32).astype(jnp.bfloat16)
    a_one = gelu_value(z_one).astype(jnp.bfloat16)
    h_two = jnp.dot(a_one, w_two, preferred_element_type=jnp.float32).astype(jnp.bfloat16)
    z_three = jnp.dot(h_two, w_three, preferred_element_type=jnp.float32).astype(jnp.bfloat16)
    a_three = gelu_value(z_three).astype(jnp.bfloat16)
    g_four = jnp.dot(a_three.T, dy_rows, preferred_element_type=jnp.float32)
    da_three = jnp.dot(dy_rows, w_four.T, preferred_element_type=jnp.float32).astype(jnp.bfloat16)
    dz_three = (da_three.astype(jnp.float32) * gelu_slope(z_three)).astype(jnp.bfloat16)
    g_three = jnp.dot(h_two.T, dz_three, preferred_element_type=jnp.float32)
    dh_two = jnp.dot(dz_three, w_three.T, preferred_element_type=jnp.float32).astype(jnp.bfloat16)
    g_two = jnp.dot(a_one.T, dh_two, preferred_element_type=jnp.float32)
    da_one = jnp.dot(dh_two, w_two.T, preferred_element_type=jnp.float32).astype(jnp.bfloat16)
    dz_one = (da_one.astype(jnp.float32) * gelu_slope(z_one)).astype(jnp.bfloat16)
    g_one = jnp.dot(x_rows.T, dz_one, preferred_element_type=jnp.float32)
    return g_one, g_two, g_three, g_four


def mean_grads(x_rows, dy_rows, w_one, w_two, w_three, w_four):
    x_parts = x_rows.reshape(DP_SIZE, ROWS_DEV, MODEL_DIM)
    dy_parts = dy_rows.reshape(DP_SIZE, ROWS_DEV, MODEL_DIM)
    zero_sums = (jnp.zeros((MODEL_DIM, WIDE_DIM), jnp.float32), jnp.zeros((WIDE_DIM, MODEL_DIM), jnp.float32), jnp.zeros((MODEL_DIM, FF_DIM), jnp.float32), jnp.zeros((FF_DIM, MODEL_DIM), jnp.float32))

    def add_part(running, part_pair):
        part_grads = local_grads(part_pair[0], part_pair[1], w_one, w_two, w_three, w_four)
        return tuple(run_sum + new_grad for run_sum, new_grad in zip(running, part_grads)), None

    grad_sums, _unused = lax.scan(add_part, zero_sums, (x_parts, dy_parts))
    return tuple(grad_sum / DP_SIZE for grad_sum in grad_sums)


def adam_rows(grad_mat, master_mat, mom_mat, var_mat, clip_scale, learn_rate):
    scaled = clip_scale * grad_mat
    mom_new = BETA_ONE * mom_mat + (1.0 - BETA_ONE) * scaled
    var_new = BETA_TWO * var_mat + (1.0 - BETA_TWO) * scaled * scaled
    master_new = master_mat - learn_rate * (mom_new / BIAS_ONE) / (jnp.sqrt(var_new / BIAS_TWO) + ADAM_EPS)
    return master_new, mom_new, var_new


def setup_inputs(seed: int = 0) -> dict:
    key_list = jax.random.split(jax.random.key(seed), 16)
    batch_rows = DP_SIZE * ROWS_DEV
    x_rows = (1.5 * jax.random.normal(key_list[0], (batch_rows, MODEL_DIM), jnp.float32)).astype(jnp.bfloat16)
    dy_rows = jax.random.normal(key_list[1], (batch_rows, MODEL_DIM), jnp.float32).astype(jnp.bfloat16)
    shape_list = ((MODEL_DIM, WIDE_DIM), (WIDE_DIM, MODEL_DIM), (MODEL_DIM, FF_DIM), (FF_DIM, MODEL_DIM))
    std_list = (STD_ONE, STD_TWO, STD_THREE, STD_FOUR)
    masters = [std_val * jax.random.normal(key_list[2 + mat_index], shape_list[mat_index], jnp.float32) for mat_index, std_val in enumerate(std_list)]
    weights = [master_mat.astype(jnp.bfloat16) for master_mat in masters]
    grads = mean_grads(x_rows, dy_rows, weights[0], weights[1], weights[2], weights[3])
    grad_norm = jnp.sqrt(sum(jnp.sum(grad_mat * grad_mat) for grad_mat in grads))
    clip_frac = jax.random.uniform(key_list[6], (), jnp.float32, minval=0.3, maxval=0.7)
    clip_max = clip_frac * grad_norm
    learn_rate = jax.random.uniform(key_list[7], (), jnp.float32, minval=0.5, maxval=1.5) / math.sqrt(MODEL_DIM)
    mom_list = []
    var_list = []
    for mat_index, grad_mat in enumerate(grads):
        grad_rms = clip_frac * jnp.sqrt(jnp.mean(grad_mat * grad_mat))
        mom_list.append(0.1 * grad_rms * jax.random.normal(key_list[8 + mat_index], shape_list[mat_index], jnp.float32))
        var_list.append(grad_rms * grad_rms * jax.random.uniform(key_list[12 + mat_index], shape_list[mat_index], jnp.float32, minval=0.5, maxval=1.5))
    return {'x_rows': x_rows, 'dy_rows': dy_rows, 'w_one': weights[0], 'w_two': weights[1], 'w_three': weights[2], 'w_four': weights[3], 'master_one': masters[0], 'master_two': masters[1], 'master_three': masters[2], 'master_four': masters[3], 'm_one': mom_list[0], 'm_two': mom_list[1], 'm_three': mom_list[2], 'm_four': mom_list[3], 'v_one': var_list[0], 'v_two': var_list[1], 'v_three': var_list[2], 'v_four': var_list[3], 'learn_rate': learn_rate, 'clip_max': clip_max}


def reference(x_rows, dy_rows, w_one, w_two, w_three, w_four, master_one, master_two, master_three, master_four, m_one, m_two, m_three, m_four, v_one, v_two, v_three, v_four, learn_rate, clip_max):
    grads = mean_grads(x_rows, dy_rows, w_one, w_two, w_three, w_four)
    grad_norm = jnp.sqrt(sum(jnp.sum(grad_mat * grad_mat) for grad_mat in grads))
    clip_scale = jnp.minimum(1.0, clip_max / (grad_norm + NORM_EPS))
    res_one = adam_rows(grads[0], master_one, m_one, v_one, clip_scale, learn_rate)
    res_two = adam_rows(grads[1], master_two, m_two, v_two, clip_scale, learn_rate)
    res_three = adam_rows(grads[2], master_three, m_three, v_three, clip_scale, learn_rate)
    res_four = adam_rows(grads[3], master_four, m_four, v_four, clip_scale, learn_rate)
    return (res_one[0].astype(jnp.bfloat16), res_two[0].astype(jnp.bfloat16), res_three[0].astype(jnp.bfloat16), res_four[0].astype(jnp.bfloat16), res_one[0], res_two[0], res_three[0], res_four[0], res_one[1], res_two[1], res_three[1], res_four[1], res_one[2], res_two[2], res_three[2], res_four[2], grad_norm)
```

```python
import functools

import jax
import jax.numpy as jnp
from jax import lax
from jax.experimental import pallas as pl
from jax.experimental.pallas import tpu as pltpu
from jax.sharding import PartitionSpec as P

ADAM_STEP = 10
BETA_ONE = 0.9
BETA_TWO = 0.95
ADAM_EPS = 1e-8
NORM_EPS = 1e-6
BIAS_ONE = 1.0 - BETA_ONE ** ADAM_STEP
BIAS_TWO = 1.0 - BETA_TWO ** ADAM_STEP
INV_SQRT2 = 0.7071067811865476
INV_SQRT2PI = 0.3989422804014327

WIDTH = 512
SIDE = 4
ROWS = 8
UNITS_OF = {3: 2, 4: 2, 2: 8, 1: 8}
SLOTS = 4
MESH_ID = pl.DeviceIdType.MESH
VMEM_BYTES = 62 * 1024 * 1024


def unit_list():
    return [(mat, piece) for mat in (3, 4, 2, 1) for piece in range(UNITS_OF[mat])]


def first_unit(mat):
    return unit_list().index((mat, 0))


def gelu_value(pre_act):
    pre_wide = pre_act.astype(jnp.float32)
    return 0.5 * pre_wide * (1.0 + lax.erf(pre_wide * INV_SQRT2))


def gelu_slope(pre_act):
    pre_wide = pre_act.astype(jnp.float32)
    return 0.5 * (1.0 + lax.erf(pre_wide * INV_SQRT2)) + pre_wide * INV_SQRT2PI * jnp.exp(-0.5 * pre_wide * pre_wide)


def local_grads(x_rows, dy_rows, w_one, w_two, w_three, w_four):
    z_one = jnp.dot(x_rows, w_one, preferred_element_type=jnp.float32).astype(jnp.bfloat16)
    a_one = gelu_value(z_one).astype(jnp.bfloat16)
    h_two = jnp.dot(a_one, w_two, preferred_element_type=jnp.float32).astype(jnp.bfloat16)
    z_three = jnp.dot(h_two, w_three, preferred_element_type=jnp.float32).astype(jnp.bfloat16)
    a_three = gelu_value(z_three).astype(jnp.bfloat16)
    g_four = jnp.einsum('rf,rd->fd', a_three, dy_rows, preferred_element_type=jnp.float32)
    da_three = jnp.einsum('rd,fd->rf', dy_rows, w_four, preferred_element_type=jnp.float32).astype(jnp.bfloat16)
    dz_three = (da_three.astype(jnp.float32) * gelu_slope(z_three)).astype(jnp.bfloat16)
    g_three = jnp.einsum('rd,rf->df', h_two, dz_three, preferred_element_type=jnp.float32)
    dh_two = jnp.einsum('rf,df->rd', dz_three, w_three, preferred_element_type=jnp.float32).astype(jnp.bfloat16)
    g_two = jnp.einsum('rw,rd->wd', a_one, dh_two, preferred_element_type=jnp.float32)
    da_one = jnp.einsum('rd,wd->rw', dh_two, w_two, preferred_element_type=jnp.float32).astype(jnp.bfloat16)
    dz_one = (da_one.astype(jnp.float32) * gelu_slope(z_one)).astype(jnp.bfloat16)
    g_one = jnp.einsum('rd,rw->dw', x_rows, dz_one, preferred_element_type=jnp.float32)
    return g_one, g_two, g_three, g_four


class Place:
    def __init__(self):
        me = lax.axis_index('dp')
        self.core = lax.rem(me, 2)
        self.coords = [lax.div(me, 2 * SIDE * SIDE), lax.rem(lax.div(me, 2 * SIDE), SIDE), lax.rem(lax.div(me, 2), SIDE)]

    def step(self, axis, by):
        return lax.rem(self.coords[axis] + by, SIDE)

    def device(self, moves=None, other_core=False):
        pos = list(self.coords)
        for axis, by in (moves or {}).items():
            pos[axis] = self.step(axis, by)
        core = 1 - self.core if other_core else self.core
        return (((pos[0] * SIDE + pos[1]) * SIDE + pos[2]) * 2 + core,)

    def neighbours(self):
        found = [self.device(other_core=True)]
        for axis in range(3):
            found += [self.device({axis: 1}), self.device({axis: SIDE - 1})]
        return found


def enter(peers):
    barrier = pltpu.get_barrier_semaphore()
    for peer in peers:
        pl.semaphore_signal(barrier, inc=1, device_id=peer, device_id_type=MESH_ID)
    pl.semaphore_wait(barrier, len(peers))


def send(src, dst, send_sem, recv_sem, peer):
    pltpu.make_async_remote_copy(src_ref=src, dst_ref=dst, send_sem=send_sem, recv_sem=recv_sem, device_id=peer, device_id_type=MESH_ID).start()


def await_bytes(ref, sem):
    pltpu.make_async_copy(ref, ref, sem).wait()


def spot(lead, dims, fixed, cols):
    return tuple(lead) + tuple(fixed.get(axis, slice(None)) for axis in dims) + (slice(None), cols)


LEFT = pl.ds(0, WIDTH // 2)
RIGHT = pl.ds(WIDTH // 2, WIDTH // 2)
ALL = slice(None)


class RingSum:
    def __init__(self, place, dims, axis, relay, final, relay_sem, final_sem, send_sem):
        self.place, self.dims, self.axis = place, dims, axis
        self.relay, self.final = relay, final
        self.relay_sem, self.final_sem, self.send_sem = relay_sem, final_sem, send_sem
        self.own = place.coords[axis]
        self.up, self.down, self.far = place.step(axis, 1), place.step(axis, SIDE - 1), place.step(axis, 2)
        self.up_dev, self.down_dev = place.device({axis: 1}), place.device({axis: SIDE - 1})
        self.rest = [dim for dim in dims if dim != axis]

    def start(self, src, lead, unit):
        s = self
        send(src.at[spot(lead, s.dims, {s.axis: s.far}, LEFT)], s.relay.at[unit, 0], s.send_sem.at[unit], s.relay_sem.at[unit], s.up_dev)
        send(src.at[spot(lead, s.dims, {s.axis: s.far}, RIGHT)], s.relay.at[unit, 1], s.send_sem.at[unit], s.relay_sem.at[unit], s.down_dev)
        send(src.at[spot(lead, s.dims, {s.axis: s.up}, RIGHT)], s.final.at[spot((unit, 0), s.rest, {}, RIGHT)], s.send_sem.at[unit], s.final_sem.at[unit], s.up_dev)
        send(src.at[spot(lead, s.dims, {s.axis: s.down}, LEFT)], s.final.at[spot((unit, 1), s.rest, {}, LEFT)], s.send_sem.at[unit], s.final_sem.at[unit], s.down_dev)

    def pass_on(self, src, lead, unit):
        s = self
        await_bytes(s.relay.at[unit], s.relay_sem.at[unit])
        up_spot = spot(lead, s.dims, {s.axis: s.up}, LEFT)
        src[up_spot] = src[up_spot] + s.relay[unit, 0]
        send(src.at[up_spot], s.final.at[spot((unit, 0), s.rest, {}, LEFT)], s.send_sem.at[unit], s.final_sem.at[unit], s.up_dev)
        down_spot = spot(lead, s.dims, {s.axis: s.down}, RIGHT)
        src[down_spot] = src[down_spot] + s.relay[unit, 1]
        send(src.at[down_spot], s.final.at[spot((unit, 1), s.rest, {}, RIGHT)], s.send_sem.at[unit], s.final_sem.at[unit], s.down_dev)

    def finish(self, src, lead, unit):
        s = self
        await_bytes(s.final.at[unit], s.final_sem.at[unit])
        return src[spot(lead, s.dims, {s.axis: s.own}, ALL)] + s.final[unit, 0] + s.final[unit, 1]

    def drain(self, unit):
        await_bytes(self.relay.at[unit], self.send_sem.at[unit])
        await_bytes(self.final.at[unit], self.send_sem.at[unit])


def reduce_kernel(g_one, g_two, g_three, g_four, shard, swapped, norm_tile, own, part, relay1, final1, relay2, final2, relay3, final3, mid, low, norm_own, norm_a, norm_b, norm_c, load_sem, part_send, part_recv, ring_sems, swap_sems, norm_sems):
    place = Place()
    units = unit_list()
    chunks = -(-len(units) // 3)
    counts = [len(range(order, len(units), 3)) for order in range(3)]
    partner = place.device(other_core=True)
    group_x = [(place.device({2: by}, other_core=swap)) for by in range(SIDE) for swap in (False, True) if by or swap]
    group_y = [place.device({1: by}) for by in range(1, SIDE)]
    group_z = [place.device({0: by}) for by in range(1, SIDE)]
    enter(group_x + group_y + group_z)

    def source(mat, piece, core):
        if mat in (1, 3):
            ref = g_one if mat == 1 else g_three
            start = core * (UNITS_OF[mat] * WIDTH) + piece * WIDTH
            return ref.at[:, :, :, :, pl.ds(pl.multiple_of(start, WIDTH), WIDTH)]
        ref = g_two if mat == 2 else g_four
        return ref.at[:, :, :, core, pl.ds(piece * ROWS, ROWS), :]

    rings = []
    for order in range(3):
        a, b = order, (order + 1) % 3
        c = (order + 2) % 3
        first = RingSum(place, [0, 1, 2], a, relay1, final1, ring_sems.at[0, 0], ring_sems.at[0, 1], ring_sems.at[0, 2])
        second = RingSum(place, first.rest, b, relay2, final2, ring_sems.at[1, 0], ring_sems.at[1, 1], ring_sems.at[1, 2])
        third = RingSum(place, second.rest, c, relay3, final3, ring_sems.at[2, 0], ring_sems.at[2, 1], ring_sems.at[2, 2])
        rings.append((first, second, third))

    def load(chunk):
        for order in range(3):
            unit = 3 * chunk + order
            if unit >= len(units):
                continue
            mat, piece = units[unit]
            send(source(mat, piece, 1 - place.core), part.at[unit], part_send.at[unit], part_recv.at[unit], partner)
            if chunk >= SLOTS:
                rings[order][0].drain(unit - 3 * SLOTS)
            pltpu.make_async_copy(source(mat, piece, place.core), own.at[order, chunk % SLOTS], load_sem.at[unit]).start()

    def stage_b(order, chunk, unit):
        lead = (order, lax.rem(chunk, SLOTS))
        await_bytes(own.at[lead], load_sem.at[unit])
        await_bytes(part.at[unit], part_recv.at[unit])
        own[lead] = own[lead] + part[unit]
        rings[order][0].start(own, lead, unit)

    def stage_c(order, chunk, unit):
        rings[order][0].pass_on(own, (order, lax.rem(chunk, SLOTS)), unit)

    def stage_d(order, chunk, unit):
        mid[unit] = rings[order][0].finish(own, (order, lax.rem(chunk, SLOTS)), unit)
        rings[order][1].start(mid, (unit,), unit)

    def stage_e(order, chunk, unit):
        rings[order][1].pass_on(mid, (unit,), unit)

    def stage_f(order, chunk, unit):
        low[unit] = rings[order][1].finish(mid, (unit,), unit)
        rings[order][2].start(low, (unit,), unit)

    def stage_g(order, chunk, unit):
        rings[order][2].pass_on(low, (unit,), unit)

    def stage_h(order, chunk, unit):
        shard[unit] = rings[order][2].finish(low, (unit,), unit) * (1.0 / (2 * SIDE ** 3))

    stages = (stage_b, stage_c, stage_d, stage_e, stage_f, stage_g, stage_h)

    def turn(now, carry):
        for chunk in range(chunks):
            @pl.when(now == chunk)
            def _(chunk=chunk):
                load(chunk)
        for lag, stage in enumerate(stages):
            chunk = now - lag - 1
            for order in range(3):
                @pl.when((chunk >= 0) & (chunk < counts[order]))
                def _(stage=stage, order=order, chunk=chunk):
                    stage(order, chunk, 3 * chunk + order)
        return carry

    lax.fori_loop(0, chunks + len(stages), turn, 0)

    n_three = UNITS_OF[3]
    n_one = UNITS_OF[1]
    base_one = first_unit(1)
    send(shard.at[pl.ds(0, n_three)], swapped.at[pl.ds(0, n_three)], swap_sems.at[0], swap_sems.at[1], partner)
    send(shard.at[pl.ds(base_one, n_one)], swapped.at[pl.ds(n_three, n_one)], swap_sems.at[0], swap_sems.at[1], partner)

    def fold(unit, total):
        value = shard[unit]
        return total + value * value

    squares = lax.fori_loop(0, len(units), fold, jnp.zeros((ROWS, WIDTH), jnp.float32))
    total = squares[:, 0:128]
    for col in range(1, WIDTH // 128):
        total = total + squares[:, col * 128:(col + 1) * 128]
    levels = ((norm_a, group_x, place.coords[2] * 2 + place.core), (norm_b, group_y, place.coords[1]), (norm_c, group_z, place.coords[0]))
    for level, (board, group, seat) in enumerate(levels):
        norm_own[level] = total
        board[seat] = total
        for peer in group:
            send(norm_own.at[level], board.at[seat], norm_sems.at[0, level], norm_sems.at[1, level], peer)
        await_bytes(board.at[pl.ds(0, len(group))], norm_sems.at[1, level])
        total = board[0]
        for row in range(1, len(group) + 1):
            total = total + board[row]
    norm_tile[...] = total

    await_bytes(swapped, swap_sems.at[0])
    await_bytes(swapped, swap_sems.at[1])
    for level, (board, group, seat) in enumerate(levels):
        await_bytes(board.at[pl.ds(0, len(group))], norm_sems.at[0, level])
    for order in range(3):
        def tidy(chunk, carry, order=order):
            unit = 3 * chunk + order
            await_bytes(part.at[unit], part_send.at[unit])
            rings[order][1].drain(unit)
            rings[order][2].drain(unit)

            @pl.when(chunk >= counts[order] - SLOTS)
            def _():
                rings[order][0].drain(unit)
            return carry

        lax.fori_loop(0, counts[order], tidy, 0)


def reduce_grads(g_one, g_two, g_three, g_four):
    n = len(unit_list())
    cube = (SIDE, SIDE, SIDE)
    args = (
        g_one.reshape(cube + (ROWS, 2 * UNITS_OF[1] * WIDTH)),
        g_two.reshape(cube + (2, UNITS_OF[2] * ROWS, WIDTH)),
        g_three.reshape(cube + (ROWS, 2 * UNITS_OF[3] * WIDTH)),
        g_four.reshape(cube + (2, UNITS_OF[4] * ROWS, WIDTH)),
    )
    f32 = jnp.float32
    dma = pltpu.SemaphoreType.DMA
    scratch = [
        pltpu.VMEM((3, SLOTS) + cube + (ROWS, WIDTH), f32),
        pltpu.VMEM((n,) + cube + (ROWS, WIDTH), f32),
        pltpu.VMEM((n, 2, SIDE, SIDE, ROWS, WIDTH // 2), f32),
        pltpu.VMEM((n, 2, SIDE, SIDE, ROWS, WIDTH), f32),
        pltpu.VMEM((n, 2, SIDE, ROWS, WIDTH // 2), f32),
        pltpu.VMEM((n, 2, SIDE, ROWS, WIDTH), f32),
        pltpu.VMEM((n, 2, ROWS, WIDTH // 2), f32),
        pltpu.VMEM((n, 2, ROWS, WIDTH), f32),
        pltpu.VMEM((n, SIDE, SIDE, ROWS, WIDTH), f32),
        pltpu.VMEM((n, SIDE, ROWS, WIDTH), f32),
        pltpu.VMEM((3, ROWS, 128), f32),
        pltpu.VMEM((2 * SIDE, ROWS, 128), f32),
        pltpu.VMEM((SIDE, ROWS, 128), f32),
        pltpu.VMEM((SIDE, ROWS, 128), f32),
        dma((n,)), dma((n,)), dma((n,)), dma((3, 3, n)), dma((2,)), dma((2, 3)),
    ]
    any_spec = pl.BlockSpec(memory_space=pl.ANY)
    vmem_spec = pl.BlockSpec(memory_space=pltpu.VMEM)
    return pl.pallas_call(
        reduce_kernel,
        out_shape=(
            jax.ShapeDtypeStruct((n, ROWS, WIDTH), f32),
            jax.ShapeDtypeStruct((UNITS_OF[3] + UNITS_OF[1], ROWS, WIDTH), f32),
            jax.ShapeDtypeStruct((ROWS, 128), f32),
        ),
        in_specs=[any_spec] * 4,
        out_specs=(vmem_spec,) * 3,
        scratch_shapes=scratch,
        compiler_params=pltpu.CompilerParams(collective_id=0, has_side_effects=True, vmem_limit_bytes=VMEM_BYTES),
        name='reduce_grads',
    )(*args)


def adam_kernel(lr_ref, clip_ref, norm_tile, shard, swapped, *refs):
    masters, moms, variances = refs[0:4], refs[4:8], refs[8:12]
    new_masters, new_moms, new_vars = refs[12:16], refs[16:20], refs[20:24]
    two_rows, four_rows, norm_ref = refs[24:27]
    core = lax.rem(lax.axis_index('dp'), 2)
    grad_norm = jnp.sqrt(jnp.sum(jnp.sum(norm_tile[...], axis=1, keepdims=True), axis=0, keepdims=True))
    norm_ref[...] = grad_norm
    clip_scale = jnp.minimum(1.0, clip_ref[...] / (grad_norm + NORM_EPS))
    learn_rate = lr_ref[...]

    def update(mat, where, grad):
        scaled = clip_scale * grad
        mom_new = BETA_ONE * moms[mat][where] + (1.0 - BETA_ONE) * scaled
        var_new = BETA_TWO * variances[mat][where] + (1.0 - BETA_TWO) * scaled * scaled
        master_new = masters[mat][where] - learn_rate * (mom_new / BIAS_ONE) / (jnp.sqrt(var_new / BIAS_TWO) + ADAM_EPS)
        new_moms[mat][where] = mom_new
        new_vars[mat][where] = var_new
        new_masters[mat][where] = master_new
        return master_new

    for mat, rows_out in ((2, two_rows), (4, four_rows)):
        for piece in range(UNITS_OF[mat]):
            where = (slice(piece * ROWS, (piece + 1) * ROWS), slice(None))
            rows_out[piece] = update(mat - 1, where, shard[first_unit(mat) + piece]).astype(jnp.bfloat16)
    for mat, base in ((3, 0), (1, UNITS_OF[3])):
        for half in range(2):
            for piece in range(UNITS_OF[mat]):
                col = (half * UNITS_OF[mat] + piece) * WIDTH
                where = (slice(None), slice(col, col + WIDTH))
                block = jnp.where(core == half, shard[first_unit(mat) + piece], swapped[base + piece])
                update(mat - 1, where, jnp.where(core == 0, block[0:ROWS // 2], block[ROWS // 2:ROWS]))


def adam_update(learn_rate, clip_max, norm_tile, shard, swapped, masters, moms, variances):
    state = list(masters) + list(moms) + list(variances)
    f32, bf16 = jnp.float32, jnp.bfloat16
    vmem_spec = pl.BlockSpec(memory_space=pltpu.VMEM)
    out_shape = [jax.ShapeDtypeStruct(part.shape, f32) for part in state]
    out_shape += [
        jax.ShapeDtypeStruct((UNITS_OF[2], ROWS, WIDTH), bf16),
        jax.ShapeDtypeStruct((UNITS_OF[4], ROWS, WIDTH), bf16),
        jax.ShapeDtypeStruct((1, 1), f32),
    ]
    args = [learn_rate.reshape(1, 1), clip_max.reshape(1, 1), norm_tile, shard, swapped] + state
    return pl.pallas_call(
        adam_kernel,
        out_shape=out_shape,
        in_specs=[vmem_spec] * len(args),
        out_specs=[vmem_spec] * len(out_shape),
        name='adam_update',
    )(*args)


class RingSpread:
    def __init__(self, place, axis, known, board, near_sem, far_sem, send_sem):
        self.place, self.axis, self.known, self.board = place, axis, known, board
        self.near_sem, self.far_sem, self.send_sem = near_sem, far_sem, send_sem
        self.up_dev, self.down_dev = place.device({axis: 1}), place.device({axis: SIDE - 1})

    def block(self, unit, by, cols):
        fixed = {dim: self.place.coords[dim] for dim in range(3) if dim not in self.known}
        fixed[self.axis] = self.place.step(self.axis, by)
        return self.board.at[spot((unit,), [0, 1, 2], fixed, cols)]

    def blocks(self, unit, count):
        return self.board.at[(unit,) + (0,) * (2 - len(self.known)) + (pl.ds(0, count),)]

    def start(self, unit):
        s = self
        mine = s.block(unit, 0, ALL)
        send(mine, mine, s.send_sem.at[unit], s.near_sem.at[unit], s.up_dev)
        send(mine, mine, s.send_sem.at[unit], s.near_sem.at[unit], s.down_dev)

    def pass_on(self, unit):
        s = self
        await_bytes(s.blocks(unit, 2), s.near_sem.at[unit])
        from_down, from_up = s.block(unit, SIDE - 1, LEFT), s.block(unit, 1, RIGHT)
        send(from_down, from_down, s.send_sem.at[unit], s.far_sem.at[unit], s.up_dev)
        send(from_up, from_up, s.send_sem.at[unit], s.far_sem.at[unit], s.down_dev)

    def finish(self, unit):
        await_bytes(self.block(unit, 0, ALL), self.far_sem.at[unit])

    def drain(self, unit):
        await_bytes(self.blocks(unit, 3), self.send_sem.at[unit])


def gather_kernel(one_rows, three_rows, two_rows, four_rows, board, other, swap_one, swap_three, ring_sems, pair_sems, swap_sems):
    place = Place()
    units = unit_list()
    chunks = -(-len(units) // 3)
    counts = [len(range(order, len(units), 3)) for order in range(3)]
    partner = place.device(other_core=True)
    here = tuple(place.coords)
    enter(place.neighbours())
    splits = ((1, one_rows, swap_one), (3, three_rows, swap_three))
    for index, (mat, rows, landing) in enumerate(splits):
        span = UNITS_OF[mat] * WIDTH
        theirs = rows.at[:, pl.ds(pl.multiple_of((1 - place.core) * span, WIDTH), span)]
        send(theirs, landing, swap_sems.at[0, index], swap_sems.at[1, index], partner)
    for mat, rows in ((2, two_rows), (4, four_rows)):
        for piece in range(UNITS_OF[mat]):
            board[(first_unit(mat) + piece,) + here] = rows[piece]
    for index, (mat, rows, landing) in enumerate(splits):
        await_bytes(landing, swap_sems.at[1, index])
        for piece in range(UNITS_OF[mat]):
            start = place.core * (UNITS_OF[mat] * WIDTH) + piece * WIDTH
            mine = rows[:, pl.ds(pl.multiple_of(start, WIDTH), WIDTH)]
            theirs = landing[:, piece * WIDTH:(piece + 1) * WIDTH]
            top = jnp.where(place.core == 0, mine, theirs)
            bottom = jnp.where(place.core == 0, theirs, mine)
            board[(first_unit(mat) + piece,) + here] = jnp.concatenate([top, bottom], axis=0).astype(board.dtype)

    rings = []
    for order in range(3):
        axes = (order + 2) % 3, (order + 1) % 3, order
        rings.append([RingSpread(place, axis, axes[:level], board, ring_sems.at[level, 0], ring_sems.at[level, 1], ring_sems.at[level, 2]) for level, axis in enumerate(axes)])

    def every(action):
        def turn(chunk, carry):
            for order in range(3):
                @pl.when(chunk < counts[order])
                def _(order=order):
                    action(order, 3 * chunk + order)
            return carry

        lax.fori_loop(0, chunks, turn, 0)

    def begin(order, unit):
        rings[order][0].start(unit)

    every(begin)
    for level in range(3):
        def pass_on(order, unit, level=level):
            rings[order][level].pass_on(unit)

        def onward(order, unit, level=level):
            rings[order][level].finish(unit)
            if level < 2:
                rings[order][level + 1].start(unit)
            else:
                send(board.at[unit], other.at[unit], pair_sems.at[0, unit], pair_sems.at[1, unit], partner)

        every(pass_on)
        every(onward)

    def tidy(order, unit):
        await_bytes(other.at[unit], pair_sems.at[1, unit])
        await_bytes(board.at[unit], pair_sems.at[0, unit])
        for level in range(3):
            rings[order][level].drain(unit)

    every(tidy)
    for index, (mat, rows, landing) in enumerate(splits):
        await_bytes(landing, swap_sems.at[0, index])


def gather_rows(one_rows, three_rows, two_rows, four_rows):
    n = len(unit_list())
    cube = (SIDE, SIDE, SIDE)
    bf16, f32 = jnp.bfloat16, jnp.float32
    dma = pltpu.SemaphoreType.DMA
    vmem_spec = pl.BlockSpec(memory_space=pltpu.VMEM)
    full = jax.ShapeDtypeStruct((n,) + cube + (ROWS, WIDTH), bf16)
    return pl.pallas_call(
        gather_kernel,
        out_shape=(full, full),
        in_specs=[vmem_spec] * 4,
        out_specs=(vmem_spec, vmem_spec),
        scratch_shapes=[
            pltpu.VMEM((ROWS // 2, UNITS_OF[1] * WIDTH), f32),
            pltpu.VMEM((ROWS // 2, UNITS_OF[3] * WIDTH), f32),
            dma((3, 3, n)), dma((2, n)), dma((2, 2)),
        ],
        compiler_params=pltpu.CompilerParams(collective_id=1, has_side_effects=True, vmem_limit_bytes=32 * 1024 * 1024),
        name='gather_rows',
    )(one_rows, three_rows, two_rows, four_rows)


def place_kernel(board, other, w_one, w_two, w_three, w_four, sems):
    core = lax.rem(lax.axis_index('dp'), 2)
    outs = {1: w_one, 2: w_two, 3: w_three, 4: w_four}
    copies = []
    for unit, (mat, piece) in enumerate(unit_list()):
        for index, (source, owner) in enumerate(((board, core), (other, 1 - core))):
            if mat in (1, 3):
                start = owner * (UNITS_OF[mat] * WIDTH) + piece * WIDTH
                target = outs[mat].at[:, :, :, :, pl.ds(pl.multiple_of(start, WIDTH), WIDTH)]
            else:
                target = outs[mat].at[:, :, :, owner, pl.ds(piece * ROWS, ROWS), :]
            copies.append(pltpu.make_async_copy(source.at[unit], target, sems.at[index, unit]))
    for copy in copies:
        copy.start()
    for copy in copies:
        copy.wait()


def place_weights(board, other):
    n = len(unit_list())
    cube = (SIDE, SIDE, SIDE)
    bf16 = jnp.bfloat16
    vmem_spec = pl.BlockSpec(memory_space=pltpu.VMEM)
    any_spec = pl.BlockSpec(memory_space=pl.ANY)
    outs = pl.pallas_call(
        place_kernel,
        out_shape=(
            jax.ShapeDtypeStruct(cube + (ROWS, 2 * UNITS_OF[1] * WIDTH), bf16),
            jax.ShapeDtypeStruct(cube + (2, UNITS_OF[2] * ROWS, WIDTH), bf16),
            jax.ShapeDtypeStruct(cube + (ROWS, 2 * UNITS_OF[3] * WIDTH), bf16),
            jax.ShapeDtypeStruct(cube + (2, UNITS_OF[4] * ROWS, WIDTH), bf16),
        ),
        in_specs=[vmem_spec] * 2,
        out_specs=(any_spec,) * 4,
        scratch_shapes=[pltpu.SemaphoreType.DMA((2, n))],
        compiler_params=pltpu.CompilerParams(vmem_limit_bytes=2 * 1024 * 1024),
        name='place_weights',
    )(board, other)
    rows = SIDE ** 3 * ROWS
    return (
        outs[0].reshape(rows, 2 * UNITS_OF[1] * WIDTH),
        outs[1].reshape(2 * SIDE ** 3 * UNITS_OF[2] * ROWS, WIDTH),
        outs[2].reshape(rows, 2 * UNITS_OF[3] * WIDTH),
        outs[3].reshape(2 * SIDE ** 3 * UNITS_OF[4] * ROWS, WIDTH),
    )


def sync_and_update(grads, masters, moms, variances, learn_rate, clip_max):
    shard, swapped, norm_tile = reduce_grads(*grads)
    results = adam_update(learn_rate, clip_max, norm_tile, shard, swapped, masters, moms, variances)
    new_masters, new_moms, new_vars = results[0:4], results[4:8], results[8:12]
    two_rows, four_rows, grad_norm = results[12:15]
    board, other = gather_rows(new_masters[0], new_masters[2], two_rows, four_rows)
    new_weights = place_weights(board, other)
    return tuple(new_weights) + tuple(new_masters) + tuple(new_moms) + tuple(new_vars) + (grad_norm.reshape(()),)


def solution(mesh):
    row_spec = P('dp', None)
    rep_spec = P()

    def per_device(x_rows, dy_rows, w_one, w_two, w_three, w_four, master_one, master_two, master_three, master_four, m_one, m_two, m_three, m_four, v_one, v_two, v_three, v_four, learn_rate, clip_max):
        grads = local_grads(x_rows, dy_rows, w_one, w_two, w_three, w_four)
        return sync_and_update(grads, (master_one, master_two, master_three, master_four), (m_one, m_two, m_three, m_four), (v_one, v_two, v_three, v_four), learn_rate, clip_max)

    in_specs = (row_spec, row_spec) + (rep_spec,) * 4 + (row_spec,) * 12 + (rep_spec, rep_spec)
    out_specs = (rep_spec,) * 4 + (row_spec,) * 12 + (rep_spec,)
    return jax.shard_map(per_device, mesh=mesh, in_specs=in_specs, out_specs=out_specs, check_vma=False)
```

```python
import functools

import jax
import jax.numpy as jnp
from jax import lax
from jax.experimental import pallas as pl
from jax.experimental.pallas import tpu as pltpu
from jax.sharding import PartitionSpec as P

ADAM_STEP = 10
BETA_ONE = 0.9
BETA_TWO = 0.95
ADAM_EPS = 1e-8
NORM_EPS = 1e-6
BIAS_ONE = 1.0 - BETA_ONE ** ADAM_STEP
BIAS_TWO = 1.0 - BETA_TWO ** ADAM_STEP
INV_SQRT2 = 0.7071067811865476
INV_SQRT2PI = 0.3989422804014327

WIDTH = 512
SIDE = 4
ROWS = 8
UNITS_OF = {3: 2, 4: 2, 2: 8, 1: 8}
MESH_ID = pl.DeviceIdType.MESH
VMEM_BYTES = 62 * 1024 * 1024


def unit_list():
    return [(mat, piece) for mat in (3, 4, 2, 1) for piece in range(UNITS_OF[mat])]


def first_unit(mat):
    return unit_list().index((mat, 0))


def gelu_value(pre_act):
    pre_wide = pre_act.astype(jnp.float32)
    return 0.5 * pre_wide * (1.0 + lax.erf(pre_wide * INV_SQRT2))


def gelu_slope(pre_act):
    pre_wide = pre_act.astype(jnp.float32)
    return 0.5 * (1.0 + lax.erf(pre_wide * INV_SQRT2)) + pre_wide * INV_SQRT2PI * jnp.exp(-0.5 * pre_wide * pre_wide)


def forward_kernel(x_ref, w_one, w_two, z_out, a_out, h_out, total):
    step = pl.program_id(0)

    @pl.when(step == 0)
    def _():
        total[...] = jnp.zeros_like(total)

    z_one = jnp.dot(x_ref[...], w_one[...], preferred_element_type=jnp.float32).astype(jnp.bfloat16)
    z_out[...] = z_one
    a_one = gelu_value(z_one).astype(jnp.bfloat16)
    a_out[...] = a_one
    total[...] += jnp.dot(a_one, w_two[...], preferred_element_type=jnp.float32)

    @pl.when(step == pl.num_programs(0) - 1)
    def _():
        h_out[...] = total[...].astype(jnp.bfloat16)


def forward_wide(x_rows, w_one, w_two):
    rows, dim = x_rows.shape
    wide = w_one.shape[1]
    block = 512
    bf16 = jnp.bfloat16
    return pl.pallas_call(
        forward_kernel,
        grid=(wide // block,),
        out_shape=(jax.ShapeDtypeStruct((rows, wide), bf16), jax.ShapeDtypeStruct((rows, wide), bf16), jax.ShapeDtypeStruct((rows, dim), bf16)),
        in_specs=[pl.BlockSpec((rows, dim), lambda i: (0, 0)), pl.BlockSpec((dim, block), lambda i: (0, i)), pl.BlockSpec((block, dim), lambda i: (i, 0))],
        out_specs=(pl.BlockSpec((rows, block), lambda i: (0, i)), pl.BlockSpec((rows, block), lambda i: (0, i)), pl.BlockSpec((rows, dim), lambda i: (0, 0))),
        scratch_shapes=[pltpu.VMEM((rows, dim), jnp.float32)],
        compiler_params=pltpu.CompilerParams(vmem_limit_bytes=VMEM_BYTES),
        name='forward_wide',
    )(x_rows, w_one, w_two)


def local_grads(x_rows, dy_rows, w_one, w_two, w_three, w_four):
    z_one, a_one, h_two = forward_wide(x_rows, w_one, w_two)
    z_three = jnp.dot(h_two, w_three, preferred_element_type=jnp.float32).astype(jnp.bfloat16)
    a_three = gelu_value(z_three).astype(jnp.bfloat16)
    g_four = jnp.einsum('rf,rd->fd', a_three, dy_rows, preferred_element_type=jnp.float32)
    da_three = jnp.einsum('rd,fd->rf', dy_rows, w_four, preferred_element_type=jnp.float32).astype(jnp.bfloat16)
    dz_three = (da_three.astype(jnp.float32) * gelu_slope(z_three)).astype(jnp.bfloat16)
    g_three = jnp.einsum('rd,rf->df', h_two, dz_three, preferred_element_type=jnp.float32)
    dh_two = jnp.einsum('rf,df->rd', dz_three, w_three, preferred_element_type=jnp.float32).astype(jnp.bfloat16)
    g_two = jnp.einsum('rw,rd->wd', a_one, dh_two, preferred_element_type=jnp.float32)
    return (x_rows.T, dh_two, z_one, w_two), g_two, g_three, g_four


class Place:
    def __init__(self):
        me = lax.axis_index('dp')
        self.core = lax.rem(me, 2)
        self.coords = [lax.div(me, 2 * SIDE * SIDE), lax.rem(lax.div(me, 2 * SIDE), SIDE), lax.rem(lax.div(me, 2), SIDE)]

    def step(self, axis, by):
        return lax.rem(self.coords[axis] + by, SIDE)

    def device(self, moves=None, other_core=False):
        pos = list(self.coords)
        for axis, by in (moves or {}).items():
            pos[axis] = self.step(axis, by)
        core = 1 - self.core if other_core else self.core
        return (((pos[0] * SIDE + pos[1]) * SIDE + pos[2]) * 2 + core,)

    def neighbours(self):
        found = [self.device(other_core=True)]
        for axis in range(3):
            found += [self.device({axis: 1}), self.device({axis: SIDE - 1})]
        return found


def enter(peers):
    barrier = pltpu.get_barrier_semaphore()
    for peer in peers:
        pl.semaphore_signal(barrier, inc=1, device_id=peer, device_id_type=MESH_ID)
    pl.semaphore_wait(barrier, len(peers))


def send(src, dst, send_sem, recv_sem, peer):
    pltpu.make_async_remote_copy(src_ref=src, dst_ref=dst, send_sem=send_sem, recv_sem=recv_sem, device_id=peer, device_id_type=MESH_ID).start()


def await_bytes(ref, sem):
    pltpu.make_async_copy(ref, ref, sem).wait()


def spot(lead, dims, fixed, cols):
    return tuple(lead) + tuple(fixed.get(axis, slice(None)) for axis in dims) + (slice(None), cols)


LEFT = pl.ds(0, WIDTH // 2)
RIGHT = pl.ds(WIDTH // 2, WIDTH // 2)
ALL = slice(None)


class RingSum:
    def __init__(self, place, dims, axis, relay, final, relay_sem, final_sem, send_sem):
        self.place, self.dims, self.axis = place, dims, axis
        self.relay, self.final = relay, final
        self.relay_sem, self.final_sem, self.send_sem = relay_sem, final_sem, send_sem
        self.own = place.coords[axis]
        self.up, self.down, self.far = place.step(axis, 1), place.step(axis, SIDE - 1), place.step(axis, 2)
        self.up_dev, self.down_dev = place.device({axis: 1}), place.device({axis: SIDE - 1})
        self.rest = [dim for dim in dims if dim != axis]

    def start(self, src, lead, unit):
        s = self
        send(src.at[spot(lead, s.dims, {s.axis: s.far}, LEFT)], s.relay.at[unit, 0], s.send_sem.at[unit], s.relay_sem.at[unit], s.up_dev)
        send(src.at[spot(lead, s.dims, {s.axis: s.far}, RIGHT)], s.relay.at[unit, 1], s.send_sem.at[unit], s.relay_sem.at[unit], s.down_dev)
        send(src.at[spot(lead, s.dims, {s.axis: s.up}, RIGHT)], s.final.at[spot((unit, 0), s.rest, {}, RIGHT)], s.send_sem.at[unit], s.final_sem.at[unit], s.up_dev)
        send(src.at[spot(lead, s.dims, {s.axis: s.down}, LEFT)], s.final.at[spot((unit, 1), s.rest, {}, LEFT)], s.send_sem.at[unit], s.final_sem.at[unit], s.down_dev)

    def pass_on(self, src, lead, unit):
        s = self
        await_bytes(s.relay.at[unit], s.relay_sem.at[unit])
        up_spot = spot(lead, s.dims, {s.axis: s.up}, LEFT)
        src[up_spot] = src[up_spot] + s.relay[unit, 0]
        send(src.at[up_spot], s.final.at[spot((unit, 0), s.rest, {}, LEFT)], s.send_sem.at[unit], s.final_sem.at[unit], s.up_dev)
        down_spot = spot(lead, s.dims, {s.axis: s.down}, RIGHT)
        src[down_spot] = src[down_spot] + s.relay[unit, 1]
        send(src.at[down_spot], s.final.at[spot((unit, 1), s.rest, {}, RIGHT)], s.send_sem.at[unit], s.final_sem.at[unit], s.down_dev)

    def finish(self, src, lead, unit):
        s = self
        await_bytes(s.final.at[unit], s.final_sem.at[unit])
        return src[spot(lead, s.dims, {s.axis: s.own}, ALL)] + s.final[unit, 0] + s.final[unit, 1]

    def drain(self, unit):
        await_bytes(self.relay.at[unit], self.send_sem.at[unit])
        await_bytes(self.final.at[unit], self.send_sem.at[unit])


BLOCK = 256
BLOCKS_PER_UNIT = 2 * (WIDTH // BLOCK)
BLOCKS_PER_TURN = 6


def reduce_kernel(x_turned, dh_two, z_one, w_two, g_two, g_three, g_four, shard, swapped, norm_tile, own, wide_own, part, relay1, final1, relay2, final2, relay3, final3, norm_own, norm_a, norm_b, norm_c, x_buf, dh_buf, z_buf, w_buf, out_buf, load_sem, part_send, part_recv, ring_sems, swap_sems, norm_sems, fetch_sems, out_sems):
    place = Place()
    units = unit_list()
    chunks = -(-len(units) // 3)
    counts = [len(range(order, len(units), 3)) for order in range(3)]
    wide_base = first_unit(1)
    wide_units = UNITS_OF[1]
    wide_half = wide_units * WIDTH
    pieces = WIDTH // BLOCK
    blocks = wide_units * BLOCKS_PER_UNIT
    partner = place.device(other_core=True)
    group_x = [(place.device({2: by}, other_core=swap)) for by in range(SIDE) for swap in (False, True) if by or swap]
    group_y = [place.device({1: by}) for by in range(1, SIDE)]
    group_z = [place.device({0: by}) for by in range(1, SIDE)]

    def block_start(block):
        unit = lax.div(block, BLOCKS_PER_UNIT)
        mine = lax.rem(lax.div(block, pieces), 2)
        owner = lax.rem(place.core + 1 + mine, 2)
        start = owner * wide_half + unit * WIDTH + lax.rem(block, pieces) * BLOCK
        return pl.multiple_of(start, BLOCK)

    def fetch(block):
        slot = lax.rem(block, 2)
        start = block_start(block)
        return (
            pltpu.make_async_copy(z_one.at[:, pl.ds(start, BLOCK)], z_buf.at[slot], fetch_sems.at[0, slot]),
            pltpu.make_async_copy(w_two.at[pl.ds(start, BLOCK), :], w_buf.at[slot], fetch_sems.at[1, slot]),
        )

    steady = (pltpu.make_async_copy(x_turned, x_buf, fetch_sems.at[2, 0]), pltpu.make_async_copy(dh_two, dh_buf, fetch_sems.at[2, 1]))
    for copy in steady + fetch(0):
        copy.start()
    enter(group_x + group_y + group_z)

    def source(mat, piece, core):
        if mat == 3:
            start = core * (UNITS_OF[mat] * WIDTH) + piece * WIDTH
            return g_three.at[:, :, :, :, pl.ds(pl.multiple_of(start, WIDTH), WIDTH)]
        ref = g_two if mat == 2 else g_four
        return ref.at[:, :, :, core, pl.ds(piece * ROWS, ROWS), :]

    rings = []
    for order in range(3):
        a, b = order, (order + 1) % 3
        c = (order + 2) % 3
        first = RingSum(place, [0, 1, 2], a, relay1, final1, ring_sems.at[0, 0], ring_sems.at[0, 1], ring_sems.at[0, 2])
        second = RingSum(place, first.rest, b, relay2, final2, ring_sems.at[1, 0], ring_sems.at[1, 1], ring_sems.at[1, 2])
        third = RingSum(place, second.rest, c, relay3, final3, ring_sems.at[2, 0], ring_sems.at[2, 1], ring_sems.at[2, 2])
        rings.append((first, second, third))

    def load(chunk):
        for order in range(3):
            unit = 3 * chunk + order
            if unit >= wide_base:
                continue
            mat, piece = units[unit]
            send(source(mat, piece, 1 - place.core), part.at[unit], part_send.at[unit], part_recv.at[unit], partner)
            pltpu.make_async_copy(source(mat, piece, place.core), own.at[order], load_sem.at[unit]).start()

    def wide_block(block, carry):
        slot = lax.rem(block, 2)

        @pl.when(block + 1 < blocks)
        def _():
            for copy in fetch(block + 1):
                copy.start()

        for copy in fetch(block):
            copy.wait()
        da_one = lax.dot_general(dh_buf[...], w_buf[slot], (((1,), (1,)), ((), ())), preferred_element_type=jnp.float32).astype(jnp.bfloat16)
        dz_one = (da_one.astype(jnp.float32) * gelu_slope(z_buf[slot])).astype(jnp.bfloat16)
        grad = jnp.dot(x_buf[...], dz_one, preferred_element_type=jnp.float32)
        grad = grad.reshape(SIDE, SIDE, SIDE, ROWS, BLOCK)
        unit = lax.div(block, BLOCKS_PER_UNIT)
        piece = lax.rem(block, pieces)
        mine = lax.rem(lax.div(block, pieces), 2)
        cols = pl.ds(pl.multiple_of(piece * BLOCK, BLOCK), BLOCK)

        @pl.when(mine == 1)
        def _():
            wide_own[unit, :, :, :, :, cols] = grad

        @pl.when(mine == 0)
        def _():
            @pl.when(unit > 0)
            def _():
                await_bytes(out_buf.at[piece], out_sems.at[piece])
            out_buf[piece] = grad
            send(out_buf.at[piece], part.at[wide_base + unit, :, :, :, :, cols], out_sems.at[piece], part_recv.at[wide_base + unit], partner)
        return carry

    def stage_b(order, chunk, unit):
        await_bytes(part.at[unit], part_recv.at[unit])

        @pl.when(unit < wide_base)
        def _():
            await_bytes(own.at[order], load_sem.at[unit])
            part[unit] = part[unit] + own[order]

        @pl.when(unit >= wide_base)
        def _():
            part[unit] = part[unit] + wide_own[unit - wide_base]
        rings[order][0].start(part, (unit,), unit)

    def stage_c(order, chunk, unit):
        rings[order][0].pass_on(part, (unit,), unit)

    def stage_d(order, chunk, unit):
        final1[unit, 0] = rings[order][0].finish(part, (unit,), unit)
        rings[order][1].start(final1, (unit, 0), unit)

    def stage_e(order, chunk, unit):
        rings[order][1].pass_on(final1, (unit, 0), unit)

    def stage_f(order, chunk, unit):
        final2[unit, 0] = rings[order][1].finish(final1, (unit, 0), unit)
        rings[order][2].start(final2, (unit, 0), unit)

    def stage_g(order, chunk, unit):
        rings[order][2].pass_on(final2, (unit, 0), unit)

    def stage_h(order, chunk, unit):
        shard[unit] = rings[order][2].finish(final2, (unit, 0), unit) * (1.0 / (2 * SIDE ** 3))

    stages = (stage_b, stage_c, stage_d, stage_e, stage_f, stage_g, stage_h)

    def run(now, lag):
        chunk = now - lag - 1
        for order in range(3):
            @pl.when((chunk >= 0) & (chunk < counts[order]))
            def _(order=order):
                stages[lag](order, chunk, 3 * chunk + order)

    load(0)
    for copy in steady:
        copy.wait()

    def turn(now, carry):
        run(now, 0)
        for chunk in range(1, chunks):
            if 3 * chunk < wide_base:
                @pl.when(now == chunk)
                def _(chunk=chunk):
                    load(chunk)
        low = lax.min(now * BLOCKS_PER_TURN, blocks)
        high = lax.min((now + 1) * BLOCKS_PER_TURN, blocks)
        lax.fori_loop(low, high, wide_block, 0)
        for lag in range(1, len(stages)):
            run(now, lag)
        return carry

    lax.fori_loop(0, chunks + len(stages), turn, 0)

    n_three = UNITS_OF[3]
    send(shard.at[pl.ds(0, n_three)], swapped.at[pl.ds(0, n_three)], swap_sems.at[0], swap_sems.at[1], partner)
    send(shard.at[pl.ds(wide_base, wide_units)], swapped.at[pl.ds(n_three, wide_units)], swap_sems.at[0], swap_sems.at[1], partner)

    def fold(unit, total):
        value = shard[unit]
        return total + value * value

    squares = lax.fori_loop(0, len(units), fold, jnp.zeros((ROWS, WIDTH), jnp.float32))
    total = squares[:, 0:128]
    for col in range(1, WIDTH // 128):
        total = total + squares[:, col * 128:(col + 1) * 128]
    levels = ((norm_a, group_x, place.coords[2] * 2 + place.core), (norm_b, group_y, place.coords[1]), (norm_c, group_z, place.coords[0]))
    for level, (board, group, seat) in enumerate(levels):
        norm_own[level] = total
        board[seat] = total
        for peer in group:
            send(norm_own.at[level], board.at[seat], norm_sems.at[0, level], norm_sems.at[1, level], peer)
        await_bytes(board.at[pl.ds(0, len(group))], norm_sems.at[1, level])
        total = board[0]
        for row in range(1, len(group) + 1):
            total = total + board[row]
    norm_tile[...] = total

    await_bytes(swapped, swap_sems.at[0])
    await_bytes(swapped, swap_sems.at[1])
    for level, (board, group, seat) in enumerate(levels):
        await_bytes(board.at[pl.ds(0, len(group))], norm_sems.at[0, level])
    for piece in range(pieces):
        await_bytes(out_buf.at[piece], out_sems.at[piece])
    for order in range(3):
        def tidy(chunk, carry, order=order):
            unit = 3 * chunk + order
            for ring in rings[order]:
                ring.drain(unit)

            @pl.when(unit < wide_base)
            def _():
                await_bytes(part.at[unit], part_send.at[unit])
            return carry

        lax.fori_loop(0, counts[order], tidy, 0)


def reduce_grads(wide_parts, g_two, g_three, g_four):
    n = len(unit_list())
    cube = (SIDE, SIDE, SIDE)
    args = tuple(wide_parts) + (
        g_two.reshape(cube + (2, UNITS_OF[2] * ROWS, WIDTH)),
        g_three.reshape(cube + (ROWS, 2 * UNITS_OF[3] * WIDTH)),
        g_four.reshape(cube + (2, UNITS_OF[4] * ROWS, WIDTH)),
    )
    f32, bf16 = jnp.float32, jnp.bfloat16
    dma = pltpu.SemaphoreType.DMA
    dim, rows = wide_parts[0].shape
    model = wide_parts[1].shape[1]
    scratch = [
        pltpu.VMEM((3,) + cube + (ROWS, WIDTH), f32),
        pltpu.VMEM((UNITS_OF[1],) + cube + (ROWS, WIDTH), f32),
        pltpu.VMEM((n,) + cube + (ROWS, WIDTH), f32),
        pltpu.VMEM((n, 2, SIDE, SIDE, ROWS, WIDTH // 2), f32),
        pltpu.VMEM((n, 2, SIDE, SIDE, ROWS, WIDTH), f32),
        pltpu.VMEM((n, 2, SIDE, ROWS, WIDTH // 2), f32),
        pltpu.VMEM((n, 2, SIDE, ROWS, WIDTH), f32),
        pltpu.VMEM((n, 2, ROWS, WIDTH // 2), f32),
        pltpu.VMEM((n, 2, ROWS, WIDTH), f32),
        pltpu.VMEM((3, ROWS, 128), f32),
        pltpu.VMEM((2 * SIDE, ROWS, 128), f32),
        pltpu.VMEM((SIDE, ROWS, 128), f32),
        pltpu.VMEM((SIDE, ROWS, 128), f32),
        pltpu.VMEM((dim, rows), bf16),
        pltpu.VMEM((rows, model), bf16),
        pltpu.VMEM((2, rows, BLOCK), bf16),
        pltpu.VMEM((2, BLOCK, model), bf16),
        pltpu.VMEM((WIDTH // BLOCK,) + cube + (ROWS, BLOCK), f32),
        dma((n,)), dma((n,)), dma((n,)), dma((3, 3, n)), dma((2,)), dma((2, 3)), dma((3, 2)), dma((WIDTH // BLOCK,)),
    ]
    any_spec = pl.BlockSpec(memory_space=pl.ANY)
    vmem_spec = pl.BlockSpec(memory_space=pltpu.VMEM)
    return pl.pallas_call(
        reduce_kernel,
        out_shape=(
            jax.ShapeDtypeStruct((n, ROWS, WIDTH), f32),
            jax.ShapeDtypeStruct((UNITS_OF[3] + UNITS_OF[1], ROWS, WIDTH), f32),
            jax.ShapeDtypeStruct((ROWS, 128), f32),
        ),
        in_specs=[any_spec] * len(args),
        out_specs=(vmem_spec,) * 3,
        scratch_shapes=scratch,
        compiler_params=pltpu.CompilerParams(collective_id=0, has_side_effects=True, vmem_limit_bytes=VMEM_BYTES),
        name='reduce_grads',
    )(*args)


def adam_kernel(lr_ref, clip_ref, norm_tile, shard, swapped, *refs):
    masters, moms, variances = refs[0:4], refs[4:8], refs[8:12]
    new_masters, new_moms, new_vars = refs[12:16], refs[16:20], refs[20:24]
    two_rows, four_rows, norm_ref = refs[24:27]
    core = lax.rem(lax.axis_index('dp'), 2)
    grad_norm = jnp.sqrt(jnp.sum(jnp.sum(norm_tile[...], axis=1, keepdims=True), axis=0, keepdims=True))
    norm_ref[...] = grad_norm
    clip_scale = jnp.minimum(1.0, clip_ref[...] / (grad_norm + NORM_EPS))
    learn_rate = lr_ref[...]

    def update(mat, where, grad):
        scaled = clip_scale * grad
        mom_new = BETA_ONE * moms[mat][where] + (1.0 - BETA_ONE) * scaled
        var_new = BETA_TWO * variances[mat][where] + (1.0 - BETA_TWO) * scaled * scaled
        master_new = masters[mat][where] - learn_rate * (mom_new / BIAS_ONE) / (jnp.sqrt(var_new / BIAS_TWO) + ADAM_EPS)
        new_moms[mat][where] = mom_new
        new_vars[mat][where] = var_new
        new_masters[mat][where] = master_new
        return master_new

    for mat, rows_out in ((2, two_rows), (4, four_rows)):
        for piece in range(UNITS_OF[mat]):
            where = (slice(piece * ROWS, (piece + 1) * ROWS), slice(None))
            rows_out[piece] = update(mat - 1, where, shard[first_unit(mat) + piece]).astype(jnp.bfloat16)
    for mat, base in ((3, 0), (1, UNITS_OF[3])):
        for half in range(2):
            for piece in range(UNITS_OF[mat]):
                col = (half * UNITS_OF[mat] + piece) * WIDTH
                where = (slice(None), slice(col, col + WIDTH))
                block = jnp.where(core == half, shard[first_unit(mat) + piece], swapped[base + piece])
                update(mat - 1, where, jnp.where(core == 0, block[0:ROWS // 2], block[ROWS // 2:ROWS]))


def adam_update(learn_rate, clip_max, norm_tile, shard, swapped, masters, moms, variances):
    state = list(masters) + list(moms) + list(variances)
    f32, bf16 = jnp.float32, jnp.bfloat16
    vmem_spec = pl.BlockSpec(memory_space=pltpu.VMEM)
    out_shape = [jax.ShapeDtypeStruct(part.shape, f32) for part in state]
    out_shape += [
        jax.ShapeDtypeStruct((UNITS_OF[2], ROWS, WIDTH), bf16),
        jax.ShapeDtypeStruct((UNITS_OF[4], ROWS, WIDTH), bf16),
        jax.ShapeDtypeStruct((1, 1), f32),
    ]
    args = [learn_rate.reshape(1, 1), clip_max.reshape(1, 1), norm_tile, shard, swapped] + state
    return pl.pallas_call(
        adam_kernel,
        out_shape=out_shape,
        in_specs=[vmem_spec] * len(args),
        out_specs=[vmem_spec] * len(out_shape),
        name='adam_update',
    )(*args)


class RingSpread:
    def __init__(self, place, axis, known, board, near_sem, far_sem, send_sem):
        self.place, self.axis, self.known, self.board = place, axis, known, board
        self.near_sem, self.far_sem, self.send_sem = near_sem, far_sem, send_sem
        self.up_dev, self.down_dev = place.device({axis: 1}), place.device({axis: SIDE - 1})

    def block(self, unit, by, cols):
        fixed = {dim: self.place.coords[dim] for dim in range(3) if dim not in self.known}
        fixed[self.axis] = self.place.step(self.axis, by)
        return self.board.at[spot((unit,), [0, 1, 2], fixed, cols)]

    def blocks(self, unit, count):
        return self.board.at[(unit,) + (0,) * (2 - len(self.known)) + (pl.ds(0, count),)]

    def start(self, unit):
        s = self
        mine = s.block(unit, 0, ALL)
        send(mine, mine, s.send_sem.at[unit], s.near_sem.at[unit], s.up_dev)
        send(mine, mine, s.send_sem.at[unit], s.near_sem.at[unit], s.down_dev)

    def pass_on(self, unit):
        s = self
        await_bytes(s.blocks(unit, 2), s.near_sem.at[unit])
        from_down, from_up = s.block(unit, SIDE - 1, LEFT), s.block(unit, 1, RIGHT)
        send(from_down, from_down, s.send_sem.at[unit], s.far_sem.at[unit], s.up_dev)
        send(from_up, from_up, s.send_sem.at[unit], s.far_sem.at[unit], s.down_dev)

    def finish(self, unit):
        await_bytes(self.block(unit, 0, ALL), self.far_sem.at[unit])

    def drain(self, unit):
        await_bytes(self.blocks(unit, 3), self.send_sem.at[unit])


def gather_kernel(one_rows, three_rows, two_rows, four_rows, board, other, swap_one, swap_three, ring_sems, pair_sems, swap_sems):
    place = Place()
    units = unit_list()
    chunks = -(-len(units) // 3)
    counts = [len(range(order, len(units), 3)) for order in range(3)]
    partner = place.device(other_core=True)
    here = tuple(place.coords)
    enter(place.neighbours())
    splits = ((1, one_rows, swap_one), (3, three_rows, swap_three))
    for index, (mat, rows, landing) in enumerate(splits):
        span = UNITS_OF[mat] * WIDTH
        theirs = rows.at[:, pl.ds(pl.multiple_of((1 - place.core) * span, WIDTH), span)]
        send(theirs, landing, swap_sems.at[0, index], swap_sems.at[1, index], partner)
    for mat, rows in ((2, two_rows), (4, four_rows)):
        for piece in range(UNITS_OF[mat]):
            board[(first_unit(mat) + piece,) + here] = rows[piece]
    for index, (mat, rows, landing) in enumerate(splits):
        await_bytes(landing, swap_sems.at[1, index])
        for piece in range(UNITS_OF[mat]):
            start = place.core * (UNITS_OF[mat] * WIDTH) + piece * WIDTH
            mine = rows[:, pl.ds(pl.multiple_of(start, WIDTH), WIDTH)]
            theirs = landing[:, piece * WIDTH:(piece + 1) * WIDTH]
            top = jnp.where(place.core == 0, mine, theirs)
            bottom = jnp.where(place.core == 0, theirs, mine)
            board[(first_unit(mat) + piece,) + here] = jnp.concatenate([top, bottom], axis=0).astype(board.dtype)

    rings = []
    for order in range(3):
        axes = (order + 2) % 3, (order + 1) % 3, order
        rings.append([RingSpread(place, axis, axes[:level], board, ring_sems.at[level, 0], ring_sems.at[level, 1], ring_sems.at[level, 2]) for level, axis in enumerate(axes)])

    def every(action):
        def turn(chunk, carry):
            for order in range(3):
                @pl.when(chunk < counts[order])
                def _(order=order):
                    action(order, 3 * chunk + order)
            return carry

        lax.fori_loop(0, chunks, turn, 0)

    def begin(order, unit):
        rings[order][0].start(unit)

    every(begin)
    for level in range(3):
        def pass_on(order, unit, level=level):
            rings[order][level].pass_on(unit)

        def onward(order, unit, level=level):
            rings[order][level].finish(unit)
            if level < 2:
                rings[order][level + 1].start(unit)
            else:
                send(board.at[unit], other.at[unit], pair_sems.at[0, unit], pair_sems.at[1, unit], partner)

        every(pass_on)
        every(onward)

    def tidy(order, unit):
        await_bytes(other.at[unit], pair_sems.at[1, unit])
        await_bytes(board.at[unit], pair_sems.at[0, unit])
        for level in range(3):
            rings[order][level].drain(unit)

    every(tidy)
    for index, (mat, rows, landing) in enumerate(splits):
        await_bytes(landing, swap_sems.at[0, index])


def gather_rows(one_rows, three_rows, two_rows, four_rows):
    n = len(unit_list())
    cube = (SIDE, SIDE, SIDE)
    bf16, f32 = jnp.bfloat16, jnp.float32
    dma = pltpu.SemaphoreType.DMA
    vmem_spec = pl.BlockSpec(memory_space=pltpu.VMEM)
    full = jax.ShapeDtypeStruct((n,) + cube + (ROWS, WIDTH), bf16)
    return pl.pallas_call(
        gather_kernel,
        out_shape=(full, full),
        in_specs=[vmem_spec] * 4,
        out_specs=(vmem_spec, vmem_spec),
        scratch_shapes=[
            pltpu.VMEM((ROWS // 2, UNITS_OF[1] * WIDTH), f32),
            pltpu.VMEM((ROWS // 2, UNITS_OF[3] * WIDTH), f32),
            dma((3, 3, n)), dma((2, n)), dma((2, 2)),
        ],
        compiler_params=pltpu.CompilerParams(collective_id=1, has_side_effects=True, vmem_limit_bytes=32 * 1024 * 1024),
        name='gather_rows',
    )(one_rows, three_rows, two_rows, four_rows)


def place_kernel(board, other, w_one, w_two, w_three, w_four, sems):
    core = lax.rem(lax.axis_index('dp'), 2)
    outs = {1: w_one, 2: w_two, 3: w_three, 4: w_four}
    copies = []
    for unit, (mat, piece) in enumerate(unit_list()):
        for index, (source, owner) in enumerate(((board, core), (other, 1 - core))):
            if mat in (1, 3):
                start = owner * (UNITS_OF[mat] * WIDTH) + piece * WIDTH
                target = outs[mat].at[:, :, :, :, pl.ds(pl.multiple_of(start, WIDTH), WIDTH)]
            else:
                target = outs[mat].at[:, :, :, owner, pl.ds(piece * ROWS, ROWS), :]
            copies.append(pltpu.make_async_copy(source.at[unit], target, sems.at[index, unit]))
    for copy in copies:
        copy.start()
    for copy in copies:
        copy.wait()


def place_weights(board, other):
    n = len(unit_list())
    cube = (SIDE, SIDE, SIDE)
    bf16 = jnp.bfloat16
    vmem_spec = pl.BlockSpec(memory_space=pltpu.VMEM)
    any_spec = pl.BlockSpec(memory_space=pl.ANY)
    outs = pl.pallas_call(
        place_kernel,
        out_shape=(
            jax.ShapeDtypeStruct(cube + (ROWS, 2 * UNITS_OF[1] * WIDTH), bf16),
            jax.ShapeDtypeStruct(cube + (2, UNITS_OF[2] * ROWS, WIDTH), bf16),
            jax.ShapeDtypeStruct(cube + (ROWS, 2 * UNITS_OF[3] * WIDTH), bf16),
            jax.ShapeDtypeStruct(cube + (2, UNITS_OF[4] * ROWS, WIDTH), bf16),
        ),
        in_specs=[vmem_spec] * 2,
        out_specs=(any_spec,) * 4,
        scratch_shapes=[pltpu.SemaphoreType.DMA((2, n))],
        compiler_params=pltpu.CompilerParams(vmem_limit_bytes=2 * 1024 * 1024),
        name='place_weights',
    )(board, other)
    rows = SIDE ** 3 * ROWS
    return (
        outs[0].reshape(rows, 2 * UNITS_OF[1] * WIDTH),
        outs[1].reshape(2 * SIDE ** 3 * UNITS_OF[2] * ROWS, WIDTH),
        outs[2].reshape(rows, 2 * UNITS_OF[3] * WIDTH),
        outs[3].reshape(2 * SIDE ** 3 * UNITS_OF[4] * ROWS, WIDTH),
    )


def sync_and_update(grads, masters, moms, variances, learn_rate, clip_max):
    shard, swapped, norm_tile = reduce_grads(*grads)
    results = adam_update(learn_rate, clip_max, norm_tile, shard, swapped, masters, moms, variances)
    new_masters, new_moms, new_vars = results[0:4], results[4:8], results[8:12]
    two_rows, four_rows, grad_norm = results[12:15]
    board, other = gather_rows(new_masters[0], new_masters[2], two_rows, four_rows)
    new_weights = place_weights(board, other)
    return tuple(new_weights) + tuple(new_masters) + tuple(new_moms) + tuple(new_vars) + (grad_norm.reshape(()),)


def solution(mesh):
    row_spec = P('dp', None)
    rep_spec = P()

    def per_device(x_rows, dy_rows, w_one, w_two, w_three, w_four, master_one, master_two, master_three, master_four, m_one, m_two, m_three, m_four, v_one, v_two, v_three, v_four, learn_rate, clip_max):
        grads = local_grads(x_rows, dy_rows, w_one, w_two, w_three, w_four)
        return sync_and_update(grads, (master_one, master_two, master_three, master_four), (m_one, m_two, m_three, m_four), (v_one, v_two, v_three, v_four), learn_rate, clip_max)

    in_specs = (row_spec, row_spec) + (rep_spec,) * 4 + (row_spec,) * 12 + (rep_spec, rep_spec)
    out_specs = (rep_spec,) * 4 + (row_spec,) * 12 + (rep_spec,)
    return jax.shard_map(per_device, mesh=mesh, in_specs=in_specs, out_specs=out_specs, check_vma=False)
```

```python
import functools

import jax
import jax.numpy as jnp
from jax import lax
from jax.experimental import pallas as pl
from jax.experimental.pallas import tpu as pltpu
from jax.sharding import PartitionSpec as P

ADAM_STEP = 10
BETA_ONE = 0.9
BETA_TWO = 0.95
ADAM_EPS = 1e-8
NORM_EPS = 1e-6
BIAS_ONE = 1.0 - BETA_ONE ** ADAM_STEP
BIAS_TWO = 1.0 - BETA_TWO ** ADAM_STEP
INV_SQRT2 = 0.7071067811865476
INV_SQRT2PI = 0.3989422804014327

WIDTH = 512
SIDE = 4
ROWS = 8
UNITS_OF = {3: 2, 4: 2, 2: 8, 1: 8}
MESH_ID = pl.DeviceIdType.MESH
VMEM_BYTES = 62 * 1024 * 1024


def unit_list():
    return [(mat, piece) for mat in (3, 4, 2, 1) for piece in range(UNITS_OF[mat])]


def first_unit(mat):
    return unit_list().index((mat, 0))


def gelu_value(pre_act):
    pre_wide = pre_act.astype(jnp.float32)
    return 0.5 * pre_wide * (1.0 + lax.erf(pre_wide * INV_SQRT2))


def gelu_slope(pre_act):
    pre_wide = pre_act.astype(jnp.float32)
    return 0.5 * (1.0 + lax.erf(pre_wide * INV_SQRT2)) + pre_wide * INV_SQRT2PI * jnp.exp(-0.5 * pre_wide * pre_wide)


def forward_kernel(x_ref, w_one, w_two, z_out, a_out, h_out, x_turned, total):
    step = pl.program_id(0)

    @pl.when(step == 0)
    def _():
        total[...] = jnp.zeros_like(total)
        x_turned[...] = x_ref[...].T

    z_one = jnp.dot(x_ref[...], w_one[...], preferred_element_type=jnp.float32).astype(jnp.bfloat16)
    z_out[...] = z_one
    a_one = gelu_value(z_one).astype(jnp.bfloat16)
    a_out[...] = a_one
    total[...] += jnp.dot(a_one, w_two[...], preferred_element_type=jnp.float32)

    @pl.when(step == pl.num_programs(0) - 1)
    def _():
        h_out[...] = total[...].astype(jnp.bfloat16)


def forward_wide(x_rows, w_one, w_two):
    rows, dim = x_rows.shape
    wide = w_one.shape[1]
    block = 512
    bf16 = jnp.bfloat16
    return pl.pallas_call(
        forward_kernel,
        grid=(wide // block,),
        out_shape=(jax.ShapeDtypeStruct((rows, wide), bf16), jax.ShapeDtypeStruct((rows, wide), bf16), jax.ShapeDtypeStruct((rows, dim), bf16), jax.ShapeDtypeStruct((dim, rows), bf16)),
        in_specs=[pl.BlockSpec((rows, dim), lambda i: (0, 0)), pl.BlockSpec((dim, block), lambda i: (0, i)), pl.BlockSpec((block, dim), lambda i: (i, 0))],
        out_specs=(pl.BlockSpec((rows, block), lambda i: (0, i)), pl.BlockSpec((rows, block), lambda i: (0, i)), pl.BlockSpec((rows, dim), lambda i: (0, 0)), pl.BlockSpec((dim, rows), lambda i: (0, 0))),
        scratch_shapes=[pltpu.VMEM((rows, dim), jnp.float32)],
        compiler_params=pltpu.CompilerParams(vmem_limit_bytes=VMEM_BYTES),
        name='forward_wide',
    )(x_rows, w_one, w_two)


def middle_kernel(h_ref, dy_ref, w_three, w_four, g_three, g_four, dh_out, total, h_turned):
    step = pl.program_id(0)
    f32, bf16 = jnp.float32, jnp.bfloat16

    @pl.when(step == 0)
    def _():
        total[...] = jnp.zeros_like(total)
        h_turned[...] = h_ref[...].T

    z_three = jnp.dot(h_ref[...], w_three[...], preferred_element_type=f32).astype(bf16)
    a_three = gelu_value(z_three).astype(bf16)
    da_three = lax.dot_general(dy_ref[...], w_four[...], (((1,), (1,)), ((), ())), preferred_element_type=f32).astype(bf16)
    dz_three = (da_three.astype(f32) * gelu_slope(z_three)).astype(bf16)
    g_four[...] = lax.dot_general(a_three, dy_ref[...], (((0,), (0,)), ((), ())), preferred_element_type=f32)
    g_three[...] = jnp.dot(h_turned[...], dz_three, preferred_element_type=f32)
    total[...] += lax.dot_general(dz_three, w_three[...], (((1,), (1,)), ((), ())), preferred_element_type=f32)

    @pl.when(step == pl.num_programs(0) - 1)
    def _():
        dh_out[...] = total[...].astype(bf16)


def middle(h_two, dy_rows, w_three, w_four):
    rows, dim = h_two.shape
    wide = w_three.shape[1]
    block = 512
    f32, bf16 = jnp.float32, jnp.bfloat16
    whole = pl.BlockSpec((rows, dim), lambda i: (0, 0))
    across, down = pl.BlockSpec((dim, block), lambda i: (0, i)), pl.BlockSpec((block, dim), lambda i: (i, 0))
    return pl.pallas_call(
        middle_kernel,
        grid=(wide // block,),
        out_shape=(jax.ShapeDtypeStruct((dim, wide), f32), jax.ShapeDtypeStruct((wide, dim), f32), jax.ShapeDtypeStruct((rows, dim), bf16)),
        in_specs=[whole, whole, across, down],
        out_specs=(across, down, whole),
        scratch_shapes=[pltpu.VMEM((rows, dim), f32), pltpu.VMEM((dim, rows), bf16)],
        compiler_params=pltpu.CompilerParams(vmem_limit_bytes=VMEM_BYTES),
        name='middle',
    )(h_two, dy_rows, w_three, w_four)


def local_grads(x_rows, dy_rows, w_one, w_two, w_three, w_four):
    z_one, a_one, h_two, x_turned = forward_wide(x_rows, w_one, w_two)
    g_three, g_four, dh_two = middle(h_two, dy_rows, w_three, w_four)
    g_two = jnp.einsum('rw,rd->wd', a_one, dh_two, preferred_element_type=jnp.float32)
    return (x_turned, dh_two, z_one, w_two), g_two, g_three, g_four


class Place:
    def __init__(self):
        me = lax.axis_index('dp')
        self.core = lax.rem(me, 2)
        self.coords = [lax.div(me, 2 * SIDE * SIDE), lax.rem(lax.div(me, 2 * SIDE), SIDE), lax.rem(lax.div(me, 2), SIDE)]

    def step(self, axis, by):
        return lax.rem(self.coords[axis] + by, SIDE)

    def device(self, moves=None, other_core=False):
        pos = list(self.coords)
        for axis, by in (moves or {}).items():
            pos[axis] = self.step(axis, by)
        core = 1 - self.core if other_core else self.core
        return (((pos[0] * SIDE + pos[1]) * SIDE + pos[2]) * 2 + core,)

    def neighbours(self):
        found = [self.device(other_core=True)]
        for axis in range(3):
            found += [self.device({axis: 1}), self.device({axis: SIDE - 1})]
        return found


def enter(peers):
    barrier = pltpu.get_barrier_semaphore()
    for peer in peers:
        pl.semaphore_signal(barrier, inc=1, device_id=peer, device_id_type=MESH_ID)
    pl.semaphore_wait(barrier, len(peers))


def send(src, dst, send_sem, recv_sem, peer):
    pltpu.make_async_remote_copy(src_ref=src, dst_ref=dst, send_sem=send_sem, recv_sem=recv_sem, device_id=peer, device_id_type=MESH_ID).start()


def await_bytes(ref, sem):
    pltpu.make_async_copy(ref, ref, sem).wait()


def spot(lead, dims, fixed, cols):
    return tuple(lead) + tuple(fixed.get(axis, slice(None)) for axis in dims) + (slice(None), cols)


LEFT = pl.ds(0, WIDTH // 2)
RIGHT = pl.ds(WIDTH // 2, WIDTH // 2)
ALL = slice(None)


class RingSum:
    def __init__(self, place, dims, axis, relay, final, relay_sem, final_sem, send_sem):
        self.place, self.dims, self.axis = place, dims, axis
        self.relay, self.final = relay, final
        self.relay_sem, self.final_sem, self.send_sem = relay_sem, final_sem, send_sem
        self.own = place.coords[axis]
        self.up, self.down, self.far = place.step(axis, 1), place.step(axis, SIDE - 1), place.step(axis, 2)
        self.up_dev, self.down_dev = place.device({axis: 1}), place.device({axis: SIDE - 1})
        self.rest = [dim for dim in dims if dim != axis]

    def start(self, src, lead, unit):
        s = self
        send(src.at[spot(lead, s.dims, {s.axis: s.far}, LEFT)], s.relay.at[unit, 0], s.send_sem.at[unit], s.relay_sem.at[unit], s.up_dev)
        send(src.at[spot(lead, s.dims, {s.axis: s.far}, RIGHT)], s.relay.at[unit, 1], s.send_sem.at[unit], s.relay_sem.at[unit], s.down_dev)
        send(src.at[spot(lead, s.dims, {s.axis: s.up}, RIGHT)], s.final.at[spot((unit, 0), s.rest, {}, RIGHT)], s.send_sem.at[unit], s.final_sem.at[unit], s.up_dev)
        send(src.at[spot(lead, s.dims, {s.axis: s.down}, LEFT)], s.final.at[spot((unit, 1), s.rest, {}, LEFT)], s.send_sem.at[unit], s.final_sem.at[unit], s.down_dev)

    def pass_on(self, src, lead, unit):
        s = self
        await_bytes(s.relay.at[unit], s.relay_sem.at[unit])
        up_spot = spot(lead, s.dims, {s.axis: s.up}, LEFT)
        src[up_spot] = src[up_spot] + s.relay[unit, 0]
        send(src.at[up_spot], s.final.at[spot((unit, 0), s.rest, {}, LEFT)], s.send_sem.at[unit], s.final_sem.at[unit], s.up_dev)
        down_spot = spot(lead, s.dims, {s.axis: s.down}, RIGHT)
        src[down_spot] = src[down_spot] + s.relay[unit, 1]
        send(src.at[down_spot], s.final.at[spot((unit, 1), s.rest, {}, RIGHT)], s.send_sem.at[unit], s.final_sem.at[unit], s.down_dev)

    def finish(self, src, lead, unit):
        s = self
        await_bytes(s.final.at[unit], s.final_sem.at[unit])
        return src[spot(lead, s.dims, {s.axis: s.own}, ALL)] + s.final[unit, 0] + s.final[unit, 1]

    def drain(self, unit):
        await_bytes(self.relay.at[unit], self.send_sem.at[unit])
        await_bytes(self.final.at[unit], self.send_sem.at[unit])


BLOCK = 256
BLOCKS_PER_UNIT = 2 * (WIDTH // BLOCK)
BLOCKS_AFTER = (2, 2, 1)


def reduce_kernel(x_turned, dh_two, z_one, w_two, g_two, g_three, g_four, shard, swapped, norm_tile, own, wide_own, part, relay1, final1, relay2, final2, relay3, final3, norm_own, norm_a, norm_b, norm_c, x_buf, dh_buf, z_buf, w_buf, out_buf, load_sem, part_send, part_recv, ring_sems, swap_sems, norm_sems, fetch_sems, out_sems):
    place = Place()
    units = unit_list()
    chunks = -(-len(units) // 3)
    counts = [len(range(order, len(units), 3)) for order in range(3)]
    wide_base = first_unit(1)
    wide_units = UNITS_OF[1]
    wide_half = wide_units * WIDTH
    pieces = WIDTH // BLOCK
    blocks = wide_units * BLOCKS_PER_UNIT
    partner = place.device(other_core=True)
    group_x = [(place.device({2: by}, other_core=swap)) for by in range(SIDE) for swap in (False, True) if by or swap]
    group_y = [place.device({1: by}) for by in range(1, SIDE)]
    group_z = [place.device({0: by}) for by in range(1, SIDE)]

    def block_start(block):
        unit = lax.div(block, BLOCKS_PER_UNIT)
        mine = lax.rem(lax.div(block, pieces), 2)
        owner = lax.rem(place.core + 1 + mine, 2)
        start = owner * wide_half + unit * WIDTH + lax.rem(block, pieces) * BLOCK
        return pl.multiple_of(start, BLOCK)

    def fetch(block):
        slot = lax.rem(block, 2)
        start = block_start(block)
        return (
            pltpu.make_async_copy(z_one.at[:, pl.ds(start, BLOCK)], z_buf.at[slot], fetch_sems.at[0, slot]),
            pltpu.make_async_copy(w_two.at[pl.ds(start, BLOCK), :], w_buf.at[slot], fetch_sems.at[1, slot]),
        )

    steady = (pltpu.make_async_copy(x_turned, x_buf, fetch_sems.at[2, 0]), pltpu.make_async_copy(dh_two, dh_buf, fetch_sems.at[2, 1]))
    for copy in steady + fetch(0):
        copy.start()
    enter(group_x + group_y + group_z)

    def source(mat, piece, core):
        if mat == 3:
            start = core * (UNITS_OF[mat] * WIDTH) + piece * WIDTH
            return g_three.at[:, :, :, :, pl.ds(pl.multiple_of(start, WIDTH), WIDTH)]
        ref = g_two if mat == 2 else g_four
        return ref.at[:, :, :, core, pl.ds(piece * ROWS, ROWS), :]

    rings = []
    for order in range(3):
        a, b = order, (order + 1) % 3
        c = (order + 2) % 3
        first = RingSum(place, [0, 1, 2], a, relay1, final1, ring_sems.at[0, 0], ring_sems.at[0, 1], ring_sems.at[0, 2])
        second = RingSum(place, first.rest, b, relay2, final2, ring_sems.at[1, 0], ring_sems.at[1, 1], ring_sems.at[1, 2])
        third = RingSum(place, second.rest, c, relay3, final3, ring_sems.at[2, 0], ring_sems.at[2, 1], ring_sems.at[2, 2])
        rings.append((first, second, third))

    def load(chunk):
        for order in range(3):
            unit = 3 * chunk + order
            if unit >= wide_base:
                continue
            mat, piece = units[unit]
            send(source(mat, piece, 1 - place.core), part.at[unit], part_send.at[unit], part_recv.at[unit], partner)
            pltpu.make_async_copy(source(mat, piece, place.core), own.at[order], load_sem.at[unit]).start()

    def wide_block(block, carry):
        slot = lax.rem(block, 2)

        @pl.when(block + 1 < blocks)
        def _():
            for copy in fetch(block + 1):
                copy.start()

        for copy in fetch(block):
            copy.wait()
        da_one = lax.dot_general(dh_buf[...], w_buf[slot], (((1,), (1,)), ((), ())), preferred_element_type=jnp.float32).astype(jnp.bfloat16)
        dz_one = (da_one.astype(jnp.float32) * gelu_slope(z_buf[slot])).astype(jnp.bfloat16)
        grad = jnp.dot(x_buf[...], dz_one, preferred_element_type=jnp.float32)
        grad = grad.reshape(SIDE, SIDE, SIDE, ROWS, BLOCK)
        unit = lax.div(block, BLOCKS_PER_UNIT)
        piece = lax.rem(block, pieces)
        mine = lax.rem(lax.div(block, pieces), 2)
        cols = pl.ds(pl.multiple_of(piece * BLOCK, BLOCK), BLOCK)

        @pl.when(mine == 1)
        def _():
            wide_own[unit, :, :, :, :, cols] = grad

        @pl.when(mine == 0)
        def _():
            @pl.when(unit > 0)
            def _():
                await_bytes(out_buf.at[piece], out_sems.at[piece])
            out_buf[piece] = grad
            send(out_buf.at[piece], part.at[wide_base + unit, :, :, :, :, cols], out_sems.at[piece], part_recv.at[wide_base + unit], partner)
        return carry

    def stage_b(order, chunk, unit):
        await_bytes(part.at[unit], part_recv.at[unit])

        @pl.when(unit < wide_base)
        def _():
            await_bytes(own.at[order], load_sem.at[unit])
            part[unit] = part[unit] + own[order]

        @pl.when(unit >= wide_base)
        def _():
            part[unit] = part[unit] + wide_own[unit - wide_base]
        rings[order][0].start(part, (unit,), unit)

    def stage_c(order, chunk, unit):
        rings[order][0].pass_on(part, (unit,), unit)

    def stage_d(order, chunk, unit):
        final1[unit, 0] = rings[order][0].finish(part, (unit,), unit)
        rings[order][1].start(final1, (unit, 0), unit)

    def stage_e(order, chunk, unit):
        rings[order][1].pass_on(final1, (unit, 0), unit)

    def stage_f(order, chunk, unit):
        final2[unit, 0] = rings[order][1].finish(final1, (unit, 0), unit)
        rings[order][2].start(final2, (unit, 0), unit)

    def stage_g(order, chunk, unit):
        rings[order][2].pass_on(final2, (unit, 0), unit)

    def stage_h(order, chunk, unit):
        shard[unit] = rings[order][2].finish(final2, (unit, 0), unit) * (1.0 / (2 * SIDE ** 3))

    stages = (stage_b, stage_c, stage_d, stage_e, stage_f, stage_g, stage_h)

    def run(now, lag):
        chunk = now - lag - 1
        for order in range(3):
            @pl.when((chunk >= 0) & (chunk < counts[order]))
            def _(order=order):
                stages[lag](order, chunk, 3 * chunk + order)

    def wide_blocks(low, count):
        lax.fori_loop(lax.min(low, blocks), lax.min(low + count, blocks), wide_block, 0)

    load(0)
    for copy in steady:
        copy.wait()
    first_blocks = 6
    wide_blocks(0, first_blocks)

    def turn(now, carry):
        run(now, 0)
        for chunk in range(1, chunks):
            if 3 * chunk < wide_base:
                @pl.when(now == chunk)
                def _(chunk=chunk):
                    load(chunk)
        done = first_blocks + (now - 1) * sum(BLOCKS_AFTER)
        for lag in range(1, len(stages)):
            if lag <= len(BLOCKS_AFTER):
                wide_blocks(done, BLOCKS_AFTER[lag - 1])
                done = done + BLOCKS_AFTER[lag - 1]
            run(now, lag)
        return carry

    lax.fori_loop(1, chunks + len(stages), turn, 0)

    n_three = UNITS_OF[3]
    send(shard.at[pl.ds(0, n_three)], swapped.at[pl.ds(0, n_three)], swap_sems.at[0], swap_sems.at[1], partner)
    send(shard.at[pl.ds(wide_base, wide_units)], swapped.at[pl.ds(n_three, wide_units)], swap_sems.at[0], swap_sems.at[1], partner)

    def fold(unit, total):
        value = shard[unit]
        return total + value * value

    squares = lax.fori_loop(0, len(units), fold, jnp.zeros((ROWS, WIDTH), jnp.float32))
    total = squares[:, 0:128]
    for col in range(1, WIDTH // 128):
        total = total + squares[:, col * 128:(col + 1) * 128]
    levels = ((norm_a, group_x, place.coords[2] * 2 + place.core), (norm_b, group_y, place.coords[1]), (norm_c, group_z, place.coords[0]))
    for level, (board, group, seat) in enumerate(levels):
        norm_own[level] = total
        board[seat] = total
        for peer in group:
            send(norm_own.at[level], board.at[seat], norm_sems.at[0, level], norm_sems.at[1, level], peer)
        await_bytes(board.at[pl.ds(0, len(group))], norm_sems.at[1, level])
        total = board[0]
        for row in range(1, len(group) + 1):
            total = total + board[row]
    norm_tile[...] = total

    await_bytes(swapped, swap_sems.at[0])
    await_bytes(swapped, swap_sems.at[1])
    for level, (board, group, seat) in enumerate(levels):
        await_bytes(board.at[pl.ds(0, len(group))], norm_sems.at[0, level])
    for piece in range(pieces):
        await_bytes(out_buf.at[piece], out_sems.at[piece])
    for order in range(3):
        def tidy(chunk, carry, order=order):
            unit = 3 * chunk + order
            for ring in rings[order]:
                ring.drain(unit)

            @pl.when(unit < wide_base)
            def _():
                await_bytes(part.at[unit], part_send.at[unit])
            return carry

        lax.fori_loop(0, counts[order], tidy, 0)


def reduce_grads(wide_parts, g_two, g_three, g_four):
    n = len(unit_list())
    cube = (SIDE, SIDE, SIDE)
    args = tuple(wide_parts) + (
        g_two.reshape(cube + (2, UNITS_OF[2] * ROWS, WIDTH)),
        g_three.reshape(cube + (ROWS, 2 * UNITS_OF[3] * WIDTH)),
        g_four.reshape(cube + (2, UNITS_OF[4] * ROWS, WIDTH)),
    )
    f32, bf16 = jnp.float32, jnp.bfloat16
    dma = pltpu.SemaphoreType.DMA
    dim, rows = wide_parts[0].shape
    model = wide_parts[1].shape[1]
    scratch = [
        pltpu.VMEM((3,) + cube + (ROWS, WIDTH), f32),
        pltpu.VMEM((UNITS_OF[1],) + cube + (ROWS, WIDTH), f32),
        pltpu.VMEM((n,) + cube + (ROWS, WIDTH), f32),
        pltpu.VMEM((n, 2, SIDE, SIDE, ROWS, WIDTH // 2), f32),
        pltpu.VMEM((n, 2, SIDE, SIDE, ROWS, WIDTH), f32),
        pltpu.VMEM((n, 2, SIDE, ROWS, WIDTH // 2), f32),
        pltpu.VMEM((n, 2, SIDE, ROWS, WIDTH), f32),
        pltpu.VMEM((n, 2, ROWS, WIDTH // 2), f32),
        pltpu.VMEM((n, 2, ROWS, WIDTH), f32),
        pltpu.VMEM((3, ROWS, 128), f32),
        pltpu.VMEM((2 * SIDE, ROWS, 128), f32),
        pltpu.VMEM((SIDE, ROWS, 128), f32),
        pltpu.VMEM((SIDE, ROWS, 128), f32),
        pltpu.VMEM((dim, rows), bf16),
        pltpu.VMEM((rows, model), bf16),
        pltpu.VMEM((2, rows, BLOCK), bf16),
        pltpu.VMEM((2, BLOCK, model), bf16),
        pltpu.VMEM((WIDTH // BLOCK,) + cube + (ROWS, BLOCK), f32),
        dma((n,)), dma((n,)), dma((n,)), dma((3, 3, n)), dma((2,)), dma((2, 3)), dma((3, 2)), dma((WIDTH // BLOCK,)),
    ]
    any_spec = pl.BlockSpec(memory_space=pl.ANY)
    vmem_spec = pl.BlockSpec(memory_space=pltpu.VMEM)
    return pl.pallas_call(
        reduce_kernel,
        out_shape=(
            jax.ShapeDtypeStruct((n, ROWS, WIDTH), f32),
            jax.ShapeDtypeStruct((UNITS_OF[3] + UNITS_OF[1], ROWS, WIDTH), f32),
            jax.ShapeDtypeStruct((ROWS, 128), f32),
        ),
        in_specs=[any_spec] * len(args),
        out_specs=(vmem_spec,) * 3,
        scratch_shapes=scratch,
        compiler_params=pltpu.CompilerParams(collective_id=0, has_side_effects=True, vmem_limit_bytes=VMEM_BYTES),
        name='reduce_grads',
    )(*args)


def adam_kernel(lr_ref, clip_ref, norm_tile, shard, swapped, *refs):
    masters, moms, variances = refs[0:4], refs[4:8], refs[8:12]
    new_masters, new_moms, new_vars = refs[12:16], refs[16:20], refs[20:24]
    two_rows, four_rows, norm_ref = refs[24:27]
    core = lax.rem(lax.axis_index('dp'), 2)
    grad_norm = jnp.sqrt(jnp.sum(jnp.sum(norm_tile[...], axis=1, keepdims=True), axis=0, keepdims=True))
    norm_ref[...] = grad_norm
    clip_scale = jnp.minimum(1.0, clip_ref[...] / (grad_norm + NORM_EPS))
    learn_rate = lr_ref[...]

    def update(mat, where, grad):
        scaled = clip_scale * grad
        mom_new = BETA_ONE * moms[mat][where] + (1.0 - BETA_ONE) * scaled
        var_new = BETA_TWO * variances[mat][where] + (1.0 - BETA_TWO) * scaled * scaled
        master_new = masters[mat][where] - learn_rate * (mom_new / BIAS_ONE) / (jnp.sqrt(var_new / BIAS_TWO) + ADAM_EPS)
        new_moms[mat][where] = mom_new
        new_vars[mat][where] = var_new
        new_masters[mat][where] = master_new
        return master_new

    for mat, rows_out in ((2, two_rows), (4, four_rows)):
        for piece in range(UNITS_OF[mat]):
            where = (slice(piece * ROWS, (piece + 1) * ROWS), slice(None))
            rows_out[piece] = update(mat - 1, where, shard[first_unit(mat) + piece]).astype(jnp.bfloat16)
    for mat, base in ((3, 0), (1, UNITS_OF[3])):
        for half in range(2):
            for piece in range(UNITS_OF[mat]):
                col = (half * UNITS_OF[mat] + piece) * WIDTH
                where = (slice(None), slice(col, col + WIDTH))
                block = jnp.where(core == half, shard[first_unit(mat) + piece], swapped[base + piece])
                update(mat - 1, where, jnp.where(core == 0, block[0:ROWS // 2], block[ROWS // 2:ROWS]))


def adam_update(learn_rate, clip_max, norm_tile, shard, swapped, masters, moms, variances):
    state = list(masters) + list(moms) + list(variances)
    f32, bf16 = jnp.float32, jnp.bfloat16
    vmem_spec = pl.BlockSpec(memory_space=pltpu.VMEM)
    out_shape = [jax.ShapeDtypeStruct(part.shape, f32) for part in state]
    out_shape += [
        jax.ShapeDtypeStruct((UNITS_OF[2], ROWS, WIDTH), bf16),
        jax.ShapeDtypeStruct((UNITS_OF[4], ROWS, WIDTH), bf16),
        jax.ShapeDtypeStruct((1, 1), f32),
    ]
    args = [learn_rate.reshape(1, 1), clip_max.reshape(1, 1), norm_tile, shard, swapped] + state
    return pl.pallas_call(
        adam_kernel,
        out_shape=out_shape,
        in_specs=[vmem_spec] * len(args),
        out_specs=[vmem_spec] * len(out_shape),
        name='adam_update',
    )(*args)


class RingSpread:
    def __init__(self, place, axis, known, board, near_sem, far_sem, send_sem):
        self.place, self.axis, self.known, self.board = place, axis, known, board
        self.near_sem, self.far_sem, self.send_sem = near_sem, far_sem, send_sem
        self.up_dev, self.down_dev = place.device({axis: 1}), place.device({axis: SIDE - 1})

    def block(self, unit, by, cols):
        fixed = {dim: self.place.coords[dim] for dim in range(3) if dim not in self.known}
        fixed[self.axis] = self.place.step(self.axis, by)
        return self.board.at[spot((unit,), [0, 1, 2], fixed, cols)]

    def blocks(self, unit, count):
        return self.board.at[(unit,) + (0,) * (2 - len(self.known)) + (pl.ds(0, count),)]

    def start(self, unit):
        s = self
        mine = s.block(unit, 0, ALL)
        send(mine, mine, s.send_sem.at[unit], s.near_sem.at[unit], s.up_dev)
        send(mine, mine, s.send_sem.at[unit], s.near_sem.at[unit], s.down_dev)

    def pass_on(self, unit):
        s = self
        await_bytes(s.blocks(unit, 2), s.near_sem.at[unit])
        from_down, from_up = s.block(unit, SIDE - 1, LEFT), s.block(unit, 1, RIGHT)
        send(from_down, from_down, s.send_sem.at[unit], s.far_sem.at[unit], s.up_dev)
        send(from_up, from_up, s.send_sem.at[unit], s.far_sem.at[unit], s.down_dev)

    def finish(self, unit):
        await_bytes(self.block(unit, 0, ALL), self.far_sem.at[unit])

    def drain(self, unit):
        await_bytes(self.blocks(unit, 3), self.send_sem.at[unit])


def gather_kernel(one_rows, three_rows, two_rows, four_rows, board, other, own_one, own_three, swap_one, swap_three, ring_sems, pair_sems, swap_sems, load_sems):
    place = Place()
    units = unit_list()
    chunks = -(-len(units) // 3)
    counts = [len(range(order, len(units), 3)) for order in range(3)]
    partner = place.device(other_core=True)
    here = tuple(place.coords)
    splits = ((1, one_rows, own_one, swap_one), (3, three_rows, own_three, swap_three))
    loads = []
    for index, (mat, rows, mine, landing) in enumerate(splits):
        span = UNITS_OF[mat] * WIDTH
        loads.append(pltpu.make_async_copy(rows.at[:, pl.ds(pl.multiple_of(place.core * span, WIDTH), span)], mine, load_sems.at[index]))
    for index, (mat, rows) in enumerate(((2, two_rows), (4, four_rows))):
        loads.append(pltpu.make_async_copy(rows, board.at[(pl.ds(first_unit(mat), UNITS_OF[mat]),) + here], load_sems.at[2 + index]))
    for copy in loads:
        copy.start()
    enter(place.neighbours())
    for index, (mat, rows, mine, landing) in enumerate(splits):
        span = UNITS_OF[mat] * WIDTH
        theirs = rows.at[:, pl.ds(pl.multiple_of((1 - place.core) * span, WIDTH), span)]
        send(theirs, landing, swap_sems.at[0, index], swap_sems.at[1, index], partner)
    for copy in loads:
        copy.wait()
    for index, (mat, rows, mine, landing) in enumerate(splits):
        await_bytes(landing, swap_sems.at[1, index])
        for piece in range(UNITS_OF[mat]):
            cols = slice(piece * WIDTH, (piece + 1) * WIDTH)
            top = jnp.where(place.core == 0, mine[:, cols], landing[:, cols])
            bottom = jnp.where(place.core == 0, landing[:, cols], mine[:, cols])
            board[(first_unit(mat) + piece,) + here] = jnp.concatenate([top, bottom], axis=0).astype(board.dtype)

    rings = []
    for order in range(3):
        axes = (order + 2) % 3, (order + 1) % 3, order
        rings.append([RingSpread(place, axis, axes[:level], board, ring_sems.at[level, 0], ring_sems.at[level, 1], ring_sems.at[level, 2]) for level, axis in enumerate(axes)])

    def begin(order, unit, level):
        if level:
            rings[order][level - 1].finish(unit)
        rings[order][level].start(unit)

    def pass_on(order, unit, level):
        rings[order][level].pass_on(unit)

    def hand_over(order, unit, level):
        rings[order][level].finish(unit)
        send(board.at[unit], other.at[unit], pair_sems.at[0, unit], pair_sems.at[1, unit], partner)

    def tidy(order, unit, level):
        await_bytes(other.at[unit], pair_sems.at[1, unit])
        await_bytes(board.at[unit], pair_sems.at[0, unit])
        for ring in rings[order]:
            ring.drain(unit)

    stages = ((begin, 0), (pass_on, 0), (begin, 1), (pass_on, 1), (begin, 2), (pass_on, 2), (hand_over, 2), (tidy, 2))

    def turn(now, carry):
        for lag, (stage, level) in enumerate(stages):
            chunk = now - lag
            for order in range(3):
                @pl.when((chunk >= 0) & (chunk < counts[order]))
                def _(stage=stage, level=level, chunk=chunk, order=order):
                    stage(order, 3 * chunk + order, level)
        return carry

    lax.fori_loop(0, chunks + len(stages) - 1, turn, 0)
    for index, (mat, rows, mine, landing) in enumerate(splits):
        await_bytes(landing, swap_sems.at[0, index])


def gather_rows(one_rows, three_rows, two_rows, four_rows):
    n = len(unit_list())
    cube = (SIDE, SIDE, SIDE)
    bf16, f32 = jnp.bfloat16, jnp.float32
    dma = pltpu.SemaphoreType.DMA
    vmem_spec = pl.BlockSpec(memory_space=pltpu.VMEM)
    full = jax.ShapeDtypeStruct((n,) + cube + (ROWS, WIDTH), bf16)
    return pl.pallas_call(
        gather_kernel,
        out_shape=(full, full),
        in_specs=[pl.BlockSpec(memory_space=pltpu.HBM)] * 4,
        out_specs=(vmem_spec, vmem_spec),
        scratch_shapes=[
            pltpu.VMEM((ROWS // 2, UNITS_OF[1] * WIDTH), f32),
            pltpu.VMEM((ROWS // 2, UNITS_OF[3] * WIDTH), f32),
            pltpu.VMEM((ROWS // 2, UNITS_OF[1] * WIDTH), f32),
            pltpu.VMEM((ROWS // 2, UNITS_OF[3] * WIDTH), f32),
            dma((3, 3, n)), dma((2, n)), dma((2, 2)), dma((4,)),
        ],
        compiler_params=pltpu.CompilerParams(collective_id=1, has_side_effects=True, vmem_limit_bytes=32 * 1024 * 1024),
        name='gather_rows',
    )(one_rows, three_rows, two_rows, four_rows)


def place_kernel(board, other, w_one, w_two, w_three, w_four, sems):
    core = lax.rem(lax.axis_index('dp'), 2)
    outs = {1: w_one, 2: w_two, 3: w_three, 4: w_four}
    copies = []
    for unit, (mat, piece) in enumerate(unit_list()):
        for index, (source, owner) in enumerate(((board, core), (other, 1 - core))):
            if mat in (1, 3):
                start = owner * (UNITS_OF[mat] * WIDTH) + piece * WIDTH
                target = outs[mat].at[:, :, :, :, pl.ds(pl.multiple_of(start, WIDTH), WIDTH)]
            else:
                target = outs[mat].at[:, :, :, owner, pl.ds(piece * ROWS, ROWS), :]
            copies.append(pltpu.make_async_copy(source.at[unit], target, sems.at[index, unit]))
    for copy in copies:
        copy.start()
    for copy in copies:
        copy.wait()


def place_weights(board, other):
    n = len(unit_list())
    cube = (SIDE, SIDE, SIDE)
    bf16 = jnp.bfloat16
    vmem_spec = pl.BlockSpec(memory_space=pltpu.VMEM)
    any_spec = pl.BlockSpec(memory_space=pl.ANY)
    outs = pl.pallas_call(
        place_kernel,
        out_shape=(
            jax.ShapeDtypeStruct(cube + (ROWS, 2 * UNITS_OF[1] * WIDTH), bf16),
            jax.ShapeDtypeStruct(cube + (2, UNITS_OF[2] * ROWS, WIDTH), bf16),
            jax.ShapeDtypeStruct(cube + (ROWS, 2 * UNITS_OF[3] * WIDTH), bf16),
            jax.ShapeDtypeStruct(cube + (2, UNITS_OF[4] * ROWS, WIDTH), bf16),
        ),
        in_specs=[vmem_spec] * 2,
        out_specs=(any_spec,) * 4,
        scratch_shapes=[pltpu.SemaphoreType.DMA((2, n))],
        compiler_params=pltpu.CompilerParams(vmem_limit_bytes=2 * 1024 * 1024),
        name='place_weights',
    )(board, other)
    rows = SIDE ** 3 * ROWS
    return (
        outs[0].reshape(rows, 2 * UNITS_OF[1] * WIDTH),
        outs[1].reshape(2 * SIDE ** 3 * UNITS_OF[2] * ROWS, WIDTH),
        outs[2].reshape(rows, 2 * UNITS_OF[3] * WIDTH),
        outs[3].reshape(2 * SIDE ** 3 * UNITS_OF[4] * ROWS, WIDTH),
    )


def sync_and_update(grads, masters, moms, variances, learn_rate, clip_max):
    shard, swapped, norm_tile = reduce_grads(*grads)
    results = adam_update(learn_rate, clip_max, norm_tile, shard, swapped, masters, moms, variances)
    new_masters, new_moms, new_vars = results[0:4], results[4:8], results[8:12]
    two_rows, four_rows, grad_norm = results[12:15]
    board, other = gather_rows(new_masters[0], new_masters[2], two_rows, four_rows)
    new_weights = place_weights(board, other)
    return tuple(new_weights) + tuple(new_masters) + tuple(new_moms) + tuple(new_vars) + (grad_norm.reshape(()),)


def solution(mesh):
    row_spec = P('dp', None)
    rep_spec = P()

    def per_device(x_rows, dy_rows, w_one, w_two, w_three, w_four, master_one, master_two, master_three, master_four, m_one, m_two, m_three, m_four, v_one, v_two, v_three, v_four, learn_rate, clip_max):
        grads = local_grads(x_rows, dy_rows, w_one, w_two, w_three, w_four)
        return sync_and_update(grads, (master_one, master_two, master_three, master_four), (m_one, m_two, m_three, m_four), (v_one, v_two, v_three, v_four), learn_rate, clip_max)

    in_specs = (row_spec, row_spec) + (rep_spec,) * 4 + (row_spec,) * 12 + (rep_spec, rep_spec)
    out_specs = (rep_spec,) * 4 + (row_spec,) * 12 + (rep_spec,)
    return jax.shard_map(per_device, mesh=mesh, in_specs=in_specs, out_specs=out_specs, check_vma=False)
```

```python
import functools

import jax
import jax.numpy as jnp
from jax import lax
from jax.experimental import pallas as pl
from jax.experimental.pallas import tpu as pltpu
from jax.sharding import PartitionSpec as P

ADAM_STEP = 10
BETA_ONE = 0.9
BETA_TWO = 0.95
ADAM_EPS = 1e-8
NORM_EPS = 1e-6
BIAS_ONE = 1.0 - BETA_ONE ** ADAM_STEP
BIAS_TWO = 1.0 - BETA_TWO ** ADAM_STEP
INV_SQRT2 = 0.7071067811865476
INV_SQRT2PI = 0.3989422804014327

WIDTH = 512
SIDE = 4
ROWS = 8
UNITS_OF = {3: 2, 4: 2, 2: 8, 1: 8}
MESH_ID = pl.DeviceIdType.MESH
BY_COLUMNS = (((1,), (1,)), ((), ()))
BY_ROWS = (((0,), (0,)), ((), ()))
VMEM_BYTES = 62 * 1024 * 1024
ADAM_VMEM = 8 * 1024 * 1024


def unit_list():
    return [(mat, piece) for mat in (3, 4, 1, 2) for piece in range(UNITS_OF[mat])]


def first_unit(mat):
    return unit_list().index((mat, 0))


def gelu_value(pre_act):
    pre_wide = pre_act.astype(jnp.float32)
    return 0.5 * pre_wide * (1.0 + lax.erf(pre_wide * INV_SQRT2))


def gelu_slope(pre_act):
    pre_wide = pre_act.astype(jnp.float32)
    return 0.5 * (1.0 + lax.erf(pre_wide * INV_SQRT2)) + pre_wide * INV_SQRT2PI * jnp.exp(-0.5 * pre_wide * pre_wide)


def forward_kernel(x_ref, w_one, w_two, z_out, a_turned, h_out, x_turned, total):
    step = pl.program_id(0)

    @pl.when(step == 0)
    def _():
        total[...] = jnp.zeros_like(total)
        x_turned[...] = x_ref[...].T

    z_one = jnp.dot(x_ref[...], w_one[...], preferred_element_type=jnp.float32).astype(jnp.bfloat16)
    z_out[...] = z_one
    a_one = gelu_value(z_one).astype(jnp.bfloat16)
    a_turned[...] = a_one.T
    total[...] += jnp.dot(a_one, w_two[...], preferred_element_type=jnp.float32)

    @pl.when(step == pl.num_programs(0) - 1)
    def _():
        h_out[...] = total[...].astype(jnp.bfloat16)


def forward_wide(x_rows, w_one, w_two):
    rows, dim = x_rows.shape
    wide = w_one.shape[1]
    block = 512
    bf16 = jnp.bfloat16
    return pl.pallas_call(
        forward_kernel,
        grid=(wide // block,),
        out_shape=(jax.ShapeDtypeStruct((rows, wide), bf16), jax.ShapeDtypeStruct((wide, rows), bf16), jax.ShapeDtypeStruct((rows, dim), bf16), jax.ShapeDtypeStruct((dim, rows), bf16)),
        in_specs=[pl.BlockSpec((rows, dim), whole_at), pl.BlockSpec((dim, block), across_at), pl.BlockSpec((block, dim), down_at)],
        out_specs=(pl.BlockSpec((rows, block), across_at), pl.BlockSpec((block, rows), down_at), pl.BlockSpec((rows, dim), whole_at), pl.BlockSpec((dim, rows), whole_at)),
        scratch_shapes=[pltpu.VMEM((rows, dim), jnp.float32)],
        compiler_params=pltpu.CompilerParams(vmem_limit_bytes=VMEM_BYTES),
        name='forward_wide',
    )(x_rows, w_one, w_two)


def middle_kernel(h_ref, dy_ref, w_three, w_four, g_three, g_four, dh_out, total, h_turned):
    step = pl.program_id(0)
    f32, bf16 = jnp.float32, jnp.bfloat16

    @pl.when(step == 0)
    def _():
        total[...] = jnp.zeros_like(total)
        h_turned[...] = h_ref[...].T

    z_three = jnp.dot(h_ref[...], w_three[...], preferred_element_type=f32).astype(bf16)
    a_three = gelu_value(z_three).astype(bf16)
    da_three = lax.dot_general(dy_ref[...], w_four[...], BY_COLUMNS, preferred_element_type=f32).astype(bf16)
    dz_three = (da_three.astype(f32) * gelu_slope(z_three)).astype(bf16)
    g_four[...] = lax.dot_general(a_three, dy_ref[...], BY_ROWS, preferred_element_type=f32)
    g_three[...] = jnp.dot(h_turned[...], dz_three, preferred_element_type=f32)
    total[...] += lax.dot_general(dz_three, w_three[...], BY_COLUMNS, preferred_element_type=f32)

    @pl.when(step == pl.num_programs(0) - 1)
    def _():
        dh_out[...] = total[...].astype(bf16)


def middle(h_two, dy_rows, w_three, w_four):
    rows, dim = h_two.shape
    wide = w_three.shape[1]
    block = 512
    f32, bf16 = jnp.float32, jnp.bfloat16
    whole = pl.BlockSpec((rows, dim), whole_at)
    across, down = pl.BlockSpec((dim, block), across_at), pl.BlockSpec((block, dim), down_at)
    return pl.pallas_call(
        middle_kernel,
        grid=(wide // block,),
        out_shape=(jax.ShapeDtypeStruct((dim, wide), f32), jax.ShapeDtypeStruct((wide, dim), f32), jax.ShapeDtypeStruct((rows, dim), bf16)),
        in_specs=[whole, whole, across, down],
        out_specs=(across, down, whole),
        scratch_shapes=[pltpu.VMEM((rows, dim), f32), pltpu.VMEM((dim, rows), bf16)],
        compiler_params=pltpu.CompilerParams(vmem_limit_bytes=VMEM_BYTES),
        name='middle',
    )(h_two, dy_rows, w_three, w_four)


def local_grads(x_rows, dy_rows, w_one, w_two, w_three, w_four):
    z_one, a_turned, h_two, x_turned = forward_wide(x_rows, w_one, w_two)
    g_three, g_four, dh_two = middle(h_two, dy_rows, w_three, w_four)
    return x_turned, dh_two, z_one, w_two, a_turned, g_three, g_four


def whole_at(step):
    return 0, 0


def across_at(step):
    return 0, step


def down_at(step):
    return step, 0


class Place:
    def __init__(self):
        me = lax.axis_index('dp')
        self.core = lax.rem(me, 2)
        self.coords = [lax.div(me, 2 * SIDE * SIDE), lax.rem(lax.div(me, 2 * SIDE), SIDE), lax.rem(lax.div(me, 2), SIDE)]

    def step(self, axis, by):
        return lax.rem(self.coords[axis] + by, SIDE)

    def device(self, moves=None, other_core=False):
        pos = list(self.coords)
        for axis, by in (moves or {}).items():
            pos[axis] = self.step(axis, by)
        core = 1 - self.core if other_core else self.core
        return (((pos[0] * SIDE + pos[1]) * SIDE + pos[2]) * 2 + core,)

    def neighbours(self):
        found = [self.device(other_core=True)]
        for axis in range(3):
            found += [self.device({axis: 1}), self.device({axis: SIDE - 1})]
        return found


def enter(peers):
    barrier = pltpu.get_barrier_semaphore()
    for peer in peers:
        pl.semaphore_signal(barrier, inc=1, device_id=peer, device_id_type=MESH_ID)
    pl.semaphore_wait(barrier, len(peers))


def send(src, dst, send_sem, recv_sem, peer):
    pltpu.make_async_remote_copy(src_ref=src, dst_ref=dst, send_sem=send_sem, recv_sem=recv_sem, device_id=peer, device_id_type=MESH_ID).start()


def await_bytes(ref, sem):
    pltpu.make_async_copy(ref, ref, sem).wait()


def spot(lead, dims, fixed, cols):
    return tuple(lead) + tuple(fixed.get(axis, slice(None)) for axis in dims) + (slice(None), cols)


LEFT = pl.ds(0, WIDTH // 2)
RIGHT = pl.ds(WIDTH // 2, WIDTH // 2)
ALL = slice(None)


class RingSum:
    def __init__(self, place, dims, axis, relay, final, relay_sem, final_sem, send_sem):
        self.place, self.dims, self.axis = place, dims, axis
        self.relay, self.final = relay, final
        self.relay_sem, self.final_sem, self.send_sem = relay_sem, final_sem, send_sem
        self.own = place.coords[axis]
        self.up, self.down, self.far = place.step(axis, 1), place.step(axis, SIDE - 1), place.step(axis, 2)
        self.up_dev, self.down_dev = place.device({axis: 1}), place.device({axis: SIDE - 1})
        self.rest = [dim for dim in dims if dim != axis]

    def start(self, src, lead, unit):
        s = self
        send(src.at[spot(lead, s.dims, {s.axis: s.far}, LEFT)], s.relay.at[unit, 0], s.send_sem.at[unit], s.relay_sem.at[unit], s.up_dev)
        send(src.at[spot(lead, s.dims, {s.axis: s.far}, RIGHT)], s.relay.at[unit, 1], s.send_sem.at[unit], s.relay_sem.at[unit], s.down_dev)
        send(src.at[spot(lead, s.dims, {s.axis: s.up}, RIGHT)], s.final.at[spot((unit, 0), s.rest, {}, RIGHT)], s.send_sem.at[unit], s.final_sem.at[unit], s.up_dev)
        send(src.at[spot(lead, s.dims, {s.axis: s.down}, LEFT)], s.final.at[spot((unit, 1), s.rest, {}, LEFT)], s.send_sem.at[unit], s.final_sem.at[unit], s.down_dev)

    def pass_on(self, src, lead, unit):
        s = self
        await_bytes(s.relay.at[unit], s.relay_sem.at[unit])
        up_spot = spot(lead, s.dims, {s.axis: s.up}, LEFT)
        src[up_spot] = src[up_spot] + s.relay[unit, 0]
        send(src.at[up_spot], s.final.at[spot((unit, 0), s.rest, {}, LEFT)], s.send_sem.at[unit], s.final_sem.at[unit], s.up_dev)
        down_spot = spot(lead, s.dims, {s.axis: s.down}, RIGHT)
        src[down_spot] = src[down_spot] + s.relay[unit, 1]
        send(src.at[down_spot], s.final.at[spot((unit, 1), s.rest, {}, RIGHT)], s.send_sem.at[unit], s.final_sem.at[unit], s.down_dev)

    def finish(self, src, lead, unit):
        s = self
        await_bytes(s.final.at[unit], s.final_sem.at[unit])
        return src[spot(lead, s.dims, {s.axis: s.own}, ALL)] + s.final[unit, 0] + s.final[unit, 1]

    def drain(self, unit):
        await_bytes(self.relay.at[unit], self.send_sem.at[unit])
        await_bytes(self.final.at[unit], self.send_sem.at[unit])


BLOCK = 256
BLOCKS_PER_UNIT = 2 * (WIDTH // BLOCK)
BLOCKS_AFTER = (3, 3, 2)
TALL_AFTER = (4, 4, 4)
WIDE_DEEP = 3
TALL_DEEP = 6
STORE_DEEP = 3


def reduce_kernel(x_turned, dh_two, z_one, w_two, a_turned, g_three, g_four, shard, swapped, norm_tile, g_two, own, part, relay1, final1, relay2, final2, relay3, final3, norm_own, norm_a, norm_b, norm_c, x_buf, dh_buf, z_buf, w_buf, out_buf, a_buf, tall_buf, load_sem, part_send, part_recv, ring_sems, swap_sems, norm_sems, fetch_sems, out_sems, tall_sems):
    place = Place()
    units = unit_list()
    chunks = -(-len(units) // 3)
    counts = [len(range(order, len(units), 3)) for order in range(3)]
    wide_base = first_unit(1)
    wide_units = UNITS_OF[1]
    wide_half = wide_units * WIDTH
    pieces = WIDTH // BLOCK
    blocks = wide_units * BLOCKS_PER_UNIT
    partner = place.device(other_core=True)
    group_x = [(place.device({2: by}, other_core=swap)) for by in range(SIDE) for swap in (False, True) if by or swap]
    group_y = [place.device({1: by}) for by in range(1, SIDE)]
    group_z = [place.device({0: by}) for by in range(1, SIDE)]

    def block_start(block):
        unit = lax.div(block, BLOCKS_PER_UNIT)
        mine = lax.rem(lax.div(block, pieces), 2)
        owner = lax.rem(place.core + 1 + mine, 2)
        start = owner * wide_half + unit * WIDTH + lax.rem(block, pieces) * BLOCK
        return pl.multiple_of(start, BLOCK)

    def fetch(block):
        slot = lax.rem(block, WIDE_DEEP)
        start = block_start(block)
        return (
            pltpu.make_async_copy(z_one.at[:, pl.ds(start, BLOCK)], z_buf.at[slot], fetch_sems.at[0, slot]),
            pltpu.make_async_copy(w_two.at[pl.ds(start, BLOCK), :], w_buf.at[slot], fetch_sems.at[1, slot]),
        )

    steady = (pltpu.make_async_copy(x_turned, x_buf, fetch_sems.at[2, 0]), pltpu.make_async_copy(dh_two, dh_buf, fetch_sems.at[2, 1]))
    tall_blocks_all = 2 * UNITS_OF[2] * ROWS * SIDE ** 3 // BLOCK
    tall_chips = BLOCK // (2 * UNITS_OF[2] * ROWS)

    def tall_fetch(block):
        slot = lax.rem(block, TALL_DEEP)
        return pltpu.make_async_copy(a_turned.at[pl.ds(pl.multiple_of(block * BLOCK, BLOCK), BLOCK), :], a_buf.at[slot], tall_sems.at[0, slot])

    def tall_store(block):
        slot = lax.rem(block, STORE_DEEP)
        chip = block * tall_chips
        spot_of = (lax.div(chip, SIDE * SIDE), lax.rem(lax.div(chip, SIDE), SIDE), pl.ds(lax.rem(chip, SIDE), tall_chips))
        return pltpu.make_async_copy(tall_buf.at[slot], g_two.at[spot_of], tall_sems.at[1, slot])

    for copy in steady:
        copy.start()
    for block in range(WIDE_DEEP - 1):
        for copy in fetch(block):
            copy.start()
    for block in range(TALL_DEEP - 1):
        tall_fetch(block).start()
    enter(group_x + group_y + group_z)

    def source(mat, piece, core):
        if mat == 3:
            start = core * (UNITS_OF[mat] * WIDTH) + piece * WIDTH
            return g_three.at[:, :, :, :, pl.ds(pl.multiple_of(start, WIDTH), WIDTH)]
        ref = g_two if mat == 2 else g_four
        return ref.at[:, :, :, core, pl.ds(piece * ROWS, ROWS), :]

    def sems_of(level):
        return [ring_sems.at[level, kind] for kind in range(3)]

    rings = []
    for order in range(3):
        a, b = order, (order + 1) % 3
        c = (order + 2) % 3
        first = RingSum(place, [0, 1, 2], a, relay1, final1, *sems_of(0))
        second = RingSum(place, first.rest, b, relay2, final2, *sems_of(1))
        third = RingSum(place, second.rest, c, relay3, final3, *sems_of(2))
        rings.append((first, second, third))

    def own_slot(unit):
        return lax.rem(unit + wide_base, wide_units) if not isinstance(unit, int) else (unit + wide_base) % wide_units

    def load(chunk):
        for order in range(3):
            unit = 3 * chunk + order
            if unit >= len(units) or units[unit][0] == 1:
                continue
            mat, piece = units[unit]
            send(source(mat, piece, 1 - place.core), part.at[unit], part_send.at[unit], part_recv.at[unit], partner)
            pltpu.make_async_copy(source(mat, piece, place.core), own.at[own_slot(unit)], load_sem.at[unit]).start()

    def wide_block(block, carry):
        slot = lax.rem(block, WIDE_DEEP)

        @pl.when(block + WIDE_DEEP - 1 < blocks)
        def _():
            for copy in fetch(block + WIDE_DEEP - 1):
                copy.start()

        for copy in fetch(block):
            copy.wait()
        da_one = lax.dot_general(dh_buf[...], w_buf[slot], BY_COLUMNS, preferred_element_type=jnp.float32).astype(jnp.bfloat16)
        dz_one = (da_one.astype(jnp.float32) * gelu_slope(z_buf[slot])).astype(jnp.bfloat16)
        grad = jnp.dot(x_buf[...], dz_one, preferred_element_type=jnp.float32)
        grad = grad.reshape(SIDE, SIDE, SIDE, ROWS, BLOCK)
        unit = lax.div(block, BLOCKS_PER_UNIT)
        piece = lax.rem(block, pieces)
        mine = lax.rem(lax.div(block, pieces), 2)
        cols = pl.ds(pl.multiple_of(piece * BLOCK, BLOCK), BLOCK)
        cube_all = (ALL,) * 4

        @pl.when(mine == 1)
        def _():
            own[(unit,) + cube_all + (cols,)] = grad

        @pl.when(mine == 0)
        def _():
            @pl.when(unit > 0)
            def _():
                await_bytes(out_buf.at[piece], out_sems.at[piece])
            out_buf[piece] = grad
            send(out_buf.at[piece], part.at[(wide_base + unit,) + cube_all + (cols,)], out_sems.at[piece], part_recv.at[wide_base + unit], partner)
        return carry

    def tall_block(block, carry):
        slot = lax.rem(block, STORE_DEEP)

        @pl.when(block + TALL_DEEP - 1 < tall_blocks_all)
        def _():
            tall_fetch(block + TALL_DEEP - 1).start()

        tall_fetch(block).wait()
        grad = jnp.dot(a_buf[lax.rem(block, TALL_DEEP)], dh_buf[...], preferred_element_type=jnp.float32)

        @pl.when(block >= STORE_DEEP)
        def _():
            tall_store(block - STORE_DEEP).wait()
        tall_buf[slot] = grad.reshape(tall_buf.shape[1:])
        tall_store(block).start()

        @pl.when(block == tall_blocks_all - 1)
        def _():
            for back in range(STORE_DEEP):
                tall_store(block - back).wait()
        return carry

    def stage_b(order, chunk, unit):
        await_bytes(part.at[unit], part_recv.at[unit])

        slot = own_slot(unit)

        @pl.when((unit < wide_base) | (unit >= wide_base + wide_units))
        def _():
            await_bytes(own.at[slot], load_sem.at[unit])
        part[unit] = part[unit] + own[slot]
        rings[order][0].start(part, (unit,), unit)

    def stage_c(order, chunk, unit):
        rings[order][0].pass_on(part, (unit,), unit)

    def stage_d(order, chunk, unit):
        final1[unit, 0] = rings[order][0].finish(part, (unit,), unit)
        rings[order][1].start(final1, (unit, 0), unit)

    def stage_e(order, chunk, unit):
        rings[order][1].pass_on(final1, (unit, 0), unit)

    def stage_f(order, chunk, unit):
        final2[unit, 0] = rings[order][1].finish(final1, (unit, 0), unit)
        rings[order][2].start(final2, (unit, 0), unit)

    def stage_g(order, chunk, unit):
        rings[order][2].pass_on(final2, (unit, 0), unit)

    def stage_h(order, chunk, unit):
        shard[unit] = rings[order][2].finish(final2, (unit, 0), unit) * (1.0 / (2 * SIDE ** 3))

    stages = (stage_b, stage_c, stage_d, stage_e, stage_f, stage_g, stage_h)

    def run(now, lag):
        chunk = now - lag - 1
        for order in range(3):
            @pl.when((chunk >= 0) & (chunk < counts[order]))
            def _(order=order):
                stages[lag](order, chunk, 3 * chunk + order)

    def wide_blocks(low, count):
        lax.fori_loop(lax.min(low, blocks), lax.min(low + count, blocks), wide_block, 0)

    def wide_blocks(low, count):
        lax.fori_loop(lax.min(low, blocks), lax.min(low + count, blocks), wide_block, 0)

    def tall_blocks(low, count):
        lax.fori_loop(lax.min(low, tall_blocks_all), lax.min(low + count, tall_blocks_all), tall_block, 0)

    load(0)
    for copy in steady:
        copy.wait()
    first_wide = 8
    wide_blocks(0, first_wide)

    def turn(now, carry):
        run(now, 0)
        for chunk in range(1, chunks):
            if any(mat != 1 for mat, _ in units[3 * chunk:3 * chunk + 3]):
                @pl.when(now == chunk)
                def _(chunk=chunk):
                    load(chunk)

        wide_done = first_wide + (now - 1) * sum(BLOCKS_AFTER)
        tall_done = (now - 1) * sum(TALL_AFTER)
        for lag in range(1, len(stages)):
            if lag <= len(BLOCKS_AFTER):
                wide_blocks(wide_done, BLOCKS_AFTER[lag - 1])
                tall_blocks(tall_done, TALL_AFTER[lag - 1])
                wide_done = wide_done + BLOCKS_AFTER[lag - 1]
                tall_done = tall_done + TALL_AFTER[lag - 1]
            run(now, lag)
        return carry

    lax.fori_loop(1, chunks + len(stages), turn, 0)

    n_three = UNITS_OF[3]
    send(shard.at[pl.ds(0, n_three)], swapped.at[pl.ds(0, n_three)], swap_sems.at[0], swap_sems.at[1], partner)
    send(shard.at[pl.ds(wide_base, wide_units)], swapped.at[pl.ds(n_three, wide_units)], swap_sems.at[0], swap_sems.at[1], partner)

    def fold(unit, total):
        value = shard[unit]
        return total + value * value

    squares = lax.fori_loop(0, len(units), fold, jnp.zeros((ROWS, WIDTH), jnp.float32))
    total = squares[:, 0:128]
    for col in range(1, WIDTH // 128):
        total = total + squares[:, col * 128:(col + 1) * 128]
    levels = ((norm_a, group_x, place.coords[2] * 2 + place.core), (norm_b, group_y, place.coords[1]), (norm_c, group_z, place.coords[0]))
    for level, (board, group, seat) in enumerate(levels):
        norm_own[level] = total
        board[seat] = total
        for peer in group:
            send(norm_own.at[level], board.at[seat], norm_sems.at[0, level], norm_sems.at[1, level], peer)
        await_bytes(board.at[pl.ds(0, len(group))], norm_sems.at[1, level])
        total = board[0]
        for row in range(1, len(group) + 1):
            total = total + board[row]
    norm_tile[...] = total

    await_bytes(swapped, swap_sems.at[0])
    await_bytes(swapped, swap_sems.at[1])
    for level, (board, group, seat) in enumerate(levels):
        await_bytes(board.at[pl.ds(0, len(group))], norm_sems.at[0, level])
    for piece in range(pieces):
        await_bytes(out_buf.at[piece], out_sems.at[piece])
    for order in range(3):
        def tidy(chunk, carry, order=order):
            unit = 3 * chunk + order
            for ring in rings[order]:
                ring.drain(unit)

            @pl.when((unit < wide_base) | (unit >= wide_base + wide_units))
            def _():
                await_bytes(part.at[unit], part_send.at[unit])
            return carry

        lax.fori_loop(0, counts[order], tidy, 0)


def reduce_grads(x_turned, dh_two, z_one, w_two, a_turned, g_three, g_four):
    n = len(unit_list())
    cube = (SIDE, SIDE, SIDE)
    args = (
        x_turned, dh_two, z_one, w_two, a_turned,
        g_three.reshape(cube + (ROWS, 2 * UNITS_OF[3] * WIDTH)),
        g_four.reshape(cube + (2, UNITS_OF[4] * ROWS, WIDTH)),
    )
    f32, bf16 = jnp.float32, jnp.bfloat16
    dma = pltpu.SemaphoreType.DMA
    dim, rows = x_turned.shape
    model = dh_two.shape[1]
    scratch = [
        pltpu.VMEM((UNITS_OF[1],) + cube + (ROWS, WIDTH), f32),
        pltpu.VMEM((n,) + cube + (ROWS, WIDTH), f32),
        pltpu.VMEM((n, 2, SIDE, SIDE, ROWS, WIDTH // 2), f32),
        pltpu.VMEM((n, 2, SIDE, SIDE, ROWS, WIDTH), f32),
        pltpu.VMEM((n, 2, SIDE, ROWS, WIDTH // 2), f32),
        pltpu.VMEM((n, 2, SIDE, ROWS, WIDTH), f32),
        pltpu.VMEM((n, 2, ROWS, WIDTH // 2), f32),
        pltpu.VMEM((n, 2, ROWS, WIDTH), f32),
        pltpu.VMEM((3, ROWS, 128), f32),
        pltpu.VMEM((2 * SIDE, ROWS, 128), f32),
        pltpu.VMEM((SIDE, ROWS, 128), f32),
        pltpu.VMEM((SIDE, ROWS, 128), f32),
        pltpu.VMEM((dim, rows), bf16),
        pltpu.VMEM((rows, model), bf16),
        pltpu.VMEM((WIDE_DEEP, rows, BLOCK), bf16),
        pltpu.VMEM((WIDE_DEEP, BLOCK, model), bf16),
        pltpu.VMEM((WIDTH // BLOCK,) + cube + (ROWS, BLOCK), f32),
        pltpu.VMEM((TALL_DEEP, BLOCK, rows), bf16),
        pltpu.VMEM((STORE_DEEP, BLOCK // (2 * UNITS_OF[2] * ROWS), 2, UNITS_OF[2] * ROWS, WIDTH), f32),
        dma((n,)), dma((n,)), dma((n,)), dma((3, 3, n)), dma((2,)), dma((2, 3)), dma((3, WIDE_DEEP)), dma((WIDTH // BLOCK,)), dma((2, TALL_DEEP)),
    ]
    any_spec = pl.BlockSpec(memory_space=pl.ANY)
    vmem_spec = pl.BlockSpec(memory_space=pltpu.VMEM)
    return pl.pallas_call(
        reduce_kernel,
        out_shape=(
            jax.ShapeDtypeStruct((n, ROWS, WIDTH), f32),
            jax.ShapeDtypeStruct((UNITS_OF[3] + UNITS_OF[1], ROWS, WIDTH), f32),
            jax.ShapeDtypeStruct((ROWS, 128), f32),
            jax.ShapeDtypeStruct(cube + (2, UNITS_OF[2] * ROWS, WIDTH), f32),
        ),
        in_specs=[any_spec] * len(args),
        out_specs=(vmem_spec,) * 3 + (any_spec,),
        scratch_shapes=scratch,
        compiler_params=pltpu.CompilerParams(collective_id=0, has_side_effects=True, vmem_limit_bytes=VMEM_BYTES),
        name='reduce_grads',
    )(*args)


def adam_kernel(lr_ref, clip_ref, norm_tile, shard, swapped, *refs):
    masters, moms, variances = refs[0:4], refs[4:8], refs[8:12]
    new_masters, new_moms, new_vars = refs[12:16], refs[16:20], refs[20:24]
    two_rows, four_rows, norm_ref = refs[24:27]
    core = lax.rem(lax.axis_index('dp'), 2)
    grad_norm = jnp.sqrt(jnp.sum(jnp.sum(norm_tile[...], axis=1, keepdims=True), axis=0, keepdims=True))
    norm_ref[...] = grad_norm
    clip_scale = jnp.minimum(1.0, clip_ref[...] / (grad_norm + NORM_EPS))
    learn_rate = lr_ref[...]

    def update(mat, where, grad):
        scaled = clip_scale * grad
        mom_new = BETA_ONE * moms[mat][where] + (1.0 - BETA_ONE) * scaled
        var_new = BETA_TWO * variances[mat][where] + (1.0 - BETA_TWO) * scaled * scaled
        master_new = masters[mat][where] - learn_rate * (mom_new / BIAS_ONE) / (jnp.sqrt(var_new / BIAS_TWO) + ADAM_EPS)
        new_moms[mat][where] = mom_new
        new_vars[mat][where] = var_new
        new_masters[mat][where] = master_new
        return master_new

    for mat, rows_out in ((2, two_rows), (4, four_rows)):
        for piece in range(UNITS_OF[mat]):
            where = (slice(piece * ROWS, (piece + 1) * ROWS), slice(None))
            rows_out[piece] = update(mat - 1, where, shard[first_unit(mat) + piece]).astype(jnp.bfloat16)
    for mat, base in ((3, 0), (1, UNITS_OF[3])):
        for half in range(2):
            for piece in range(UNITS_OF[mat]):
                col = (half * UNITS_OF[mat] + piece) * WIDTH
                where = (slice(None), slice(col, col + WIDTH))
                block = jnp.where(core == half, shard[first_unit(mat) + piece], swapped[base + piece])
                update(mat - 1, where, jnp.where(core == 0, block[0:ROWS // 2], block[ROWS // 2:ROWS]))


def adam_update(learn_rate, clip_max, norm_tile, shard, swapped, masters, moms, variances):
    state = list(masters) + list(moms) + list(variances)
    f32, bf16 = jnp.float32, jnp.bfloat16
    vmem_spec = pl.BlockSpec(memory_space=pltpu.VMEM)
    out_shape = [jax.ShapeDtypeStruct(part.shape, f32) for part in state]
    out_shape += [
        jax.ShapeDtypeStruct((UNITS_OF[2], ROWS, WIDTH), bf16),
        jax.ShapeDtypeStruct((UNITS_OF[4], ROWS, WIDTH), bf16),
        jax.ShapeDtypeStruct((1, 1), f32),
    ]
    args = [learn_rate.reshape(1, 1), clip_max.reshape(1, 1), norm_tile, shard, swapped] + state
    return pl.pallas_call(
        adam_kernel,
        out_shape=out_shape,
        in_specs=[vmem_spec] * len(args),
        out_specs=[vmem_spec] * len(out_shape),
        compiler_params=pltpu.CompilerParams(vmem_limit_bytes=ADAM_VMEM),
        name='adam_update',
    )(*args)


class RingSpread:
    def __init__(self, place, axis, known, board, near_sem, far_sem, send_sem):
        self.place, self.axis, self.known, self.board = place, axis, known, board
        self.near_sem, self.far_sem, self.send_sem = near_sem, far_sem, send_sem
        self.up_dev, self.down_dev = place.device({axis: 1}), place.device({axis: SIDE - 1})

    def block(self, unit, by, cols):
        fixed = {dim: self.place.coords[dim] for dim in range(3) if dim not in self.known}
        fixed[self.axis] = self.place.step(self.axis, by)
        return self.board.at[spot((unit,), [0, 1, 2], fixed, cols)]

    def blocks(self, unit, count):
        return self.board.at[(unit,) + (0,) * (2 - len(self.known)) + (pl.ds(0, count),)]

    def start(self, unit):
        s = self
        mine = s.block(unit, 0, ALL)
        send(mine, mine, s.send_sem.at[unit], s.near_sem.at[unit], s.up_dev)
        send(mine, mine, s.send_sem.at[unit], s.near_sem.at[unit], s.down_dev)

    def pass_on(self, unit):
        s = self
        await_bytes(s.blocks(unit, 2), s.near_sem.at[unit])
        from_down, from_up = s.block(unit, SIDE - 1, LEFT), s.block(unit, 1, RIGHT)
        send(from_down, from_down, s.send_sem.at[unit], s.far_sem.at[unit], s.up_dev)
        send(from_up, from_up, s.send_sem.at[unit], s.far_sem.at[unit], s.down_dev)

    def finish(self, unit):
        await_bytes(self.block(unit, 0, ALL), self.far_sem.at[unit])

    def drain(self, unit):
        await_bytes(self.blocks(unit, 3), self.send_sem.at[unit])


def gather_kernel(one_rows, three_rows, two_rows, four_rows, board, other, own_one, own_three, swap_one, swap_three, ring_sems, pair_sems, swap_sems, load_sems):
    place = Place()
    units = unit_list()
    chunks = -(-len(units) // 3)
    counts = [len(range(order, len(units), 3)) for order in range(3)]
    partner = place.device(other_core=True)
    here = tuple(place.coords)
    splits = ((1, one_rows, own_one, swap_one), (3, three_rows, own_three, swap_three))
    loads = []
    for index, (mat, rows, mine, landing) in enumerate(splits):
        span = UNITS_OF[mat] * WIDTH
        loads.append(pltpu.make_async_copy(rows.at[:, pl.ds(pl.multiple_of(place.core * span, WIDTH), span)], mine, load_sems.at[index]))
    for index, (mat, rows) in enumerate(((2, two_rows), (4, four_rows))):
        loads.append(pltpu.make_async_copy(rows, board.at[(pl.ds(first_unit(mat), UNITS_OF[mat]),) + here], load_sems.at[2 + index]))
    for copy in loads:
        copy.start()
    enter(place.neighbours())
    for index, (mat, rows, mine, landing) in enumerate(splits):
        span = UNITS_OF[mat] * WIDTH
        theirs = rows.at[:, pl.ds(pl.multiple_of((1 - place.core) * span, WIDTH), span)]
        send(theirs, landing, swap_sems.at[0, index], swap_sems.at[1, index], partner)
    for copy in loads:
        copy.wait()
    for index, (mat, rows, mine, landing) in enumerate(splits):
        await_bytes(landing, swap_sems.at[1, index])
        for piece in range(UNITS_OF[mat]):
            cols = slice(piece * WIDTH, (piece + 1) * WIDTH)
            top = jnp.where(place.core == 0, mine[:, cols], landing[:, cols])
            bottom = jnp.where(place.core == 0, landing[:, cols], mine[:, cols])
            board[(first_unit(mat) + piece,) + here] = jnp.concatenate([top, bottom], axis=0).astype(board.dtype)

    rings = []
    for order in range(3):
        axes = (order + 2) % 3, (order + 1) % 3, order
        rings.append([RingSpread(place, axis, axes[:level], board, *[ring_sems.at[level, kind] for kind in range(3)]) for level, axis in enumerate(axes)])

    def begin(order, unit, level):
        if level:
            rings[order][level - 1].finish(unit)
        rings[order][level].start(unit)

    def pass_on(order, unit, level):
        rings[order][level].pass_on(unit)

    def hand_over(order, unit, level):
        rings[order][level].finish(unit)
        send(board.at[unit], other.at[unit], pair_sems.at[0, unit], pair_sems.at[1, unit], partner)

    def tidy(order, unit, level):
        await_bytes(other.at[unit], pair_sems.at[1, unit])
        await_bytes(board.at[unit], pair_sems.at[0, unit])
        for ring in rings[order]:
            ring.drain(unit)

    stages = ((begin, 0), (pass_on, 0), (begin, 1), (pass_on, 1), (begin, 2), (pass_on, 2), (hand_over, 2), (tidy, 2))

    def turn(now, carry):
        for lag, (stage, level) in enumerate(stages):
            chunk = now - lag
            for order in range(3):
                @pl.when((chunk >= 0) & (chunk < counts[order]))
                def _(stage=stage, level=level, chunk=chunk, order=order):
                    stage(order, 3 * chunk + order, level)
        return carry

    lax.fori_loop(0, chunks + len(stages) - 1, turn, 0)
    for index, (mat, rows, mine, landing) in enumerate(splits):
        await_bytes(landing, swap_sems.at[0, index])


def gather_rows(one_rows, three_rows, two_rows, four_rows):
    n = len(unit_list())
    cube = (SIDE, SIDE, SIDE)
    bf16, f32 = jnp.bfloat16, jnp.float32
    dma = pltpu.SemaphoreType.DMA
    vmem_spec = pl.BlockSpec(memory_space=pltpu.VMEM)
    full = jax.ShapeDtypeStruct((n,) + cube + (ROWS, WIDTH), bf16)
    return pl.pallas_call(
        gather_kernel,
        out_shape=(full, full),
        in_specs=[pl.BlockSpec(memory_space=pltpu.HBM)] * 4,
        out_specs=(vmem_spec, vmem_spec),
        scratch_shapes=[
            pltpu.VMEM((ROWS // 2, UNITS_OF[1] * WIDTH), f32),
            pltpu.VMEM((ROWS // 2, UNITS_OF[3] * WIDTH), f32),
            pltpu.VMEM((ROWS // 2, UNITS_OF[1] * WIDTH), f32),
            pltpu.VMEM((ROWS // 2, UNITS_OF[3] * WIDTH), f32),
            dma((3, 3, n)), dma((2, n)), dma((2, 2)), dma((4,)),
        ],
        compiler_params=pltpu.CompilerParams(collective_id=1, has_side_effects=True, vmem_limit_bytes=32 * 1024 * 1024),
        name='gather_rows',
    )(one_rows, three_rows, two_rows, four_rows)


def place_kernel(board, other, w_one, w_two, w_three, w_four, sems):
    core = lax.rem(lax.axis_index('dp'), 2)
    outs = {1: w_one, 2: w_two, 3: w_three, 4: w_four}
    copies = []
    for unit, (mat, piece) in enumerate(unit_list()):
        for index, (source, owner) in enumerate(((board, core), (other, 1 - core))):
            if mat in (1, 3):
                start = owner * (UNITS_OF[mat] * WIDTH) + piece * WIDTH
                target = outs[mat].at[:, :, :, :, pl.ds(pl.multiple_of(start, WIDTH), WIDTH)]
            else:
                target = outs[mat].at[:, :, :, owner, pl.ds(piece * ROWS, ROWS), :]
            copies.append(pltpu.make_async_copy(source.at[unit], target, sems.at[index, unit]))
    for copy in copies:
        copy.start()
    for copy in copies:
        copy.wait()


def place_weights(board, other):
    n = len(unit_list())
    cube = (SIDE, SIDE, SIDE)
    bf16 = jnp.bfloat16
    vmem_spec = pl.BlockSpec(memory_space=pltpu.VMEM)
    any_spec = pl.BlockSpec(memory_space=pl.ANY)
    outs = pl.pallas_call(
        place_kernel,
        out_shape=(
            jax.ShapeDtypeStruct(cube + (ROWS, 2 * UNITS_OF[1] * WIDTH), bf16),
            jax.ShapeDtypeStruct(cube + (2, UNITS_OF[2] * ROWS, WIDTH), bf16),
            jax.ShapeDtypeStruct(cube + (ROWS, 2 * UNITS_OF[3] * WIDTH), bf16),
            jax.ShapeDtypeStruct(cube + (2, UNITS_OF[4] * ROWS, WIDTH), bf16),
        ),
        in_specs=[vmem_spec] * 2,
        out_specs=(any_spec,) * 4,
        scratch_shapes=[pltpu.SemaphoreType.DMA((2, n))],
        compiler_params=pltpu.CompilerParams(vmem_limit_bytes=2 * 1024 * 1024),
        name='place_weights',
    )(board, other)
    rows = SIDE ** 3 * ROWS
    return (
        outs[0].reshape(rows, 2 * UNITS_OF[1] * WIDTH),
        outs[1].reshape(2 * SIDE ** 3 * UNITS_OF[2] * ROWS, WIDTH),
        outs[2].reshape(rows, 2 * UNITS_OF[3] * WIDTH),
        outs[3].reshape(2 * SIDE ** 3 * UNITS_OF[4] * ROWS, WIDTH),
    )


def sync_and_update(grads, masters, moms, variances, learn_rate, clip_max):
    shard, swapped, norm_tile, _ = reduce_grads(*grads)
    results = adam_update(learn_rate, clip_max, norm_tile, shard, swapped, masters, moms, variances)
    new_masters, new_moms, new_vars = results[0:4], results[4:8], results[8:12]
    two_rows, four_rows, grad_norm = results[12:15]
    board, other = gather_rows(new_masters[0], new_masters[2], two_rows, four_rows)
    new_weights = place_weights(board, other)
    return tuple(new_weights) + tuple(new_masters) + tuple(new_moms) + tuple(new_vars) + (grad_norm.reshape(()),)


def solution(mesh):
    row_spec = P('dp', None)
    rep_spec = P()

    def per_device(x_rows, dy_rows, w_one, w_two, w_three, w_four, master_one, master_two, master_three, master_four, m_one, m_two, m_three, m_four, v_one, v_two, v_three, v_four, learn_rate, clip_max):
        grads = local_grads(x_rows, dy_rows, w_one, w_two, w_three, w_four)
        return sync_and_update(grads, (master_one, master_two, master_three, master_four), (m_one, m_two, m_three, m_four), (v_one, v_two, v_three, v_four), learn_rate, clip_max)

    in_specs = (row_spec, row_spec) + (rep_spec,) * 4 + (row_spec,) * 12 + (rep_spec, rep_spec)
    out_specs = (rep_spec,) * 4 + (row_spec,) * 12 + (rep_spec,)
    return jax.shard_map(per_device, mesh=mesh, in_specs=in_specs, out_specs=out_specs, check_vma=False)
```

```python
import functools

import jax
import jax.numpy as jnp
from jax import lax
from jax.experimental import pallas as pl
from jax.experimental.pallas import tpu as pltpu
from jax.sharding import PartitionSpec as P

ADAM_STEP = 10
BETA_ONE = 0.9
BETA_TWO = 0.95
ADAM_EPS = 1e-8
NORM_EPS = 1e-6
BIAS_ONE = 1.0 - BETA_ONE ** ADAM_STEP
BIAS_TWO = 1.0 - BETA_TWO ** ADAM_STEP
INV_SQRT2 = 0.7071067811865476
INV_SQRT2PI = 0.3989422804014327

WIDTH = 512
SIDE = 4
ROWS = 8
UNITS_OF = {3: 2, 4: 2, 2: 8, 1: 8}
MESH_ID = pl.DeviceIdType.MESH
BY_COLUMNS = (((1,), (1,)), ((), ()))
BY_ROWS = (((0,), (0,)), ((), ()))
VMEM_BYTES = 62 * 1024 * 1024
ADAM_VMEM = 8 * 1024 * 1024
WIDE_DEEP = 4


def unit_list():
    return [(mat, piece) for mat in (3, 4, 2, 1) for piece in range(UNITS_OF[mat])]


def first_unit(mat):
    return unit_list().index((mat, 0))


def gelu_value(pre_act):
    pre_wide = pre_act.astype(jnp.float32)
    return 0.5 * pre_wide * (1.0 + lax.erf(pre_wide * INV_SQRT2))


def gelu_slope(pre_act):
    pre_wide = pre_act.astype(jnp.float32)
    return 0.5 * (1.0 + lax.erf(pre_wide * INV_SQRT2)) + pre_wide * INV_SQRT2PI * jnp.exp(-0.5 * pre_wide * pre_wide)


def forward_kernel(x_ref, w_one, w_two, z_out, a_turned, h_out, x_turned, total):
    step = pl.program_id(0)

    @pl.when(step == 0)
    def _():
        total[...] = jnp.zeros_like(total)
        x_turned[...] = x_ref[...].T

    z_one = jnp.dot(x_ref[...], w_one[...], preferred_element_type=jnp.float32).astype(jnp.bfloat16)
    z_out[...] = z_one
    a_one = gelu_value(z_one).astype(jnp.bfloat16)
    a_turned[...] = a_one.T
    total[...] += jnp.dot(a_one, w_two[...], preferred_element_type=jnp.float32)

    @pl.when(step == pl.num_programs(0) - 1)
    def _():
        h_out[...] = total[...].astype(jnp.bfloat16)


def forward_wide(x_rows, w_one, w_two):
    rows, dim = x_rows.shape
    wide = w_one.shape[1]
    block = 1024
    bf16 = jnp.bfloat16
    return pl.pallas_call(
        forward_kernel,
        grid=(wide // block,),
        out_shape=(jax.ShapeDtypeStruct((rows, wide), bf16), jax.ShapeDtypeStruct((wide, rows), bf16), jax.ShapeDtypeStruct((rows, dim), bf16), jax.ShapeDtypeStruct((dim, rows), bf16)),
        in_specs=[pl.BlockSpec((rows, dim), whole_at), pl.BlockSpec((dim, block), across_at), pl.BlockSpec((block, dim), down_at)],
        out_specs=(pl.BlockSpec((rows, block), across_at), pl.BlockSpec((block, rows), down_at), pl.BlockSpec((rows, dim), whole_at), pl.BlockSpec((dim, rows), whole_at)),
        scratch_shapes=[pltpu.VMEM((rows, dim), jnp.float32)],
        compiler_params=pltpu.CompilerParams(vmem_limit_bytes=VMEM_BYTES),
        name='forward_wide',
    )(x_rows, w_one, w_two)


def middle_kernel(h_ref, dy_ref, w_three, w_four, g_three, g_four, dh_out, total, h_turned):
    step = pl.program_id(0)
    f32, bf16 = jnp.float32, jnp.bfloat16

    @pl.when(step == 0)
    def _():
        total[...] = jnp.zeros_like(total)
        h_turned[...] = h_ref[...].T

    z_three = jnp.dot(h_ref[...], w_three[...], preferred_element_type=f32).astype(bf16)
    a_three = gelu_value(z_three).astype(bf16)
    da_three = lax.dot_general(dy_ref[...], w_four[...], BY_COLUMNS, preferred_element_type=f32).astype(bf16)
    dz_three = (da_three.astype(f32) * gelu_slope(z_three)).astype(bf16)
    g_four[...] = lax.dot_general(a_three, dy_ref[...], BY_ROWS, preferred_element_type=f32)
    g_three[...] = jnp.dot(h_turned[...], dz_three, preferred_element_type=f32)
    total[...] += lax.dot_general(dz_three, w_three[...], BY_COLUMNS, preferred_element_type=f32)

    @pl.when(step == pl.num_programs(0) - 1)
    def _():
        dh_out[...] = total[...].astype(bf16)


def middle(h_two, dy_rows, w_three, w_four):
    rows, dim = h_two.shape
    wide = w_three.shape[1]
    block = 512
    f32, bf16 = jnp.float32, jnp.bfloat16
    whole = pl.BlockSpec((rows, dim), whole_at)
    across, down = pl.BlockSpec((dim, block), across_at), pl.BlockSpec((block, dim), down_at)
    return pl.pallas_call(
        middle_kernel,
        grid=(wide // block,),
        out_shape=(jax.ShapeDtypeStruct((dim, wide), f32), jax.ShapeDtypeStruct((wide, dim), f32), jax.ShapeDtypeStruct((rows, dim), bf16)),
        in_specs=[whole, whole, across, down],
        out_specs=(across, down, whole),
        scratch_shapes=[pltpu.VMEM((rows, dim), f32), pltpu.VMEM((dim, rows), bf16)],
        compiler_params=pltpu.CompilerParams(vmem_limit_bytes=VMEM_BYTES),
        name='middle',
    )(h_two, dy_rows, w_three, w_four)


def local_grads(x_rows, dy_rows, w_one, w_two, w_three, w_four):
    z_one, a_turned, h_two, x_turned = forward_wide(x_rows, w_one, w_two)
    g_three, g_four, dh_two = middle(h_two, dy_rows, w_three, w_four)
    g_two = jnp.dot(a_turned, dh_two, preferred_element_type=jnp.float32)
    return (x_turned, dh_two, z_one, w_two), g_two, g_three, g_four


def whole_at(step):
    return 0, 0


def across_at(step):
    return 0, step


def down_at(step):
    return step, 0


class Place:
    def __init__(self):
        me = lax.axis_index('dp')
        self.core = lax.rem(me, 2)
        self.coords = [lax.div(me, 2 * SIDE * SIDE), lax.rem(lax.div(me, 2 * SIDE), SIDE), lax.rem(lax.div(me, 2), SIDE)]

    def step(self, axis, by):
        return lax.rem(self.coords[axis] + by, SIDE)

    def device(self, moves=None, other_core=False):
        pos = list(self.coords)
        for axis, by in (moves or {}).items():
            pos[axis] = self.step(axis, by)
        core = 1 - self.core if other_core else self.core
        return (((pos[0] * SIDE + pos[1]) * SIDE + pos[2]) * 2 + core,)

    def neighbours(self):
        found = [self.device(other_core=True)]
        for axis in range(3):
            found += [self.device({axis: 1}), self.device({axis: SIDE - 1})]
        return found


def enter(peers):
    barrier = pltpu.get_barrier_semaphore()
    for peer in peers:
        pl.semaphore_signal(barrier, inc=1, device_id=peer, device_id_type=MESH_ID)
    pl.semaphore_wait(barrier, len(peers))


def send(src, dst, send_sem, recv_sem, peer):
    pltpu.make_async_remote_copy(src_ref=src, dst_ref=dst, send_sem=send_sem, recv_sem=recv_sem, device_id=peer, device_id_type=MESH_ID).start()


def await_bytes(ref, sem):
    pltpu.make_async_copy(ref, ref, sem).wait()


def spot(lead, dims, fixed, cols):
    return tuple(lead) + tuple(fixed.get(axis, slice(None)) for axis in dims) + (slice(None), cols)


LEFT = pl.ds(0, WIDTH // 2)
RIGHT = pl.ds(WIDTH // 2, WIDTH // 2)
ALL = slice(None)


class RingSum:
    def __init__(self, place, dims, axis, relay, final, relay_sem, final_sem, send_sem):
        self.place, self.dims, self.axis = place, dims, axis
        self.relay, self.final = relay, final
        self.relay_sem, self.final_sem, self.send_sem = relay_sem, final_sem, send_sem
        self.own = place.coords[axis]
        self.up, self.down, self.far = place.step(axis, 1), place.step(axis, SIDE - 1), place.step(axis, 2)
        self.up_dev, self.down_dev = place.device({axis: 1}), place.device({axis: SIDE - 1})
        self.rest = [dim for dim in dims if dim != axis]

    def start(self, src, lead, unit):
        s = self
        send(src.at[spot(lead, s.dims, {s.axis: s.far}, LEFT)], s.relay.at[unit, 0], s.send_sem.at[unit], s.relay_sem.at[unit], s.up_dev)
        send(src.at[spot(lead, s.dims, {s.axis: s.far}, RIGHT)], s.relay.at[unit, 1], s.send_sem.at[unit], s.relay_sem.at[unit], s.down_dev)
        send(src.at[spot(lead, s.dims, {s.axis: s.up}, RIGHT)], s.final.at[spot((unit, 0), s.rest, {}, RIGHT)], s.send_sem.at[unit], s.final_sem.at[unit], s.up_dev)
        send(src.at[spot(lead, s.dims, {s.axis: s.down}, LEFT)], s.final.at[spot((unit, 1), s.rest, {}, LEFT)], s.send_sem.at[unit], s.final_sem.at[unit], s.down_dev)

    def pass_on(self, src, lead, unit):
        s = self
        await_bytes(s.relay.at[unit], s.relay_sem.at[unit])
        up_spot = spot(lead, s.dims, {s.axis: s.up}, LEFT)
        src[up_spot] = src[up_spot] + s.relay[unit, 0]
        send(src.at[up_spot], s.final.at[spot((unit, 0), s.rest, {}, LEFT)], s.send_sem.at[unit], s.final_sem.at[unit], s.up_dev)
        down_spot = spot(lead, s.dims, {s.axis: s.down}, RIGHT)
        src[down_spot] = src[down_spot] + s.relay[unit, 1]
        send(src.at[down_spot], s.final.at[spot((unit, 1), s.rest, {}, RIGHT)], s.send_sem.at[unit], s.final_sem.at[unit], s.down_dev)

    def finish(self, src, lead, unit):
        s = self
        await_bytes(s.final.at[unit], s.final_sem.at[unit])
        return src[spot(lead, s.dims, {s.axis: s.own}, ALL)] + s.final[unit, 0] + s.final[unit, 1]

    def drain(self, unit):
        await_bytes(self.relay.at[unit], self.send_sem.at[unit])
        await_bytes(self.final.at[unit], self.send_sem.at[unit])


BLOCK = 256
BLOCKS_PER_UNIT = 2 * (WIDTH // BLOCK)
BLOCKS_AFTER = (2, 2, 1)


def reduce_kernel(x_turned, dh_two, z_one, w_two, g_two, g_three, g_four, shard, swapped, norm_tile, own, wide_own, part, relay1, final1, relay2, final2, relay3, final3, norm_own, norm_a, norm_b, norm_c, x_buf, dh_buf, z_buf, w_buf, out_buf, load_sem, part_send, part_recv, ring_sems, swap_sems, norm_sems, fetch_sems, out_sems):
    place = Place()
    units = unit_list()
    chunks = -(-len(units) // 3)
    counts = [len(range(order, len(units), 3)) for order in range(3)]
    wide_base = first_unit(1)
    wide_units = UNITS_OF[1]
    wide_half = wide_units * WIDTH
    pieces = WIDTH // BLOCK
    blocks = wide_units * BLOCKS_PER_UNIT
    partner = place.device(other_core=True)
    group_x = [(place.device({2: by}, other_core=swap)) for by in range(SIDE) for swap in (False, True) if by or swap]
    group_y = [place.device({1: by}) for by in range(1, SIDE)]
    group_z = [place.device({0: by}) for by in range(1, SIDE)]

    def block_start(block):
        unit = lax.div(block, BLOCKS_PER_UNIT)
        mine = lax.rem(lax.div(block, pieces), 2)
        owner = lax.rem(place.core + 1 + mine, 2)
        start = owner * wide_half + unit * WIDTH + lax.rem(block, pieces) * BLOCK
        return pl.multiple_of(start, BLOCK)

    def fetch(block):
        slot = lax.rem(block, WIDE_DEEP)
        start = block_start(block)
        return (
            pltpu.make_async_copy(z_one.at[:, pl.ds(start, BLOCK)], z_buf.at[slot], fetch_sems.at[0, slot]),
            pltpu.make_async_copy(w_two.at[pl.ds(start, BLOCK), :], w_buf.at[slot], fetch_sems.at[1, slot]),
        )

    steady = (pltpu.make_async_copy(x_turned, x_buf, fetch_sems.at[2, 0]), pltpu.make_async_copy(dh_two, dh_buf, fetch_sems.at[2, 1]))
    for copy in steady:
        copy.start()
    for block in range(WIDE_DEEP - 1):
        for copy in fetch(block):
            copy.start()
    enter(group_x + group_y + group_z)

    def source(mat, piece, core):
        if mat == 3:
            start = core * (UNITS_OF[mat] * WIDTH) + piece * WIDTH
            return g_three.at[:, :, :, :, pl.ds(pl.multiple_of(start, WIDTH), WIDTH)]
        ref = g_two if mat == 2 else g_four
        return ref.at[:, :, :, core, pl.ds(piece * ROWS, ROWS), :]

    def sems_of(level):
        return [ring_sems.at[level, kind] for kind in range(3)]

    rings = []
    for order in range(3):
        a, b = order, (order + 1) % 3
        c = (order + 2) % 3
        first = RingSum(place, [0, 1, 2], a, relay1, final1, *sems_of(0))
        second = RingSum(place, first.rest, b, relay2, final2, *sems_of(1))
        third = RingSum(place, second.rest, c, relay3, final3, *sems_of(2))
        rings.append((first, second, third))

    def load(chunk):
        for order in range(3):
            unit = 3 * chunk + order
            if unit >= wide_base:
                continue
            mat, piece = units[unit]
            send(source(mat, piece, 1 - place.core), part.at[unit], part_send.at[unit], part_recv.at[unit], partner)
            pltpu.make_async_copy(source(mat, piece, place.core), own.at[order], load_sem.at[unit]).start()

    def wide_block(block, carry):
        slot = lax.rem(block, WIDE_DEEP)

        @pl.when(block + WIDE_DEEP - 1 < blocks)
        def _():
            for copy in fetch(block + WIDE_DEEP - 1):
                copy.start()

        for copy in fetch(block):
            copy.wait()
        da_one = lax.dot_general(dh_buf[...], w_buf[slot], BY_COLUMNS, preferred_element_type=jnp.float32).astype(jnp.bfloat16)
        dz_one = (da_one.astype(jnp.float32) * gelu_slope(z_buf[slot])).astype(jnp.bfloat16)
        grad = jnp.dot(x_buf[...], dz_one, preferred_element_type=jnp.float32)
        grad = grad.reshape(SIDE, SIDE, SIDE, ROWS, BLOCK)
        unit = lax.div(block, BLOCKS_PER_UNIT)
        piece = lax.rem(block, pieces)
        mine = lax.rem(lax.div(block, pieces), 2)
        cols = pl.ds(pl.multiple_of(piece * BLOCK, BLOCK), BLOCK)

        @pl.when(mine == 1)
        def _():
            wide_own[unit, :, :, :, :, cols] = grad

        @pl.when(mine == 0)
        def _():
            @pl.when(unit > 0)
            def _():
                await_bytes(out_buf.at[piece], out_sems.at[piece])
            out_buf[piece] = grad
            send(out_buf.at[piece], part.at[wide_base + unit, :, :, :, :, cols], out_sems.at[piece], part_recv.at[wide_base + unit], partner)
        return carry

    def stage_b(order, chunk, unit):
        await_bytes(part.at[unit], part_recv.at[unit])

        @pl.when(unit < wide_base)
        def _():
            await_bytes(own.at[order], load_sem.at[unit])
            part[unit] = part[unit] + own[order]

        @pl.when(unit >= wide_base)
        def _():
            part[unit] = part[unit] + wide_own[unit - wide_base]
        rings[order][0].start(part, (unit,), unit)

    def stage_c(order, chunk, unit):
        rings[order][0].pass_on(part, (unit,), unit)

    def stage_d(order, chunk, unit):
        final1[unit, 0] = rings[order][0].finish(part, (unit,), unit)
        rings[order][1].start(final1, (unit, 0), unit)

    def stage_e(order, chunk, unit):
        rings[order][1].pass_on(final1, (unit, 0), unit)

    def stage_f(order, chunk, unit):
        final2[unit, 0] = rings[order][1].finish(final1, (unit, 0), unit)
        rings[order][2].start(final2, (unit, 0), unit)

    def stage_g(order, chunk, unit):
        rings[order][2].pass_on(final2, (unit, 0), unit)

    def stage_h(order, chunk, unit):
        shard[unit] = rings[order][2].finish(final2, (unit, 0), unit) * (1.0 / (2 * SIDE ** 3))

    stages = (stage_b, stage_c, stage_d, stage_e, stage_f, stage_g, stage_h)

    def run(now, lag):
        chunk = now - lag - 1
        for order in range(3):
            @pl.when((chunk >= 0) & (chunk < counts[order]))
            def _(order=order):
                stages[lag](order, chunk, 3 * chunk + order)

    def wide_blocks(low, count):
        lax.fori_loop(lax.min(low, blocks), lax.min(low + count, blocks), wide_block, 0)

    load(0)
    for copy in steady:
        copy.wait()
    first_blocks = 6
    wide_blocks(0, first_blocks)

    def turn(now, carry):
        run(now, 0)
        for chunk in range(1, chunks):
            if 3 * chunk < wide_base:
                @pl.when(now == chunk)
                def _(chunk=chunk):
                    load(chunk)
        done = first_blocks + (now - 1) * sum(BLOCKS_AFTER)
        for lag in range(1, len(stages)):
            if lag <= len(BLOCKS_AFTER):
                wide_blocks(done, BLOCKS_AFTER[lag - 1])
                done = done + BLOCKS_AFTER[lag - 1]
            run(now, lag)
        return carry

    lax.fori_loop(1, chunks + len(stages), turn, 0)

    n_three = UNITS_OF[3]
    send(shard.at[pl.ds(0, n_three)], swapped.at[pl.ds(0, n_three)], swap_sems.at[0], swap_sems.at[1], partner)
    send(shard.at[pl.ds(wide_base, wide_units)], swapped.at[pl.ds(n_three, wide_units)], swap_sems.at[0], swap_sems.at[1], partner)

    def fold(unit, total):
        value = shard[unit]
        return total + value * value

    squares = lax.fori_loop(0, len(units), fold, jnp.zeros((ROWS, WIDTH), jnp.float32))
    total = squares[:, 0:128]
    for col in range(1, WIDTH // 128):
        total = total + squares[:, col * 128:(col + 1) * 128]
    levels = ((norm_a, group_x, place.coords[2] * 2 + place.core), (norm_b, group_y, place.coords[1]), (norm_c, group_z, place.coords[0]))
    for level, (board, group, seat) in enumerate(levels):
        norm_own[level] = total
        board[seat] = total
        for peer in group:
            send(norm_own.at[level], board.at[seat], norm_sems.at[0, level], norm_sems.at[1, level], peer)
        await_bytes(board.at[pl.ds(0, len(group))], norm_sems.at[1, level])
        total = board[0]
        for row in range(1, len(group) + 1):
            total = total + board[row]
    norm_tile[...] = total

    await_bytes(swapped, swap_sems.at[0])
    await_bytes(swapped, swap_sems.at[1])
    for level, (board, group, seat) in enumerate(levels):
        await_bytes(board.at[pl.ds(0, len(group))], norm_sems.at[0, level])
    for piece in range(pieces):
        await_bytes(out_buf.at[piece], out_sems.at[piece])
    for order in range(3):
        def tidy(chunk, carry, order=order):
            unit = 3 * chunk + order
            for ring in rings[order]:
                ring.drain(unit)

            @pl.when(unit < wide_base)
            def _():
                await_bytes(part.at[unit], part_send.at[unit])
            return carry

        lax.fori_loop(0, counts[order], tidy, 0)


def reduce_grads(wide_parts, g_two, g_three, g_four):
    n = len(unit_list())
    cube = (SIDE, SIDE, SIDE)
    args = tuple(wide_parts) + (
        g_two.reshape(cube + (2, UNITS_OF[2] * ROWS, WIDTH)),
        g_three.reshape(cube + (ROWS, 2 * UNITS_OF[3] * WIDTH)),
        g_four.reshape(cube + (2, UNITS_OF[4] * ROWS, WIDTH)),
    )
    f32, bf16 = jnp.float32, jnp.bfloat16
    dma = pltpu.SemaphoreType.DMA
    dim, rows = wide_parts[0].shape
    model = wide_parts[1].shape[1]
    scratch = [
        pltpu.VMEM((3,) + cube + (ROWS, WIDTH), f32),
        pltpu.VMEM((UNITS_OF[1],) + cube + (ROWS, WIDTH), f32),
        pltpu.VMEM((n,) + cube + (ROWS, WIDTH), f32),
        pltpu.VMEM((n, 2, SIDE, SIDE, ROWS, WIDTH // 2), f32),
        pltpu.VMEM((n, 2, SIDE, SIDE, ROWS, WIDTH), f32),
        pltpu.VMEM((n, 2, SIDE, ROWS, WIDTH // 2), f32),
        pltpu.VMEM((n, 2, SIDE, ROWS, WIDTH), f32),
        pltpu.VMEM((n, 2, ROWS, WIDTH // 2), f32),
        pltpu.VMEM((n, 2, ROWS, WIDTH), f32),
        pltpu.VMEM((3, ROWS, 128), f32),
        pltpu.VMEM((2 * SIDE, ROWS, 128), f32),
        pltpu.VMEM((SIDE, ROWS, 128), f32),
        pltpu.VMEM((SIDE, ROWS, 128), f32),
        pltpu.VMEM((dim, rows), bf16),
        pltpu.VMEM((rows, model), bf16),
        pltpu.VMEM((WIDE_DEEP, rows, BLOCK), bf16),
        pltpu.VMEM((WIDE_DEEP, BLOCK, model), bf16),
        pltpu.VMEM((WIDTH // BLOCK,) + cube + (ROWS, BLOCK), f32),
        dma((n,)), dma((n,)), dma((n,)), dma((3, 3, n)), dma((2,)), dma((2, 3)), dma((3, WIDE_DEEP)), dma((WIDTH // BLOCK,)),
    ]
    any_spec = pl.BlockSpec(memory_space=pl.ANY)
    vmem_spec = pl.BlockSpec(memory_space=pltpu.VMEM)
    return pl.pallas_call(
        reduce_kernel,
        out_shape=(
            jax.ShapeDtypeStruct((n, ROWS, WIDTH), f32),
            jax.ShapeDtypeStruct((UNITS_OF[3] + UNITS_OF[1], ROWS, WIDTH), f32),
            jax.ShapeDtypeStruct((ROWS, 128), f32),
        ),
        in_specs=[any_spec] * len(args),
        out_specs=(vmem_spec,) * 3,
        scratch_shapes=scratch,
        compiler_params=pltpu.CompilerParams(collective_id=0, has_side_effects=True, vmem_limit_bytes=VMEM_BYTES),
        name='reduce_grads',
    )(*args)


def adam_kernel(lr_ref, clip_ref, norm_tile, shard, swapped, *refs):
    masters, moms, variances = refs[0:4], refs[4:8], refs[8:12]
    new_masters, new_moms, new_vars = refs[12:16], refs[16:20], refs[20:24]
    two_rows, four_rows, norm_ref = refs[24:27]
    core = lax.rem(lax.axis_index('dp'), 2)
    grad_norm = jnp.sqrt(jnp.sum(jnp.sum(norm_tile[...], axis=1, keepdims=True), axis=0, keepdims=True))
    norm_ref[...] = grad_norm
    clip_scale = jnp.minimum(1.0, clip_ref[...] / (grad_norm + NORM_EPS))
    learn_rate = lr_ref[...]

    def update(mat, where, grad):
        scaled = clip_scale * grad
        mom_new = BETA_ONE * moms[mat][where] + (1.0 - BETA_ONE) * scaled
        var_new = BETA_TWO * variances[mat][where] + (1.0 - BETA_TWO) * scaled * scaled
        master_new = masters[mat][where] - learn_rate * (mom_new / BIAS_ONE) / (jnp.sqrt(var_new / BIAS_TWO) + ADAM_EPS)
        new_moms[mat][where] = mom_new
        new_vars[mat][where] = var_new
        new_masters[mat][where] = master_new
        return master_new

    for mat, rows_out in ((2, two_rows), (4, four_rows)):
        for piece in range(UNITS_OF[mat]):
            where = (slice(piece * ROWS, (piece + 1) * ROWS), slice(None))
            rows_out[piece] = update(mat - 1, where, shard[first_unit(mat) + piece]).astype(jnp.bfloat16)
    for mat, base in ((3, 0), (1, UNITS_OF[3])):
        for half in range(2):
            for piece in range(UNITS_OF[mat]):
                col = (half * UNITS_OF[mat] + piece) * WIDTH
                where = (slice(None), slice(col, col + WIDTH))
                block = jnp.where(core == half, shard[first_unit(mat) + piece], swapped[base + piece])
                update(mat - 1, where, jnp.where(core == 0, block[0:ROWS // 2], block[ROWS // 2:ROWS]))


def adam_update(learn_rate, clip_max, norm_tile, shard, swapped, masters, moms, variances):
    state = list(masters) + list(moms) + list(variances)
    f32, bf16 = jnp.float32, jnp.bfloat16
    vmem_spec = pl.BlockSpec(memory_space=pltpu.VMEM)
    out_shape = [jax.ShapeDtypeStruct(part.shape, f32) for part in state]
    out_shape += [
        jax.ShapeDtypeStruct((UNITS_OF[2], ROWS, WIDTH), bf16),
        jax.ShapeDtypeStruct((UNITS_OF[4], ROWS, WIDTH), bf16),
        jax.ShapeDtypeStruct((1, 1), f32),
    ]
    args = [learn_rate.reshape(1, 1), clip_max.reshape(1, 1), norm_tile, shard, swapped] + state
    return pl.pallas_call(
        adam_kernel,
        out_shape=out_shape,
        in_specs=[vmem_spec] * len(args),
        out_specs=[vmem_spec] * len(out_shape),
        compiler_params=pltpu.CompilerParams(vmem_limit_bytes=ADAM_VMEM),
        name='adam_update',
    )(*args)


class RingSpread:
    def __init__(self, place, axis, known, board, near_sem, far_sem, send_sem):
        self.place, self.axis, self.known, self.board = place, axis, known, board
        self.near_sem, self.far_sem, self.send_sem = near_sem, far_sem, send_sem
        self.up_dev, self.down_dev = place.device({axis: 1}), place.device({axis: SIDE - 1})

    def block(self, unit, by, cols):
        fixed = {dim: self.place.coords[dim] for dim in range(3) if dim not in self.known}
        fixed[self.axis] = self.place.step(self.axis, by)
        return self.board.at[spot((unit,), [0, 1, 2], fixed, cols)]

    def blocks(self, unit, count):
        return self.board.at[(unit,) + (0,) * (2 - len(self.known)) + (pl.ds(0, count),)]

    def start(self, unit):
        s = self
        mine = s.block(unit, 0, ALL)
        send(mine, mine, s.send_sem.at[unit], s.near_sem.at[unit], s.up_dev)
        send(mine, mine, s.send_sem.at[unit], s.near_sem.at[unit], s.down_dev)

    def pass_on(self, unit):
        s = self
        await_bytes(s.blocks(unit, 2), s.near_sem.at[unit])
        from_down, from_up = s.block(unit, SIDE - 1, LEFT), s.block(unit, 1, RIGHT)
        send(from_down, from_down, s.send_sem.at[unit], s.far_sem.at[unit], s.up_dev)
        send(from_up, from_up, s.send_sem.at[unit], s.far_sem.at[unit], s.down_dev)

    def finish(self, unit):
        await_bytes(self.block(unit, 0, ALL), self.far_sem.at[unit])

    def drain(self, unit):
        await_bytes(self.blocks(unit, 3), self.send_sem.at[unit])


def gather_kernel(one_rows, three_rows, two_rows, four_rows, board, other, own_one, own_three, swap_one, swap_three, ring_sems, pair_sems, swap_sems, load_sems):
    place = Place()
    units = unit_list()
    chunks = -(-len(units) // 3)
    counts = [len(range(order, len(units), 3)) for order in range(3)]
    partner = place.device(other_core=True)
    here = tuple(place.coords)
    splits = ((1, one_rows, own_one, swap_one), (3, three_rows, own_three, swap_three))
    loads = []
    for index, (mat, rows, mine, landing) in enumerate(splits):
        span = UNITS_OF[mat] * WIDTH
        loads.append(pltpu.make_async_copy(rows.at[:, pl.ds(pl.multiple_of(place.core * span, WIDTH), span)], mine, load_sems.at[index]))
    for index, (mat, rows) in enumerate(((2, two_rows), (4, four_rows))):
        loads.append(pltpu.make_async_copy(rows, board.at[(pl.ds(first_unit(mat), UNITS_OF[mat]),) + here], load_sems.at[2 + index]))
    for copy in loads:
        copy.start()
    enter(place.neighbours())
    for index, (mat, rows, mine, landing) in enumerate(splits):
        span = UNITS_OF[mat] * WIDTH
        theirs = rows.at[:, pl.ds(pl.multiple_of((1 - place.core) * span, WIDTH), span)]
        send(theirs, landing, swap_sems.at[0, index], swap_sems.at[1, index], partner)
    for copy in loads:
        copy.wait()
    for index, (mat, rows, mine, landing) in enumerate(splits):
        await_bytes(landing, swap_sems.at[1, index])
        for piece in range(UNITS_OF[mat]):
            cols = slice(piece * WIDTH, (piece + 1) * WIDTH)
            top = jnp.where(place.core == 0, mine[:, cols], landing[:, cols])
            bottom = jnp.where(place.core == 0, landing[:, cols], mine[:, cols])
            board[(first_unit(mat) + piece,) + here] = jnp.concatenate([top, bottom], axis=0).astype(board.dtype)

    rings = []
    for order in range(3):
        axes = (order + 2) % 3, (order + 1) % 3, order
        rings.append([RingSpread(place, axis, axes[:level], board, *[ring_sems.at[level, kind] for kind in range(3)]) for level, axis in enumerate(axes)])

    def begin(order, unit, level):
        if level:
            rings[order][level - 1].finish(unit)
        rings[order][level].start(unit)

    def pass_on(order, unit, level):
        rings[order][level].pass_on(unit)

    def hand_over(order, unit, level):
        rings[order][level].finish(unit)
        send(board.at[unit], other.at[unit], pair_sems.at[0, unit], pair_sems.at[1, unit], partner)

    def tidy(order, unit, level):
        await_bytes(other.at[unit], pair_sems.at[1, unit])
        await_bytes(board.at[unit], pair_sems.at[0, unit])
        for ring in rings[order]:
            ring.drain(unit)

    stages = ((begin, 0), (pass_on, 0), (begin, 1), (pass_on, 1), (begin, 2), (pass_on, 2), (hand_over, 2), (tidy, 2))

    def turn(now, carry):
        for lag, (stage, level) in enumerate(stages):
            chunk = now - lag
            for order in range(3):
                @pl.when((chunk >= 0) & (chunk < counts[order]))
                def _(stage=stage, level=level, chunk=chunk, order=order):
                    stage(order, 3 * chunk + order, level)
        return carry

    lax.fori_loop(0, chunks + len(stages) - 1, turn, 0)
    for index, (mat, rows, mine, landing) in enumerate(splits):
        await_bytes(landing, swap_sems.at[0, index])


def gather_rows(one_rows, three_rows, two_rows, four_rows):
    n = len(unit_list())
    cube = (SIDE, SIDE, SIDE)
    bf16, f32 = jnp.bfloat16, jnp.float32
    dma = pltpu.SemaphoreType.DMA
    vmem_spec = pl.BlockSpec(memory_space=pltpu.VMEM)
    full = jax.ShapeDtypeStruct((n,) + cube + (ROWS, WIDTH), bf16)
    return pl.pallas_call(
        gather_kernel,
        out_shape=(full, full),
        in_specs=[pl.BlockSpec(memory_space=pltpu.HBM)] * 4,
        out_specs=(vmem_spec, vmem_spec),
        scratch_shapes=[
            pltpu.VMEM((ROWS // 2, UNITS_OF[1] * WIDTH), f32),
            pltpu.VMEM((ROWS // 2, UNITS_OF[3] * WIDTH), f32),
            pltpu.VMEM((ROWS // 2, UNITS_OF[1] * WIDTH), f32),
            pltpu.VMEM((ROWS // 2, UNITS_OF[3] * WIDTH), f32),
            dma((3, 3, n)), dma((2, n)), dma((2, 2)), dma((4,)),
        ],
        compiler_params=pltpu.CompilerParams(collective_id=1, has_side_effects=True, vmem_limit_bytes=32 * 1024 * 1024),
        name='gather_rows',
    )(one_rows, three_rows, two_rows, four_rows)


def place_kernel(board, other, w_one, w_two, w_three, w_four, sems):
    core = lax.rem(lax.axis_index('dp'), 2)
    outs = {1: w_one, 2: w_two, 3: w_three, 4: w_four}
    copies = []
    for unit, (mat, piece) in enumerate(unit_list()):
        for index, (source, owner) in enumerate(((board, core), (other, 1 - core))):
            if mat in (1, 3):
                start = owner * (UNITS_OF[mat] * WIDTH) + piece * WIDTH
                target = outs[mat].at[:, :, :, :, pl.ds(pl.multiple_of(start, WIDTH), WIDTH)]
            else:
                target = outs[mat].at[:, :, :, owner, pl.ds(piece * ROWS, ROWS), :]
            copies.append(pltpu.make_async_copy(source.at[unit], target, sems.at[index, unit]))
    for copy in copies:
        copy.start()
    for copy in copies:
        copy.wait()


def place_weights(board, other):
    n = len(unit_list())
    cube = (SIDE, SIDE, SIDE)
    bf16 = jnp.bfloat16
    vmem_spec = pl.BlockSpec(memory_space=pltpu.VMEM)
    any_spec = pl.BlockSpec(memory_space=pl.ANY)
    outs = pl.pallas_call(
        place_kernel,
        out_shape=(
            jax.ShapeDtypeStruct(cube + (ROWS, 2 * UNITS_OF[1] * WIDTH), bf16),
            jax.ShapeDtypeStruct(cube + (2, UNITS_OF[2] * ROWS, WIDTH), bf16),
            jax.ShapeDtypeStruct(cube + (ROWS, 2 * UNITS_OF[3] * WIDTH), bf16),
            jax.ShapeDtypeStruct(cube + (2, UNITS_OF[4] * ROWS, WIDTH), bf16),
        ),
        in_specs=[vmem_spec] * 2,
        out_specs=(any_spec,) * 4,
        scratch_shapes=[pltpu.SemaphoreType.DMA((2, n))],
        compiler_params=pltpu.CompilerParams(vmem_limit_bytes=2 * 1024 * 1024),
        name='place_weights',
    )(board, other)
    rows = SIDE ** 3 * ROWS
    return (
        outs[0].reshape(rows, 2 * UNITS_OF[1] * WIDTH),
        outs[1].reshape(2 * SIDE ** 3 * UNITS_OF[2] * ROWS, WIDTH),
        outs[2].reshape(rows, 2 * UNITS_OF[3] * WIDTH),
        outs[3].reshape(2 * SIDE ** 3 * UNITS_OF[4] * ROWS, WIDTH),
    )


def sync_and_update(grads, masters, moms, variances, learn_rate, clip_max):
    shard, swapped, norm_tile = reduce_grads(*grads)
    results = adam_update(learn_rate, clip_max, norm_tile, shard, swapped, masters, moms, variances)
    new_masters, new_moms, new_vars = results[0:4], results[4:8], results[8:12]
    two_rows, four_rows, grad_norm = results[12:15]
    board, other = gather_rows(new_masters[0], new_masters[2], two_rows, four_rows)
    new_weights = place_weights(board, other)
    return tuple(new_weights) + tuple(new_masters) + tuple(new_moms) + tuple(new_vars) + (grad_norm.reshape(()),)


def solution(mesh):
    row_spec = P('dp', None)
    rep_spec = P()

    def per_device(x_rows, dy_rows, w_one, w_two, w_three, w_four, master_one, master_two, master_three, master_four, m_one, m_two, m_three, m_four, v_one, v_two, v_three, v_four, learn_rate, clip_max):
        grads = local_grads(x_rows, dy_rows, w_one, w_two, w_three, w_four)
        return sync_and_update(grads, (master_one, master_two, master_three, master_four), (m_one, m_two, m_three, m_four), (v_one, v_two, v_three, v_four), learn_rate, clip_max)

    in_specs = (row_spec, row_spec) + (rep_spec,) * 4 + (row_spec,) * 12 + (rep_spec, rep_spec)
    out_specs = (rep_spec,) * 4 + (row_spec,) * 12 + (rep_spec,)
    return jax.shard_map(per_device, mesh=mesh, in_specs=in_specs, out_specs=out_specs, check_vma=False)
```

```python
import functools

import jax
import jax.numpy as jnp
from jax import lax
from jax.experimental import pallas as pl
from jax.experimental.pallas import tpu as pltpu
from jax.sharding import PartitionSpec as P

ADAM_STEP = 10
BETA_ONE = 0.9
BETA_TWO = 0.95
ADAM_EPS = 1e-8
NORM_EPS = 1e-6
BIAS_ONE = 1.0 - BETA_ONE ** ADAM_STEP
BIAS_TWO = 1.0 - BETA_TWO ** ADAM_STEP
INV_SQRT2 = 0.7071067811865476
INV_SQRT2PI = 0.3989422804014327

WIDTH = 512
SIDE = 4
ROWS = 8
UNITS_OF = {3: 2, 4: 2, 2: 8, 1: 8}
MESH_ID = pl.DeviceIdType.MESH
BY_COLUMNS = (((1,), (1,)), ((), ()))
BY_ROWS = (((0,), (0,)), ((), ()))
VMEM_BYTES = 62 * 1024 * 1024
ADAM_VMEM = 8 * 1024 * 1024
WIDE_DEEP = 4


def unit_list():
    return [(mat, piece) for mat in (4, 2, 3, 1) for piece in range(UNITS_OF[mat])]


def first_unit(mat):
    return unit_list().index((mat, 0))


def gelu_value(pre_act):
    pre_wide = pre_act.astype(jnp.float32)
    return 0.5 * pre_wide * (1.0 + lax.erf(pre_wide * INV_SQRT2))


def gelu_slope(pre_act):
    pre_wide = pre_act.astype(jnp.float32)
    return 0.5 * (1.0 + lax.erf(pre_wide * INV_SQRT2)) + pre_wide * INV_SQRT2PI * jnp.exp(-0.5 * pre_wide * pre_wide)


def forward_kernel(x_ref, w_one, w_two, z_out, a_turned, h_out, x_turned, total):
    step = pl.program_id(0)

    @pl.when(step == 0)
    def _():
        total[...] = jnp.zeros_like(total)
        x_turned[...] = x_ref[...].T

    z_one = jnp.dot(x_ref[...], w_one[...], preferred_element_type=jnp.float32).astype(jnp.bfloat16)
    z_out[...] = z_one
    a_one = gelu_value(z_one).astype(jnp.bfloat16)
    a_turned[...] = a_one.T
    total[...] += jnp.dot(a_one, w_two[...], preferred_element_type=jnp.float32)

    @pl.when(step == pl.num_programs(0) - 1)
    def _():
        h_out[...] = total[...].astype(jnp.bfloat16)


def forward_wide(x_rows, w_one, w_two):
    rows, dim = x_rows.shape
    wide = w_one.shape[1]
    block = 1024
    bf16 = jnp.bfloat16
    return pl.pallas_call(
        forward_kernel,
        grid=(wide // block,),
        out_shape=(jax.ShapeDtypeStruct((rows, wide), bf16), jax.ShapeDtypeStruct((wide, rows), bf16), jax.ShapeDtypeStruct((rows, dim), bf16), jax.ShapeDtypeStruct((dim, rows), bf16)),
        in_specs=[pl.BlockSpec((rows, dim), whole_at), pl.BlockSpec((dim, block), across_at), pl.BlockSpec((block, dim), down_at)],
        out_specs=(pl.BlockSpec((rows, block), across_at), pl.BlockSpec((block, rows), down_at), pl.BlockSpec((rows, dim), whole_at), pl.BlockSpec((dim, rows), whole_at)),
        scratch_shapes=[pltpu.VMEM((rows, dim), jnp.float32)],
        compiler_params=pltpu.CompilerParams(vmem_limit_bytes=VMEM_BYTES),
        name='forward_wide',
    )(x_rows, w_one, w_two)


NARROW_STEPS = 4
TALL_STEPS = 8


def middle_kernel(h_ref, dy_ref, w_three, w_four, a_turned, g_three, g_four, g_two, dh_out, total, h_turned):
    step = pl.program_id(0)
    f32, bf16 = jnp.float32, jnp.bfloat16

    @pl.when(step == 0)
    def _():
        total[...] = jnp.zeros_like(total)
        h_turned[...] = h_ref[...].T

    @pl.when(step < NARROW_STEPS)
    def _():
        z_three = jnp.dot(h_ref[...], w_three[...], preferred_element_type=f32).astype(bf16)
        a_three = gelu_value(z_three).astype(bf16)
        da_three = lax.dot_general(dy_ref[...], w_four[...], BY_COLUMNS, preferred_element_type=f32).astype(bf16)
        dz_three = (da_three.astype(f32) * gelu_slope(z_three)).astype(bf16)
        g_four[...] = lax.dot_general(a_three, dy_ref[...], BY_ROWS, preferred_element_type=f32)
        g_three[...] = jnp.dot(h_turned[...], dz_three, preferred_element_type=f32)
        total[...] += lax.dot_general(dz_three, w_three[...], BY_COLUMNS, preferred_element_type=f32)

    @pl.when(step == NARROW_STEPS - 1)
    def _():
        dh_out[...] = total[...].astype(bf16)

    @pl.when(step >= NARROW_STEPS)
    def _():
        g_two[...] = jnp.dot(a_turned[...], dh_out[...], preferred_element_type=f32)


def narrow_across(step):
    return across_at(jnp.minimum(step, NARROW_STEPS - 1))


def narrow_down(step):
    return down_at(jnp.minimum(step, NARROW_STEPS - 1))


def tall_down(step):
    return down_at(jnp.maximum(step - NARROW_STEPS, 0))


def middle(h_two, dy_rows, w_three, w_four, a_turned):
    rows, dim = h_two.shape
    wide, tall = w_three.shape[1], a_turned.shape[0]
    block, tall_block = wide // NARROW_STEPS, tall // TALL_STEPS
    f32, bf16 = jnp.float32, jnp.bfloat16
    whole = pl.BlockSpec((rows, dim), whole_at)
    across, down = pl.BlockSpec((dim, block), narrow_across), pl.BlockSpec((block, dim), narrow_down)
    return pl.pallas_call(
        middle_kernel,
        grid=(NARROW_STEPS + TALL_STEPS,),
        out_shape=(jax.ShapeDtypeStruct((dim, wide), f32), jax.ShapeDtypeStruct((wide, dim), f32), jax.ShapeDtypeStruct((tall, dim), f32), jax.ShapeDtypeStruct((rows, dim), bf16)),
        in_specs=[whole, whole, across, down, pl.BlockSpec((tall_block, rows), tall_down)],
        out_specs=(across, down, pl.BlockSpec((tall_block, dim), tall_down), whole),
        scratch_shapes=[pltpu.VMEM((rows, dim), f32), pltpu.VMEM((dim, rows), bf16)],
        compiler_params=pltpu.CompilerParams(vmem_limit_bytes=VMEM_BYTES),
        name='middle',
    )(h_two, dy_rows, w_three, w_four, a_turned)


def local_grads(x_rows, dy_rows, w_one, w_two, w_three, w_four):
    z_one, a_turned, h_two, x_turned = forward_wide(x_rows, w_one, w_two)
    g_three, g_four, g_two, dh_two = middle(h_two, dy_rows, w_three, w_four, a_turned)
    return (x_turned, dh_two, z_one, w_two), g_two, g_three, g_four


def whole_at(step):
    return 0, 0


def across_at(step):
    return 0, step


def down_at(step):
    return step, 0


class Place:
    def __init__(self):
        me = lax.axis_index('dp')
        self.core = lax.rem(me, 2)
        self.coords = [lax.div(me, 2 * SIDE * SIDE), lax.rem(lax.div(me, 2 * SIDE), SIDE), lax.rem(lax.div(me, 2), SIDE)]

    def step(self, axis, by):
        return lax.rem(self.coords[axis] + by, SIDE)

    def device(self, moves=None, other_core=False):
        pos = list(self.coords)
        for axis, by in (moves or {}).items():
            pos[axis] = self.step(axis, by)
        core = 1 - self.core if other_core else self.core
        return (((pos[0] * SIDE + pos[1]) * SIDE + pos[2]) * 2 + core,)

    def neighbours(self):
        found = [self.device(other_core=True)]
        for axis in range(3):
            found += [self.device({axis: 1}), self.device({axis: SIDE - 1})]
        return found


def enter(peers):
    barrier = pltpu.get_barrier_semaphore()
    for peer in peers:
        pl.semaphore_signal(barrier, inc=1, device_id=peer, device_id_type=MESH_ID)
    pl.semaphore_wait(barrier, len(peers))


def send(src, dst, send_sem, recv_sem, peer):
    pltpu.make_async_remote_copy(src_ref=src, dst_ref=dst, send_sem=send_sem, recv_sem=recv_sem, device_id=peer, device_id_type=MESH_ID).start()


def await_bytes(ref, sem):
    pltpu.make_async_copy(ref, ref, sem).wait()


def spot(lead, dims, fixed, cols):
    return tuple(lead) + tuple(fixed.get(axis, slice(None)) for axis in dims) + (slice(None), cols)


LEFT = pl.ds(0, WIDTH // 2)
RIGHT = pl.ds(WIDTH // 2, WIDTH // 2)
ALL = slice(None)


class RingSum:
    def __init__(self, place, dims, axis, relay, final, relay_sem, final_sem, send_sem):
        self.place, self.dims, self.axis = place, dims, axis
        self.relay, self.final = relay, final
        self.relay_sem, self.final_sem, self.send_sem = relay_sem, final_sem, send_sem
        self.own = place.coords[axis]
        self.up, self.down, self.far = place.step(axis, 1), place.step(axis, SIDE - 1), place.step(axis, 2)
        self.up_dev, self.down_dev = place.device({axis: 1}), place.device({axis: SIDE - 1})
        self.rest = [dim for dim in dims if dim != axis]

    def start(self, src, lead, unit):
        s = self
        send(src.at[spot(lead, s.dims, {s.axis: s.far}, LEFT)], s.relay.at[unit, 0], s.send_sem.at[unit], s.relay_sem.at[unit], s.up_dev)
        send(src.at[spot(lead, s.dims, {s.axis: s.far}, RIGHT)], s.relay.at[unit, 1], s.send_sem.at[unit], s.relay_sem.at[unit], s.down_dev)
        send(src.at[spot(lead, s.dims, {s.axis: s.up}, RIGHT)], s.final.at[spot((unit, 0), s.rest, {}, RIGHT)], s.send_sem.at[unit], s.final_sem.at[unit], s.up_dev)
        send(src.at[spot(lead, s.dims, {s.axis: s.down}, LEFT)], s.final.at[spot((unit, 1), s.rest, {}, LEFT)], s.send_sem.at[unit], s.final_sem.at[unit], s.down_dev)

    def pass_on(self, src, lead, unit):
        s = self
        await_bytes(s.relay.at[unit], s.relay_sem.at[unit])
        up_spot = spot(lead, s.dims, {s.axis: s.up}, LEFT)
        src[up_spot] = src[up_spot] + s.relay[unit, 0]
        send(src.at[up_spot], s.final.at[spot((unit, 0), s.rest, {}, LEFT)], s.send_sem.at[unit], s.final_sem.at[unit], s.up_dev)
        down_spot = spot(lead, s.dims, {s.axis: s.down}, RIGHT)
        src[down_spot] = src[down_spot] + s.relay[unit, 1]
        send(src.at[down_spot], s.final.at[spot((unit, 1), s.rest, {}, RIGHT)], s.send_sem.at[unit], s.final_sem.at[unit], s.down_dev)

    def finish(self, src, lead, unit):
        s = self
        await_bytes(s.final.at[unit], s.final_sem.at[unit])
        return src[spot(lead, s.dims, {s.axis: s.own}, ALL)] + s.final[unit, 0] + s.final[unit, 1]

    def drain(self, unit):
        await_bytes(self.relay.at[unit], self.send_sem.at[unit])
        await_bytes(self.final.at[unit], self.send_sem.at[unit])


BLOCK = 256
BLOCKS_PER_UNIT = 2 * (WIDTH // BLOCK)
BLOCKS_AFTER = (2, 2, 1)


def reduce_kernel(x_turned, dh_two, z_one, w_two, g_two, g_three, g_four, shard, own, wide_own, part, relay1, final1, relay2, final2, relay3, final3, norm_own, norm_a, norm_b, norm_c, x_buf, dh_buf, z_buf, w_buf, out_buf, load_sem, part_send, part_recv, ring_sems, swap_sems, norm_sems, fetch_sems, out_sems):
    place = Place()
    units = unit_list()
    chunks = -(-len(units) // 3)
    counts = [len(range(order, len(units), 3)) for order in range(3)]
    wide_base = first_unit(1)
    wide_units = UNITS_OF[1]
    wide_half = wide_units * WIDTH
    pieces = WIDTH // BLOCK
    blocks = wide_units * BLOCKS_PER_UNIT
    partner = place.device(other_core=True)
    group_x = [(place.device({2: by}, other_core=swap)) for by in range(SIDE) for swap in (False, True) if by or swap]
    group_y = [place.device({1: by}) for by in range(1, SIDE)]
    group_z = [place.device({0: by}) for by in range(1, SIDE)]

    def block_start(block):
        unit = lax.div(block, BLOCKS_PER_UNIT)
        mine = lax.rem(lax.div(block, pieces), 2)
        owner = lax.rem(place.core + 1 + mine, 2)
        start = owner * wide_half + unit * WIDTH + lax.rem(block, pieces) * BLOCK
        return pl.multiple_of(start, BLOCK)

    def fetch(block):
        slot = lax.rem(block, WIDE_DEEP)
        start = block_start(block)
        return (
            pltpu.make_async_copy(z_one.at[:, pl.ds(start, BLOCK)], z_buf.at[slot], fetch_sems.at[0, slot]),
            pltpu.make_async_copy(w_two.at[pl.ds(start, BLOCK), :], w_buf.at[slot], fetch_sems.at[1, slot]),
        )

    steady = (pltpu.make_async_copy(x_turned, x_buf, fetch_sems.at[2, 0]), pltpu.make_async_copy(dh_two, dh_buf, fetch_sems.at[2, 1]))
    for copy in steady:
        copy.start()
    for block in range(WIDE_DEEP - 1):
        for copy in fetch(block):
            copy.start()
    enter(group_x + group_y + group_z)

    def source(mat, piece, core):
        if mat == 3:
            start = core * (UNITS_OF[mat] * WIDTH) + piece * WIDTH
            return g_three.at[:, :, :, :, pl.ds(pl.multiple_of(start, WIDTH), WIDTH)]
        ref = g_two if mat == 2 else g_four
        return ref.at[:, :, :, core, pl.ds(piece * ROWS, ROWS), :]

    def sems_of(level):
        return [ring_sems.at[level, kind] for kind in range(3)]

    rings = []
    for order in range(3):
        a, b = order, (order + 1) % 3
        c = (order + 2) % 3
        first = RingSum(place, [0, 1, 2], a, relay1, final1, *sems_of(0))
        second = RingSum(place, first.rest, b, relay2, final2, *sems_of(1))
        third = RingSum(place, second.rest, c, relay3, final3, *sems_of(2))
        rings.append((first, second, third))

    def load(chunk):
        for order in range(3):
            unit = 3 * chunk + order
            if unit >= wide_base:
                continue
            mat, piece = units[unit]
            send(source(mat, piece, 1 - place.core), part.at[unit], part_send.at[unit], part_recv.at[unit], partner)
            pltpu.make_async_copy(source(mat, piece, place.core), own.at[order], load_sem.at[unit]).start()

    def wide_block(block, carry):
        slot = lax.rem(block, WIDE_DEEP)

        @pl.when(block + WIDE_DEEP - 1 < blocks)
        def _():
            for copy in fetch(block + WIDE_DEEP - 1):
                copy.start()

        for copy in fetch(block):
            copy.wait()
        da_one = lax.dot_general(dh_buf[...], w_buf[slot], BY_COLUMNS, preferred_element_type=jnp.float32).astype(jnp.bfloat16)
        dz_one = (da_one.astype(jnp.float32) * gelu_slope(z_buf[slot])).astype(jnp.bfloat16)
        grad = jnp.dot(x_buf[...], dz_one, preferred_element_type=jnp.float32)
        grad = grad.reshape(SIDE, SIDE, SIDE, ROWS, BLOCK)
        unit = lax.div(block, BLOCKS_PER_UNIT)
        piece = lax.rem(block, pieces)
        mine = lax.rem(lax.div(block, pieces), 2)
        cols = pl.ds(pl.multiple_of(piece * BLOCK, BLOCK), BLOCK)

        @pl.when(mine == 1)
        def _():
            wide_own[unit, :, :, :, :, cols] = grad

        @pl.when(mine == 0)
        def _():
            @pl.when(unit > 0)
            def _():
                await_bytes(out_buf.at[piece], out_sems.at[piece])
            out_buf[piece] = grad
            send(out_buf.at[piece], part.at[wide_base + unit, :, :, :, :, cols], out_sems.at[piece], part_recv.at[wide_base + unit], partner)
        return carry

    def stage_b(order, chunk, unit):
        await_bytes(part.at[unit], part_recv.at[unit])

        @pl.when(unit < wide_base)
        def _():
            await_bytes(own.at[order], load_sem.at[unit])
            part[unit] = part[unit] + own[order]

        @pl.when(unit >= wide_base)
        def _():
            part[unit] = part[unit] + wide_own[unit - wide_base]
        rings[order][0].start(part, (unit,), unit)

    def stage_c(order, chunk, unit):
        rings[order][0].pass_on(part, (unit,), unit)

    def stage_d(order, chunk, unit):
        final1[unit, 0] = rings[order][0].finish(part, (unit,), unit)
        rings[order][1].start(final1, (unit, 0), unit)

    def stage_e(order, chunk, unit):
        rings[order][1].pass_on(final1, (unit, 0), unit)

    def stage_f(order, chunk, unit):
        final2[unit, 0] = rings[order][1].finish(final1, (unit, 0), unit)
        rings[order][2].start(final2, (unit, 0), unit)

    def stage_g(order, chunk, unit):
        rings[order][2].pass_on(final2, (unit, 0), unit)

    def stage_h(order, chunk, unit):
        shard[unit] = rings[order][2].finish(final2, (unit, 0), unit) * (1.0 / (2 * SIDE ** 3))

    stages = (stage_b, stage_c, stage_d, stage_e, stage_f, stage_g, stage_h)

    def run(now, lag):
        chunk = now - lag - 1
        for order in range(3):
            @pl.when((chunk >= 0) & (chunk < counts[order]))
            def _(order=order):
                stages[lag](order, chunk, 3 * chunk + order)

    def wide_blocks(low, count):
        lax.fori_loop(lax.min(low, blocks), lax.min(low + count, blocks), wide_block, 0)

    load(0)
    for copy in steady:
        copy.wait()
    first_blocks = 2
    wide_blocks(0, first_blocks)

    def turn(now, carry):
        run(now, 0)
        for chunk in range(1, chunks):
            if 3 * chunk < wide_base:
                @pl.when(now == chunk)
                def _(chunk=chunk):
                    load(chunk)
        done = first_blocks + (now - 1) * sum(BLOCKS_AFTER)
        for lag in range(1, len(stages)):
            if lag <= len(BLOCKS_AFTER):
                wide_blocks(done, BLOCKS_AFTER[lag - 1])
                done = done + BLOCKS_AFTER[lag - 1]
            run(now, lag)
        return carry

    lax.fori_loop(1, chunks + len(stages), turn, 0)

    swap_count = UNITS_OF[3] + wide_units
    swapped = shard.at[pl.ds(len(units), swap_count)]
    send(shard.at[pl.ds(first_unit(3), swap_count)], swapped, swap_sems.at[0], swap_sems.at[1], partner)

    def fold(unit, total):
        value = shard[unit]
        return total + value * value

    squares = lax.fori_loop(0, len(units), fold, jnp.zeros((ROWS, WIDTH), jnp.float32))
    total = squares[:, 0:128]
    for col in range(1, WIDTH // 128):
        total = total + squares[:, col * 128:(col + 1) * 128]
    levels = ((norm_a, group_x, place.coords[2] * 2 + place.core), (norm_b, group_y, place.coords[1]), (norm_c, group_z, place.coords[0]))
    for level, (board, group, seat) in enumerate(levels):
        norm_own[level] = total
        board[seat] = total
        for peer in group:
            send(norm_own.at[level], board.at[seat], norm_sems.at[0, level], norm_sems.at[1, level], peer)
        await_bytes(board.at[pl.ds(0, len(group))], norm_sems.at[1, level])
        total = board[0]
        for row in range(1, len(group) + 1):
            total = total + board[row]
    shard[len(units) + swap_count] = jnp.concatenate([total] * (WIDTH // 128), axis=1)

    await_bytes(swapped, swap_sems.at[0])
    await_bytes(swapped, swap_sems.at[1])
    for level, (board, group, seat) in enumerate(levels):
        await_bytes(board.at[pl.ds(0, len(group))], norm_sems.at[0, level])
    for piece in range(pieces):
        await_bytes(out_buf.at[piece], out_sems.at[piece])
    for order in range(3):
        def tidy(chunk, carry, order=order):
            unit = 3 * chunk + order
            for ring in rings[order]:
                ring.drain(unit)

            @pl.when(unit < wide_base)
            def _():
                await_bytes(part.at[unit], part_send.at[unit])
            return carry

        lax.fori_loop(0, counts[order], tidy, 0)


def reduce_grads(wide_parts, g_two, g_three, g_four):
    n = len(unit_list())
    cube = (SIDE, SIDE, SIDE)
    args = tuple(wide_parts) + (
        g_two.reshape(cube + (2, UNITS_OF[2] * ROWS, WIDTH)),
        g_three.reshape(cube + (ROWS, 2 * UNITS_OF[3] * WIDTH)),
        g_four.reshape(cube + (2, UNITS_OF[4] * ROWS, WIDTH)),
    )
    f32, bf16 = jnp.float32, jnp.bfloat16
    dma = pltpu.SemaphoreType.DMA
    dim, rows = wide_parts[0].shape
    model = wide_parts[1].shape[1]
    scratch = [
        pltpu.VMEM((3,) + cube + (ROWS, WIDTH), f32),
        pltpu.VMEM((UNITS_OF[1],) + cube + (ROWS, WIDTH), f32),
        pltpu.VMEM((n,) + cube + (ROWS, WIDTH), f32),
        pltpu.VMEM((n, 2, SIDE, SIDE, ROWS, WIDTH // 2), f32),
        pltpu.VMEM((n, 2, SIDE, SIDE, ROWS, WIDTH), f32),
        pltpu.VMEM((n, 2, SIDE, ROWS, WIDTH // 2), f32),
        pltpu.VMEM((n, 2, SIDE, ROWS, WIDTH), f32),
        pltpu.VMEM((n, 2, ROWS, WIDTH // 2), f32),
        pltpu.VMEM((n, 2, ROWS, WIDTH), f32),
        pltpu.VMEM((3, ROWS, 128), f32),
        pltpu.VMEM((2 * SIDE, ROWS, 128), f32),
        pltpu.VMEM((SIDE, ROWS, 128), f32),
        pltpu.VMEM((SIDE, ROWS, 128), f32),
        pltpu.VMEM((dim, rows), bf16),
        pltpu.VMEM((rows, model), bf16),
        pltpu.VMEM((WIDE_DEEP, rows, BLOCK), bf16),
        pltpu.VMEM((WIDE_DEEP, BLOCK, model), bf16),
        pltpu.VMEM((WIDTH // BLOCK,) + cube + (ROWS, BLOCK), f32),
        dma((n,)), dma((n,)), dma((n,)), dma((3, 3, n)), dma((2,)), dma((2, 3)), dma((3, WIDE_DEEP)), dma((WIDTH // BLOCK,)),
    ]
    any_spec = pl.BlockSpec(memory_space=pl.ANY)
    vmem_spec = pl.BlockSpec(memory_space=pltpu.VMEM)
    return pl.pallas_call(
        reduce_kernel,
        out_shape=jax.ShapeDtypeStruct((n + UNITS_OF[3] + UNITS_OF[1] + 1, ROWS, WIDTH), f32),
        in_specs=[any_spec] * len(args),
        out_specs=vmem_spec,
        scratch_shapes=scratch,
        compiler_params=pltpu.CompilerParams(collective_id=0, has_side_effects=True, vmem_limit_bytes=VMEM_BYTES),
        name='reduce_grads',
    )(*args)


def adam_kernel(lr_ref, clip_ref, shard, *refs):
    masters, moms, variances = refs[0:4], refs[4:8], refs[8:12]
    new_masters, new_moms, new_vars = refs[12:16], refs[16:20], refs[20:24]
    two_rows, four_rows, norm_ref, one_rows, three_rows = refs[24:29]
    spread = {1: one_rows, 3: three_rows}
    units = len(unit_list())
    norm_tile = shard[units + UNITS_OF[3] + UNITS_OF[1]][:, 0:128]
    core = lax.rem(lax.axis_index('dp'), 2)
    grad_norm = jnp.sqrt(jnp.sum(jnp.sum(norm_tile, axis=1, keepdims=True), axis=0, keepdims=True))
    norm_ref[...] = grad_norm
    clip_scale = jnp.minimum(1.0, clip_ref[...] / (grad_norm + NORM_EPS))
    learn_rate = lr_ref[...]

    def update(mat, where, grad):
        scaled = clip_scale * grad
        mom_new = BETA_ONE * moms[mat][where] + (1.0 - BETA_ONE) * scaled
        var_new = BETA_TWO * variances[mat][where] + (1.0 - BETA_TWO) * scaled * scaled
        master_new = masters[mat][where] - learn_rate * (mom_new / BIAS_ONE) / (jnp.sqrt(var_new / BIAS_TWO) + ADAM_EPS)
        new_moms[mat][where] = mom_new
        new_vars[mat][where] = var_new
        new_masters[mat][where] = master_new
        return master_new

    for mat, rows_out in ((2, two_rows), (4, four_rows)):
        for piece in range(UNITS_OF[mat]):
            where = (slice(piece * ROWS, (piece + 1) * ROWS), slice(None))
            rows_out[piece] = update(mat - 1, where, shard[first_unit(mat) + piece]).astype(jnp.bfloat16)
    for mat, base in ((3, 0), (1, UNITS_OF[3])):
        for half in range(2):
            for piece in range(UNITS_OF[mat]):
                col = (half * UNITS_OF[mat] + piece) * WIDTH
                where = (slice(None), slice(col, col + WIDTH))
                block = jnp.where(core == half, shard[first_unit(mat) + piece], shard[units + base + piece])
                spread[mat][where] = update(mat - 1, where, jnp.where(core == 0, block[0:ROWS // 2], block[ROWS // 2:ROWS]))


def adam_update(learn_rate, clip_max, shard, masters, moms, variances):
    state = list(masters) + list(moms) + list(variances)
    f32, bf16 = jnp.float32, jnp.bfloat16
    vmem_spec = pl.BlockSpec(memory_space=pltpu.VMEM)
    out_shape = [jax.ShapeDtypeStruct(part.shape, f32) for part in state]
    out_shape += [
        jax.ShapeDtypeStruct((UNITS_OF[2], ROWS, WIDTH), bf16),
        jax.ShapeDtypeStruct((UNITS_OF[4], ROWS, WIDTH), bf16),
        jax.ShapeDtypeStruct((1, 1), f32),
        jax.ShapeDtypeStruct(masters[0].shape, f32),
        jax.ShapeDtypeStruct(masters[2].shape, f32),
    ]
    args = [learn_rate.reshape(1, 1), clip_max.reshape(1, 1), shard] + state
    return pl.pallas_call(
        adam_kernel,
        out_shape=out_shape,
        in_specs=[vmem_spec] * len(args),
        out_specs=[vmem_spec] * len(out_shape),
        compiler_params=pltpu.CompilerParams(vmem_limit_bytes=ADAM_VMEM),
        name='adam_update',
    )(*args)


class RingSpread:
    def __init__(self, place, axis, known, board, near_sem, far_sem, send_sem):
        self.place, self.axis, self.known, self.board = place, axis, known, board
        self.near_sem, self.far_sem, self.send_sem = near_sem, far_sem, send_sem
        self.up_dev, self.down_dev = place.device({axis: 1}), place.device({axis: SIDE - 1})

    def block(self, unit, by, cols):
        fixed = {dim: self.place.coords[dim] for dim in range(3) if dim not in self.known}
        fixed[self.axis] = self.place.step(self.axis, by)
        return self.board.at[spot((unit,), [0, 1, 2], fixed, cols)]

    def blocks(self, unit, count):
        return self.board.at[(unit,) + (0,) * (2 - len(self.known)) + (pl.ds(0, count),)]

    def start(self, unit):
        s = self
        mine = s.block(unit, 0, ALL)
        send(mine, mine, s.send_sem.at[unit], s.near_sem.at[unit], s.up_dev)
        send(mine, mine, s.send_sem.at[unit], s.near_sem.at[unit], s.down_dev)

    def pass_on(self, unit):
        s = self
        await_bytes(s.blocks(unit, 2), s.near_sem.at[unit])
        from_down, from_up = s.block(unit, SIDE - 1, LEFT), s.block(unit, 1, RIGHT)
        send(from_down, from_down, s.send_sem.at[unit], s.far_sem.at[unit], s.up_dev)
        send(from_up, from_up, s.send_sem.at[unit], s.far_sem.at[unit], s.down_dev)

    def finish(self, unit):
        await_bytes(self.block(unit, 0, ALL), self.far_sem.at[unit])

    def drain(self, unit):
        await_bytes(self.blocks(unit, 3), self.send_sem.at[unit])


def gather_kernel(one_rows, three_rows, two_rows, four_rows, board, other, own_one, own_three, swap_one, swap_three, ring_sems, pair_sems, swap_sems, load_sems):
    place = Place()
    units = unit_list()
    chunks = -(-len(units) // 3)
    counts = [len(range(order, len(units), 3)) for order in range(3)]
    partner = place.device(other_core=True)
    here = tuple(place.coords)
    splits = ((1, one_rows, own_one, swap_one), (3, three_rows, own_three, swap_three))
    loads = []
    for index, (mat, rows, mine, landing) in enumerate(splits):
        span = UNITS_OF[mat] * WIDTH
        loads.append(pltpu.make_async_copy(rows.at[:, pl.ds(pl.multiple_of(place.core * span, WIDTH), span)], mine, load_sems.at[index]))
    for index, (mat, rows) in enumerate(((2, two_rows), (4, four_rows))):
        loads.append(pltpu.make_async_copy(rows, board.at[(pl.ds(first_unit(mat), UNITS_OF[mat]),) + here], load_sems.at[2 + index]))
    for copy in loads:
        copy.start()
    enter(place.neighbours())
    for index, (mat, rows, mine, landing) in enumerate(splits):
        span = UNITS_OF[mat] * WIDTH
        theirs = rows.at[:, pl.ds(pl.multiple_of((1 - place.core) * span, WIDTH), span)]
        send(theirs, landing, swap_sems.at[0, index], swap_sems.at[1, index], partner)
    for copy in loads:
        copy.wait()

    def assemble():
        for index, (mat, rows, mine, landing) in enumerate(splits):
            await_bytes(landing, swap_sems.at[1, index])
            for piece in range(UNITS_OF[mat]):
                cols = slice(piece * WIDTH, (piece + 1) * WIDTH)
                top = jnp.where(place.core == 0, mine[:, cols], landing[:, cols])
                bottom = jnp.where(place.core == 0, landing[:, cols], mine[:, cols])
                board[(first_unit(mat) + piece,) + here] = jnp.concatenate([top, bottom], axis=0).astype(board.dtype)

    rings = []
    for order in range(3):
        axes = (order + 2) % 3, (order + 1) % 3, order
        rings.append([RingSpread(place, axis, axes[:level], board, *[ring_sems.at[level, kind] for kind in range(3)]) for level, axis in enumerate(axes)])

    def begin(order, unit, level):
        if level:
            rings[order][level - 1].finish(unit)
        rings[order][level].start(unit)

    def pass_on(order, unit, level):
        rings[order][level].pass_on(unit)

    def hand_over(order, unit, level):
        rings[order][level].finish(unit)
        send(board.at[unit], other.at[unit], pair_sems.at[0, unit], pair_sems.at[1, unit], partner)

    def tidy(order, unit, level):
        await_bytes(other.at[unit], pair_sems.at[1, unit])
        await_bytes(board.at[unit], pair_sems.at[0, unit])
        for ring in rings[order]:
            ring.drain(unit)

    stages = ((begin, 0), (pass_on, 0), (begin, 1), (pass_on, 1), (begin, 2), (pass_on, 2), (hand_over, 2), (tidy, 2))

    ready = first_unit(3) // 3

    def turn(now, carry):
        @pl.when(now == ready)
        def _():
            assemble()
        for lag, (stage, level) in enumerate(stages):
            chunk = now - lag
            for order in range(3):
                @pl.when((chunk >= 0) & (chunk < counts[order]))
                def _(stage=stage, level=level, chunk=chunk, order=order):
                    stage(order, 3 * chunk + order, level)
        return carry

    lax.fori_loop(0, chunks + len(stages) - 1, turn, 0)
    for index, (mat, rows, mine, landing) in enumerate(splits):
        await_bytes(landing, swap_sems.at[0, index])


def gather_rows(one_rows, three_rows, two_rows, four_rows):
    n = len(unit_list())
    cube = (SIDE, SIDE, SIDE)
    bf16, f32 = jnp.bfloat16, jnp.float32
    dma = pltpu.SemaphoreType.DMA
    vmem_spec = pl.BlockSpec(memory_space=pltpu.VMEM)
    full = jax.ShapeDtypeStruct((n,) + cube + (ROWS, WIDTH), bf16)
    return pl.pallas_call(
        gather_kernel,
        out_shape=(full, full),
        in_specs=[pl.BlockSpec(memory_space=pltpu.HBM)] * 4,
        out_specs=(vmem_spec, vmem_spec),
        scratch_shapes=[
            pltpu.VMEM((ROWS // 2, UNITS_OF[1] * WIDTH), f32),
            pltpu.VMEM((ROWS // 2, UNITS_OF[3] * WIDTH), f32),
            pltpu.VMEM((ROWS // 2, UNITS_OF[1] * WIDTH), f32),
            pltpu.VMEM((ROWS // 2, UNITS_OF[3] * WIDTH), f32),
            dma((3, 3, n)), dma((2, n)), dma((2, 2)), dma((4,)),
        ],
        compiler_params=pltpu.CompilerParams(collective_id=1, has_side_effects=True, vmem_limit_bytes=32 * 1024 * 1024),
        name='gather_rows',
    )(one_rows, three_rows, two_rows, four_rows)


def place_kernel(board, other, w_one, w_two, w_three, w_four, sems):
    core = lax.rem(lax.axis_index('dp'), 2)
    outs = {1: w_one, 2: w_two, 3: w_three, 4: w_four}
    copies = []
    for unit, (mat, piece) in enumerate(unit_list()):
        for index, (source, owner) in enumerate(((board, core), (other, 1 - core))):
            if mat in (1, 3):
                start = owner * (UNITS_OF[mat] * WIDTH) + piece * WIDTH
                target = outs[mat].at[:, :, :, :, pl.ds(pl.multiple_of(start, WIDTH), WIDTH)]
            else:
                target = outs[mat].at[:, :, :, owner, pl.ds(piece * ROWS, ROWS), :]
            copies.append(pltpu.make_async_copy(source.at[unit], target, sems.at[index, unit]))
    for copy in copies:
        copy.start()
    for copy in copies:
        copy.wait()


def place_weights(board, other):
    n = len(unit_list())
    cube = (SIDE, SIDE, SIDE)
    bf16 = jnp.bfloat16
    vmem_spec = pl.BlockSpec(memory_space=pltpu.VMEM)
    any_spec = pl.BlockSpec(memory_space=pl.ANY)
    outs = pl.pallas_call(
        place_kernel,
        out_shape=(
            jax.ShapeDtypeStruct(cube + (ROWS, 2 * UNITS_OF[1] * WIDTH), bf16),
            jax.ShapeDtypeStruct(cube + (2, UNITS_OF[2] * ROWS, WIDTH), bf16),
            jax.ShapeDtypeStruct(cube + (ROWS, 2 * UNITS_OF[3] * WIDTH), bf16),
            jax.ShapeDtypeStruct(cube + (2, UNITS_OF[4] * ROWS, WIDTH), bf16),
        ),
        in_specs=[vmem_spec] * 2,
        out_specs=(any_spec,) * 4,
        scratch_shapes=[pltpu.SemaphoreType.DMA((2, n))],
        compiler_params=pltpu.CompilerParams(vmem_limit_bytes=2 * 1024 * 1024),
        name='place_weights',
    )(board, other)
    rows = SIDE ** 3 * ROWS
    return (
        outs[0].reshape(rows, 2 * UNITS_OF[1] * WIDTH),
        outs[1].reshape(2 * SIDE ** 3 * UNITS_OF[2] * ROWS, WIDTH),
        outs[2].reshape(rows, 2 * UNITS_OF[3] * WIDTH),
        outs[3].reshape(2 * SIDE ** 3 * UNITS_OF[4] * ROWS, WIDTH),
    )


def sync_and_update(grads, masters, moms, variances, learn_rate, clip_max):
    shard = reduce_grads(*grads)
    results = adam_update(learn_rate, clip_max, shard, masters, moms, variances)
    new_masters, new_moms, new_vars = results[0:4], results[4:8], results[8:12]
    two_rows, four_rows, grad_norm, one_rows, three_rows = results[12:17]
    board, other = gather_rows(one_rows, three_rows, two_rows, four_rows)
    new_weights = place_weights(board, other)
    return tuple(new_weights) + tuple(new_masters) + tuple(new_moms) + tuple(new_vars) + (grad_norm.reshape(()),)


def solution(mesh):
    row_spec = P('dp', None)
    rep_spec = P()

    def per_device(x_rows, dy_rows, w_one, w_two, w_three, w_four, master_one, master_two, master_three, master_four, m_one, m_two, m_three, m_four, v_one, v_two, v_three, v_four, learn_rate, clip_max):
        grads = local_grads(x_rows, dy_rows, w_one, w_two, w_three, w_four)
        return sync_and_update(grads, (master_one, master_two, master_three, master_four), (m_one, m_two, m_three, m_four), (v_one, v_two, v_three, v_four), learn_rate, clip_max)

    in_specs = (row_spec, row_spec) + (rep_spec,) * 4 + (row_spec,) * 12 + (rep_spec, rep_spec)
    out_specs = (rep_spec,) * 4 + (row_spec,) * 12 + (rep_spec,)
    return jax.shard_map(per_device, mesh=mesh, in_specs=in_specs, out_specs=out_specs, check_vma=False)
```

```python
import functools

import jax
import jax.numpy as jnp
from jax import lax
from jax.experimental import pallas as pl
from jax.experimental.pallas import tpu as pltpu
from jax.sharding import PartitionSpec as P

ADAM_STEP = 10
BETA_ONE = 0.9
BETA_TWO = 0.95
ADAM_EPS = 1e-8
NORM_EPS = 1e-6
BIAS_ONE = 1.0 - BETA_ONE ** ADAM_STEP
BIAS_TWO = 1.0 - BETA_TWO ** ADAM_STEP
INV_SQRT2 = 0.7071067811865476
INV_SQRT2PI = 0.3989422804014327

WIDTH = 512
SIDE = 4
ROWS = 8
UNITS_OF = {3: 2, 4: 2, 2: 8, 1: 8}
MESH_ID = pl.DeviceIdType.MESH
BY_COLUMNS = (((1,), (1,)), ((), ()))
BY_ROWS = (((0,), (0,)), ((), ()))
VMEM_BYTES = 62 * 1024 * 1024
ADAM_VMEM = 8 * 1024 * 1024
WIDE_DEEP = 4


def unit_list():
    return [(mat, piece) for mat in (4, 2, 3, 1) for piece in range(UNITS_OF[mat])]


def first_unit(mat):
    return unit_list().index((mat, 0))


def gelu_value(pre_act):
    pre_wide = pre_act.astype(jnp.float32)
    return 0.5 * pre_wide * (1.0 + lax.erf(pre_wide * INV_SQRT2))


def gelu_slope(pre_act):
    pre_wide = pre_act.astype(jnp.float32)
    return 0.5 * (1.0 + lax.erf(pre_wide * INV_SQRT2)) + pre_wide * INV_SQRT2PI * jnp.exp(-0.5 * pre_wide * pre_wide)


WIDE_STEPS = 8
NARROW_STEPS = 4
TALL_STEPS = 8
NARROW_FROM = WIDE_STEPS
TALL_FROM = WIDE_STEPS + NARROW_STEPS


def local_kernel(x_ref, dy_ref, w_one, w_two, w_three, w_four, z_out, x_turned, g_three, g_four, g_two, dh_out, total, held, h_turned, a_turned):
    step = pl.program_id(0)
    f32, bf16 = jnp.float32, jnp.bfloat16

    @pl.when(step == 0)
    def _():
        total[...] = jnp.zeros_like(total)
        x_turned[...] = x_ref[...].T

    @pl.when(step < NARROW_FROM)
    def _():
        z_one = jnp.dot(x_ref[...], w_one[...], preferred_element_type=f32).astype(bf16)
        z_out[...] = z_one
        a_one = gelu_value(z_one).astype(bf16)
        a_turned[step] = a_one.T
        total[...] += jnp.dot(a_one, w_two[...], preferred_element_type=f32)

    @pl.when(step == NARROW_FROM - 1)
    def _():
        h_two = total[...].astype(bf16)
        held[...] = h_two
        h_turned[...] = h_two.T
        total[...] = jnp.zeros_like(total)

    @pl.when((step >= NARROW_FROM) & (step < TALL_FROM))
    def _():
        z_three = jnp.dot(held[...], w_three[...], preferred_element_type=f32).astype(bf16)
        a_three = gelu_value(z_three).astype(bf16)
        da_three = lax.dot_general(dy_ref[...], w_four[...], BY_COLUMNS, preferred_element_type=f32).astype(bf16)
        dz_three = (da_three.astype(f32) * gelu_slope(z_three)).astype(bf16)
        g_four[...] = lax.dot_general(a_three, dy_ref[...], BY_ROWS, preferred_element_type=f32)
        g_three[...] = jnp.dot(h_turned[...], dz_three, preferred_element_type=f32)
        total[...] += lax.dot_general(dz_three, w_three[...], BY_COLUMNS, preferred_element_type=f32)

    @pl.when(step == TALL_FROM - 1)
    def _():
        dh_out[...] = total[...].astype(bf16)

    @pl.when(step >= TALL_FROM)
    def _():
        g_two[...] = jnp.dot(a_turned[step - TALL_FROM], dh_out[...], preferred_element_type=f32)


def whole_at(step):
    return 0, 0


def held_step(step, first, count):
    return jnp.clip(step - first, 0, count - 1)


def wide_across(step):
    return 0, held_step(step, 0, WIDE_STEPS)


def wide_down(step):
    return held_step(step, 0, WIDE_STEPS), 0


def narrow_across(step):
    return 0, held_step(step, NARROW_FROM, NARROW_STEPS)


def narrow_down(step):
    return held_step(step, NARROW_FROM, NARROW_STEPS), 0


def tall_down(step):
    return held_step(step, TALL_FROM, TALL_STEPS), 0


def local_grads(x_rows, dy_rows, w_one, w_two, w_three, w_four):
    rows, dim = x_rows.shape
    wide, narrow = w_one.shape[1], w_three.shape[1]
    f32, bf16 = jnp.float32, jnp.bfloat16
    whole = pl.BlockSpec((rows, dim), whole_at)
    slab, thin, tall = wide // WIDE_STEPS, narrow // NARROW_STEPS, wide // TALL_STEPS
    z_one, x_turned, g_three, g_four, g_two, dh_two = pl.pallas_call(
        local_kernel,
        grid=(TALL_FROM + TALL_STEPS,),
        out_shape=(
            jax.ShapeDtypeStruct((rows, wide), bf16),
            jax.ShapeDtypeStruct((dim, rows), bf16),
            jax.ShapeDtypeStruct((dim, narrow), f32),
            jax.ShapeDtypeStruct((narrow, dim), f32),
            jax.ShapeDtypeStruct((wide, dim), f32),
            jax.ShapeDtypeStruct((rows, dim), bf16),
        ),
        in_specs=[
            whole, whole,
            pl.BlockSpec((dim, slab), wide_across), pl.BlockSpec((slab, dim), wide_down),
            pl.BlockSpec((dim, thin), narrow_across), pl.BlockSpec((thin, dim), narrow_down),
        ],
        out_specs=(
            pl.BlockSpec((rows, slab), wide_across),
            pl.BlockSpec((dim, rows), whole_at),
            pl.BlockSpec((dim, thin), narrow_across),
            pl.BlockSpec((thin, dim), narrow_down),
            pl.BlockSpec((tall, dim), tall_down),
            whole,
        ),
        scratch_shapes=[pltpu.VMEM((rows, dim), f32), pltpu.VMEM((rows, dim), bf16), pltpu.VMEM((dim, rows), bf16), pltpu.VMEM((WIDE_STEPS, slab, rows), bf16)],
        compiler_params=pltpu.CompilerParams(vmem_limit_bytes=VMEM_BYTES),
        name='local_grads',
    )(x_rows, dy_rows, w_one, w_two, w_three, w_four)
    return (x_turned, dh_two, z_one, w_two), g_two, g_three, g_four


class Place:
    def __init__(self):
        me = lax.axis_index('dp')
        self.core = lax.rem(me, 2)
        self.coords = [lax.div(me, 2 * SIDE * SIDE), lax.rem(lax.div(me, 2 * SIDE), SIDE), lax.rem(lax.div(me, 2), SIDE)]

    def step(self, axis, by):
        return lax.rem(self.coords[axis] + by, SIDE)

    def device(self, moves=None, other_core=False):
        pos = list(self.coords)
        for axis, by in (moves or {}).items():
            pos[axis] = self.step(axis, by)
        core = 1 - self.core if other_core else self.core
        return (((pos[0] * SIDE + pos[1]) * SIDE + pos[2]) * 2 + core,)

    def neighbours(self):
        found = [self.device(other_core=True)]
        for axis in range(3):
            found += [self.device({axis: 1}), self.device({axis: SIDE - 1})]
        return found


def enter(peers):
    barrier = pltpu.get_barrier_semaphore()
    for peer in peers:
        pl.semaphore_signal(barrier, inc=1, device_id=peer, device_id_type=MESH_ID)
    pl.semaphore_wait(barrier, len(peers))


def send(src, dst, send_sem, recv_sem, peer):
    pltpu.make_async_remote_copy(src_ref=src, dst_ref=dst, send_sem=send_sem, recv_sem=recv_sem, device_id=peer, device_id_type=MESH_ID).start()


def await_bytes(ref, sem):
    pltpu.make_async_copy(ref, ref, sem).wait()


def spot(lead, dims, fixed, cols):
    return tuple(lead) + tuple(fixed.get(axis, slice(None)) for axis in dims) + (slice(None), cols)


LEFT = pl.ds(0, WIDTH // 2)
RIGHT = pl.ds(WIDTH // 2, WIDTH // 2)
ALL = slice(None)


class RingSum:
    def __init__(self, place, dims, axis, relay, final, relay_sem, final_sem, send_sem):
        self.place, self.dims, self.axis = place, dims, axis
        self.relay, self.final = relay, final
        self.relay_sem, self.final_sem, self.send_sem = relay_sem, final_sem, send_sem
        self.own = place.coords[axis]
        self.up, self.down, self.far = place.step(axis, 1), place.step(axis, SIDE - 1), place.step(axis, 2)
        self.up_dev, self.down_dev = place.device({axis: 1}), place.device({axis: SIDE - 1})
        self.rest = [dim for dim in dims if dim != axis]

    def start(self, src, lead, unit):
        s = self
        send(src.at[spot(lead, s.dims, {s.axis: s.far}, LEFT)], s.relay.at[unit, 0], s.send_sem.at[unit], s.relay_sem.at[unit], s.up_dev)
        send(src.at[spot(lead, s.dims, {s.axis: s.far}, RIGHT)], s.relay.at[unit, 1], s.send_sem.at[unit], s.relay_sem.at[unit], s.down_dev)
        send(src.at[spot(lead, s.dims, {s.axis: s.up}, RIGHT)], s.final.at[spot((unit, 0), s.rest, {}, RIGHT)], s.send_sem.at[unit], s.final_sem.at[unit], s.up_dev)
        send(src.at[spot(lead, s.dims, {s.axis: s.down}, LEFT)], s.final.at[spot((unit, 1), s.rest, {}, LEFT)], s.send_sem.at[unit], s.final_sem.at[unit], s.down_dev)

    def pass_on(self, src, lead, unit):
        s = self
        await_bytes(s.relay.at[unit], s.relay_sem.at[unit])
        up_spot = spot(lead, s.dims, {s.axis: s.up}, LEFT)
        src[up_spot] = src[up_spot] + s.relay[unit, 0]
        send(src.at[up_spot], s.final.at[spot((unit, 0), s.rest, {}, LEFT)], s.send_sem.at[unit], s.final_sem.at[unit], s.up_dev)
        down_spot = spot(lead, s.dims, {s.axis: s.down}, RIGHT)
        src[down_spot] = src[down_spot] + s.relay[unit, 1]
        send(src.at[down_spot], s.final.at[spot((unit, 1), s.rest, {}, RIGHT)], s.send_sem.at[unit], s.final_sem.at[unit], s.down_dev)

    def finish(self, src, lead, unit):
        s = self
        await_bytes(s.final.at[unit], s.final_sem.at[unit])
        return src[spot(lead, s.dims, {s.axis: s.own}, ALL)] + s.final[unit, 0] + s.final[unit, 1]

    def drain(self, unit):
        await_bytes(self.relay.at[unit], self.send_sem.at[unit])
        await_bytes(self.final.at[unit], self.send_sem.at[unit])


BLOCK = 256
BLOCKS_PER_UNIT = 2 * (WIDTH // BLOCK)
BLOCKS_AFTER = (2, 2, 1)


def reduce_kernel(x_turned, dh_two, z_one, w_two, g_two, g_three, g_four, shard, own, wide_own, part, relay1, final1, relay2, final2, relay3, final3, norm_own, norm_a, norm_b, norm_c, x_buf, dh_buf, z_buf, w_buf, out_buf, load_sem, part_send, part_recv, ring_sems, swap_sems, norm_sems, fetch_sems, out_sems):
    place = Place()
    units = unit_list()
    chunks = -(-len(units) // 3)
    counts = [len(range(order, len(units), 3)) for order in range(3)]
    wide_base = first_unit(1)
    wide_units = UNITS_OF[1]
    wide_half = wide_units * WIDTH
    pieces = WIDTH // BLOCK
    blocks = wide_units * BLOCKS_PER_UNIT
    partner = place.device(other_core=True)
    group_x = [(place.device({2: by}, other_core=swap)) for by in range(SIDE) for swap in (False, True) if by or swap]
    group_y = [place.device({1: by}) for by in range(1, SIDE)]
    group_z = [place.device({0: by}) for by in range(1, SIDE)]

    def block_start(block):
        unit = lax.div(block, BLOCKS_PER_UNIT)
        mine = lax.rem(lax.div(block, pieces), 2)
        owner = lax.rem(place.core + 1 + mine, 2)
        start = owner * wide_half + unit * WIDTH + lax.rem(block, pieces) * BLOCK
        return pl.multiple_of(start, BLOCK)

    def fetch(block):
        slot = lax.rem(block, WIDE_DEEP)
        start = block_start(block)
        return (
            pltpu.make_async_copy(z_one.at[:, pl.ds(start, BLOCK)], z_buf.at[slot], fetch_sems.at[0, slot]),
            pltpu.make_async_copy(w_two.at[pl.ds(start, BLOCK), :], w_buf.at[slot], fetch_sems.at[1, slot]),
        )

    steady = (pltpu.make_async_copy(x_turned, x_buf, fetch_sems.at[2, 0]), pltpu.make_async_copy(dh_two, dh_buf, fetch_sems.at[2, 1]))
    for copy in steady:
        copy.start()
    for block in range(WIDE_DEEP - 1):
        for copy in fetch(block):
            copy.start()
    enter(group_x + group_y + group_z)

    def source(mat, piece, core):
        if mat == 3:
            start = core * (UNITS_OF[mat] * WIDTH) + piece * WIDTH
            return g_three.at[:, :, :, :, pl.ds(pl.multiple_of(start, WIDTH), WIDTH)]
        ref = g_two if mat == 2 else g_four
        return ref.at[:, :, :, core, pl.ds(piece * ROWS, ROWS), :]

    def sems_of(level):
        return [ring_sems.at[level, kind] for kind in range(3)]

    rings = []
    for order in range(3):
        a, b = order, (order + 1) % 3
        c = (order + 2) % 3
        first = RingSum(place, [0, 1, 2], a, relay1, final1, *sems_of(0))
        second = RingSum(place, first.rest, b, relay2, final2, *sems_of(1))
        third = RingSum(place, second.rest, c, relay3, final3, *sems_of(2))
        rings.append((first, second, third))

    def load(chunk):
        for order in range(3):
            unit = 3 * chunk + order
            if unit >= wide_base:
                continue
            mat, piece = units[unit]
            send(source(mat, piece, 1 - place.core), part.at[unit], part_send.at[unit], part_recv.at[unit], partner)
            pltpu.make_async_copy(source(mat, piece, place.core), own.at[order], load_sem.at[unit]).start()

    def wide_block(block, carry):
        slot = lax.rem(block, WIDE_DEEP)

        @pl.when(block + WIDE_DEEP - 1 < blocks)
        def _():
            for copy in fetch(block + WIDE_DEEP - 1):
                copy.start()

        for copy in fetch(block):
            copy.wait()
        da_one = lax.dot_general(dh_buf[...], w_buf[slot], BY_COLUMNS, preferred_element_type=jnp.float32).astype(jnp.bfloat16)
        dz_one = (da_one.astype(jnp.float32) * gelu_slope(z_buf[slot])).astype(jnp.bfloat16)
        grad = jnp.dot(x_buf[...], dz_one, preferred_element_type=jnp.float32)
        grad = grad.reshape(SIDE, SIDE, SIDE, ROWS, BLOCK)
        unit = lax.div(block, BLOCKS_PER_UNIT)
        piece = lax.rem(block, pieces)
        mine = lax.rem(lax.div(block, pieces), 2)
        cols = pl.ds(pl.multiple_of(piece * BLOCK, BLOCK), BLOCK)

        @pl.when(mine == 1)
        def _():
            wide_own[unit, :, :, :, :, cols] = grad

        @pl.when(mine == 0)
        def _():
            @pl.when(unit > 0)
            def _():
                await_bytes(out_buf.at[piece], out_sems.at[piece])
            out_buf[piece] = grad
            send(out_buf.at[piece], part.at[wide_base + unit, :, :, :, :, cols], out_sems.at[piece], part_recv.at[wide_base + unit], partner)
        return carry

    def stage_b(order, chunk, unit):
        await_bytes(part.at[unit], part_recv.at[unit])

        @pl.when(unit < wide_base)
        def _():
            await_bytes(own.at[order], load_sem.at[unit])
            part[unit] = part[unit] + own[order]

        @pl.when(unit >= wide_base)
        def _():
            part[unit] = part[unit] + wide_own[unit - wide_base]
        rings[order][0].start(part, (unit,), unit)

    def stage_c(order, chunk, unit):
        rings[order][0].pass_on(part, (unit,), unit)

    def stage_d(order, chunk, unit):
        final1[unit, 0] = rings[order][0].finish(part, (unit,), unit)
        rings[order][1].start(final1, (unit, 0), unit)

    def stage_e(order, chunk, unit):
        rings[order][1].pass_on(final1, (unit, 0), unit)

    def stage_f(order, chunk, unit):
        final2[unit, 0] = rings[order][1].finish(final1, (unit, 0), unit)
        rings[order][2].start(final2, (unit, 0), unit)

    def stage_g(order, chunk, unit):
        rings[order][2].pass_on(final2, (unit, 0), unit)

    def stage_h(order, chunk, unit):
        shard[unit] = rings[order][2].finish(final2, (unit, 0), unit) * (1.0 / (2 * SIDE ** 3))

    stages = (stage_b, stage_c, stage_d, stage_e, stage_f, stage_g, stage_h)

    def run(now, lag):
        chunk = now - lag - 1
        for order in range(3):
            @pl.when((chunk >= 0) & (chunk < counts[order]))
            def _(order=order):
                stages[lag](order, chunk, 3 * chunk + order)

    def wide_blocks(low, count):
        lax.fori_loop(lax.min(low, blocks), lax.min(low + count, blocks), wide_block, 0)

    load(0)
    for copy in steady:
        copy.wait()
    first_blocks = 2
    wide_blocks(0, first_blocks)

    def turn(now, carry):
        run(now, 0)
        for chunk in range(1, chunks):
            if 3 * chunk < wide_base:
                @pl.when(now == chunk)
                def _(chunk=chunk):
                    load(chunk)
        done = first_blocks + (now - 1) * sum(BLOCKS_AFTER)
        for lag in range(1, len(stages)):
            if lag <= len(BLOCKS_AFTER):
                wide_blocks(done, BLOCKS_AFTER[lag - 1])
                done = done + BLOCKS_AFTER[lag - 1]
            run(now, lag)
        return carry

    lax.fori_loop(1, chunks + len(stages), turn, 0)

    swap_count = UNITS_OF[3] + wide_units
    swapped = shard.at[pl.ds(len(units), swap_count)]
    send(shard.at[pl.ds(first_unit(3), swap_count)], swapped, swap_sems.at[0], swap_sems.at[1], partner)

    def fold(unit, total):
        value = shard[unit]
        return total + value * value

    squares = lax.fori_loop(0, len(units), fold, jnp.zeros((ROWS, WIDTH), jnp.float32))
    total = squares[:, 0:128]
    for col in range(1, WIDTH // 128):
        total = total + squares[:, col * 128:(col + 1) * 128]
    levels = ((norm_a, group_x, place.coords[2] * 2 + place.core), (norm_b, group_y, place.coords[1]), (norm_c, group_z, place.coords[0]))
    for level, (board, group, seat) in enumerate(levels):
        norm_own[level] = total
        board[seat] = total
        for peer in group:
            send(norm_own.at[level], board.at[seat], norm_sems.at[0, level], norm_sems.at[1, level], peer)
        await_bytes(board.at[pl.ds(0, len(group))], norm_sems.at[1, level])
        total = board[0]
        for row in range(1, len(group) + 1):
            total = total + board[row]
    shard[len(units) + swap_count] = jnp.concatenate([total] * (WIDTH // 128), axis=1)

    await_bytes(swapped, swap_sems.at[0])
    await_bytes(swapped, swap_sems.at[1])
    for level, (board, group, seat) in enumerate(levels):
        await_bytes(board.at[pl.ds(0, len(group))], norm_sems.at[0, level])
    for piece in range(pieces):
        await_bytes(out_buf.at[piece], out_sems.at[piece])
    for order in range(3):
        def tidy(chunk, carry, order=order):
            unit = 3 * chunk + order
            for ring in rings[order]:
                ring.drain(unit)

            @pl.when(unit < wide_base)
            def _():
                await_bytes(part.at[unit], part_send.at[unit])
            return carry

        lax.fori_loop(0, counts[order], tidy, 0)


def reduce_grads(wide_parts, g_two, g_three, g_four):
    n = len(unit_list())
    cube = (SIDE, SIDE, SIDE)
    args = tuple(wide_parts) + (
        g_two.reshape(cube + (2, UNITS_OF[2] * ROWS, WIDTH)),
        g_three.reshape(cube + (ROWS, 2 * UNITS_OF[3] * WIDTH)),
        g_four.reshape(cube + (2, UNITS_OF[4] * ROWS, WIDTH)),
    )
    f32, bf16 = jnp.float32, jnp.bfloat16
    dma = pltpu.SemaphoreType.DMA
    dim, rows = wide_parts[0].shape
    model = wide_parts[1].shape[1]
    scratch = [
        pltpu.VMEM((3,) + cube + (ROWS, WIDTH), f32),
        pltpu.VMEM((UNITS_OF[1],) + cube + (ROWS, WIDTH), f32),
        pltpu.VMEM((n,) + cube + (ROWS, WIDTH), f32),
        pltpu.VMEM((n, 2, SIDE, SIDE, ROWS, WIDTH // 2), f32),
        pltpu.VMEM((n, 2, SIDE, SIDE, ROWS, WIDTH), f32),
        pltpu.VMEM((n, 2, SIDE, ROWS, WIDTH // 2), f32),
        pltpu.VMEM((n, 2, SIDE, ROWS, WIDTH), f32),
        pltpu.VMEM((n, 2, ROWS, WIDTH // 2), f32),
        pltpu.VMEM((n, 2, ROWS, WIDTH), f32),
        pltpu.VMEM((3, ROWS, 128), f32),
        pltpu.VMEM((2 * SIDE, ROWS, 128), f32),
        pltpu.VMEM((SIDE, ROWS, 128), f32),
        pltpu.VMEM((SIDE, ROWS, 128), f32),
        pltpu.VMEM((dim, rows), bf16),
        pltpu.VMEM((rows, model), bf16),
        pltpu.VMEM((WIDE_DEEP, rows, BLOCK), bf16),
        pltpu.VMEM((WIDE_DEEP, BLOCK, model), bf16),
        pltpu.VMEM((WIDTH // BLOCK,) + cube + (ROWS, BLOCK), f32),
        dma((n,)), dma((n,)), dma((n,)), dma((3, 3, n)), dma((2,)), dma((2, 3)), dma((3, WIDE_DEEP)), dma((WIDTH // BLOCK,)),
    ]
    any_spec = pl.BlockSpec(memory_space=pl.ANY)
    vmem_spec = pl.BlockSpec(memory_space=pltpu.VMEM)
    return pl.pallas_call(
        reduce_kernel,
        out_shape=jax.ShapeDtypeStruct((n + UNITS_OF[3] + UNITS_OF[1] + 1, ROWS, WIDTH), f32),
        in_specs=[any_spec] * len(args),
        out_specs=vmem_spec,
        scratch_shapes=scratch,
        compiler_params=pltpu.CompilerParams(collective_id=0, has_side_effects=True, vmem_limit_bytes=VMEM_BYTES),
        name='reduce_grads',
    )(*args)


def adam_kernel(lr_ref, clip_ref, shard, *refs):
    masters, moms, variances = refs[0:4], refs[4:8], refs[8:12]
    new_masters, new_moms, new_vars = refs[12:16], refs[16:20], refs[20:24]
    two_rows, four_rows, norm_ref, one_rows, three_rows = refs[24:29]
    spread = {1: one_rows, 3: three_rows}
    units = len(unit_list())
    norm_tile = shard[units + UNITS_OF[3] + UNITS_OF[1]][:, 0:128]
    core = lax.rem(lax.axis_index('dp'), 2)
    grad_norm = jnp.sqrt(jnp.sum(jnp.sum(norm_tile, axis=1, keepdims=True), axis=0, keepdims=True))
    norm_ref[...] = grad_norm
    clip_scale = jnp.minimum(1.0, clip_ref[...] / (grad_norm + NORM_EPS))
    learn_rate = lr_ref[...]

    def update(mat, where, grad):
        scaled = clip_scale * grad
        mom_new = BETA_ONE * moms[mat][where] + (1.0 - BETA_ONE) * scaled
        var_new = BETA_TWO * variances[mat][where] + (1.0 - BETA_TWO) * scaled * scaled
        master_new = masters[mat][where] - learn_rate * (mom_new / BIAS_ONE) / (jnp.sqrt(var_new / BIAS_TWO) + ADAM_EPS)
        new_moms[mat][where] = mom_new
        new_vars[mat][where] = var_new
        new_masters[mat][where] = master_new
        return master_new

    for mat, rows_out in ((2, two_rows), (4, four_rows)):
        for piece in range(UNITS_OF[mat]):
            where = (slice(piece * ROWS, (piece + 1) * ROWS), slice(None))
            rows_out[piece] = update(mat - 1, where, shard[first_unit(mat) + piece]).astype(jnp.bfloat16)
    for mat, base in ((3, 0), (1, UNITS_OF[3])):
        for half in range(2):
            for piece in range(UNITS_OF[mat]):
                col = (half * UNITS_OF[mat] + piece) * WIDTH
                where = (slice(None), slice(col, col + WIDTH))
                block = jnp.where(core == half, shard[first_unit(mat) + piece], shard[units + base + piece])
                spread[mat][where] = update(mat - 1, where, jnp.where(core == 0, block[0:ROWS // 2], block[ROWS // 2:ROWS]))


def adam_update(learn_rate, clip_max, shard, masters, moms, variances):
    state = list(masters) + list(moms) + list(variances)
    f32, bf16 = jnp.float32, jnp.bfloat16
    vmem_spec = pl.BlockSpec(memory_space=pltpu.VMEM)
    out_shape = [jax.ShapeDtypeStruct(part.shape, f32) for part in state]
    out_shape += [
        jax.ShapeDtypeStruct((UNITS_OF[2], ROWS, WIDTH), bf16),
        jax.ShapeDtypeStruct((UNITS_OF[4], ROWS, WIDTH), bf16),
        jax.ShapeDtypeStruct((1, 1), f32),
        jax.ShapeDtypeStruct(masters[0].shape, f32),
        jax.ShapeDtypeStruct(masters[2].shape, f32),
    ]
    args = [learn_rate.reshape(1, 1), clip_max.reshape(1, 1), shard] + state
    return pl.pallas_call(
        adam_kernel,
        out_shape=out_shape,
        in_specs=[vmem_spec] * len(args),
        out_specs=[vmem_spec] * len(out_shape),
        compiler_params=pltpu.CompilerParams(vmem_limit_bytes=ADAM_VMEM),
        name='adam_update',
    )(*args)


class RingSpread:
    def __init__(self, place, axis, known, board, near_sem, far_sem, send_sem):
        self.place, self.axis, self.known, self.board = place, axis, known, board
        self.near_sem, self.far_sem, self.send_sem = near_sem, far_sem, send_sem
        self.up_dev, self.down_dev = place.device({axis: 1}), place.device({axis: SIDE - 1})

    def block(self, unit, by, cols):
        fixed = {dim: self.place.coords[dim] for dim in range(3) if dim not in self.known}
        fixed[self.axis] = self.place.step(self.axis, by)
        return self.board.at[spot((unit,), [0, 1, 2], fixed, cols)]

    def blocks(self, unit, count):
        return self.board.at[(unit,) + (0,) * (2 - len(self.known)) + (pl.ds(0, count),)]

    def start(self, unit):
        s = self
        mine = s.block(unit, 0, ALL)
        send(mine, mine, s.send_sem.at[unit], s.near_sem.at[unit], s.up_dev)
        send(mine, mine, s.send_sem.at[unit], s.near_sem.at[unit], s.down_dev)

    def pass_on(self, unit):
        s = self
        await_bytes(s.blocks(unit, 2), s.near_sem.at[unit])
        from_down, from_up = s.block(unit, SIDE - 1, LEFT), s.block(unit, 1, RIGHT)
        send(from_down, from_down, s.send_sem.at[unit], s.far_sem.at[unit], s.up_dev)
        send(from_up, from_up, s.send_sem.at[unit], s.far_sem.at[unit], s.down_dev)

    def finish(self, unit):
        await_bytes(self.block(unit, 0, ALL), self.far_sem.at[unit])

    def drain(self, unit):
        await_bytes(self.blocks(unit, 3), self.send_sem.at[unit])


def gather_kernel(one_rows, three_rows, two_rows, four_rows, board, other, own_one, own_three, swap_one, swap_three, ring_sems, pair_sems, swap_sems, load_sems):
    place = Place()
    units = unit_list()
    chunks = -(-len(units) // 3)
    counts = [len(range(order, len(units), 3)) for order in range(3)]
    partner = place.device(other_core=True)
    here = tuple(place.coords)
    splits = ((1, one_rows, own_one, swap_one), (3, three_rows, own_three, swap_three))
    loads = []
    for index, (mat, rows, mine, landing) in enumerate(splits):
        span = UNITS_OF[mat] * WIDTH
        loads.append(pltpu.make_async_copy(rows.at[:, pl.ds(pl.multiple_of(place.core * span, WIDTH), span)], mine, load_sems.at[index]))
    for index, (mat, rows) in enumerate(((2, two_rows), (4, four_rows))):
        loads.append(pltpu.make_async_copy(rows, board.at[(pl.ds(first_unit(mat), UNITS_OF[mat]),) + here], load_sems.at[2 + index]))
    for copy in loads:
        copy.start()
    enter(place.neighbours())
    for index, (mat, rows, mine, landing) in enumerate(splits):
        span = UNITS_OF[mat] * WIDTH
        theirs = rows.at[:, pl.ds(pl.multiple_of((1 - place.core) * span, WIDTH), span)]
        send(theirs, landing, swap_sems.at[0, index], swap_sems.at[1, index], partner)
    for copy in loads:
        copy.wait()

    def assemble():
        for index, (mat, rows, mine, landing) in enumerate(splits):
            await_bytes(landing, swap_sems.at[1, index])
            for piece in range(UNITS_OF[mat]):
                cols = slice(piece * WIDTH, (piece + 1) * WIDTH)
                top = jnp.where(place.core == 0, mine[:, cols], landing[:, cols])
                bottom = jnp.where(place.core == 0, landing[:, cols], mine[:, cols])
                board[(first_unit(mat) + piece,) + here] = jnp.concatenate([top, bottom], axis=0).astype(board.dtype)

    rings = []
    for order in range(3):
        axes = (order + 2) % 3, (order + 1) % 3, order
        rings.append([RingSpread(place, axis, axes[:level], board, *[ring_sems.at[level, kind] for kind in range(3)]) for level, axis in enumerate(axes)])

    def begin(order, unit, level):
        if level:
            rings[order][level - 1].finish(unit)
        rings[order][level].start(unit)

    def pass_on(order, unit, level):
        rings[order][level].pass_on(unit)

    def hand_over(order, unit, level):
        rings[order][level].finish(unit)
        send(board.at[unit], other.at[unit], pair_sems.at[0, unit], pair_sems.at[1, unit], partner)

    def tidy(order, unit, level):
        await_bytes(other.at[unit], pair_sems.at[1, unit])
        await_bytes(board.at[unit], pair_sems.at[0, unit])
        for ring in rings[order]:
            ring.drain(unit)

    stages = ((begin, 0), (pass_on, 0), (begin, 1), (pass_on, 1), (begin, 2), (pass_on, 2), (hand_over, 2), (tidy, 2))

    ready = first_unit(3) // 3

    def turn(now, carry):
        @pl.when(now == ready)
        def _():
            assemble()
        for lag, (stage, level) in enumerate(stages):
            chunk = now - lag
            for order in range(3):
                @pl.when((chunk >= 0) & (chunk < counts[order]))
                def _(stage=stage, level=level, chunk=chunk, order=order):
                    stage(order, 3 * chunk + order, level)
        return carry

    lax.fori_loop(0, chunks + len(stages) - 1, turn, 0)
    for index, (mat, rows, mine, landing) in enumerate(splits):
        await_bytes(landing, swap_sems.at[0, index])


def gather_rows(one_rows, three_rows, two_rows, four_rows):
    n = len(unit_list())
    cube = (SIDE, SIDE, SIDE)
    bf16, f32 = jnp.bfloat16, jnp.float32
    dma = pltpu.SemaphoreType.DMA
    vmem_spec = pl.BlockSpec(memory_space=pltpu.VMEM)
    full = jax.ShapeDtypeStruct((n,) + cube + (ROWS, WIDTH), bf16)
    return pl.pallas_call(
        gather_kernel,
        out_shape=(full, full),
        in_specs=[pl.BlockSpec(memory_space=pltpu.HBM)] * 4,
        out_specs=(vmem_spec, vmem_spec),
        scratch_shapes=[
            pltpu.VMEM((ROWS // 2, UNITS_OF[1] * WIDTH), f32),
            pltpu.VMEM((ROWS // 2, UNITS_OF[3] * WIDTH), f32),
            pltpu.VMEM((ROWS // 2, UNITS_OF[1] * WIDTH), f32),
            pltpu.VMEM((ROWS // 2, UNITS_OF[3] * WIDTH), f32),
            dma((3, 3, n)), dma((2, n)), dma((2, 2)), dma((4,)),
        ],
        compiler_params=pltpu.CompilerParams(collective_id=1, has_side_effects=True, vmem_limit_bytes=32 * 1024 * 1024),
        name='gather_rows',
    )(one_rows, three_rows, two_rows, four_rows)


def place_kernel(board, other, w_one, w_two, w_three, w_four, sems):
    core = lax.rem(lax.axis_index('dp'), 2)
    outs = {1: w_one, 2: w_two, 3: w_three, 4: w_four}
    copies = []
    for unit, (mat, piece) in enumerate(unit_list()):
        for index, (source, owner) in enumerate(((board, core), (other, 1 - core))):
            if mat in (1, 3):
                start = owner * (UNITS_OF[mat] * WIDTH) + piece * WIDTH
                target = outs[mat].at[:, :, :, :, pl.ds(pl.multiple_of(start, WIDTH), WIDTH)]
            else:
                target = outs[mat].at[:, :, :, owner, pl.ds(piece * ROWS, ROWS), :]
            copies.append(pltpu.make_async_copy(source.at[unit], target, sems.at[index, unit]))
    for copy in copies:
        copy.start()
    for copy in copies:
        copy.wait()


def place_weights(board, other):
    n = len(unit_list())
    cube = (SIDE, SIDE, SIDE)
    bf16 = jnp.bfloat16
    vmem_spec = pl.BlockSpec(memory_space=pltpu.VMEM)
    any_spec = pl.BlockSpec(memory_space=pl.ANY)
    outs = pl.pallas_call(
        place_kernel,
        out_shape=(
            jax.ShapeDtypeStruct(cube + (ROWS, 2 * UNITS_OF[1] * WIDTH), bf16),
            jax.ShapeDtypeStruct(cube + (2, UNITS_OF[2] * ROWS, WIDTH), bf16),
            jax.ShapeDtypeStruct(cube + (ROWS, 2 * UNITS_OF[3] * WIDTH), bf16),
            jax.ShapeDtypeStruct(cube + (2, UNITS_OF[4] * ROWS, WIDTH), bf16),
        ),
        in_specs=[vmem_spec] * 2,
        out_specs=(any_spec,) * 4,
        scratch_shapes=[pltpu.SemaphoreType.DMA((2, n))],
        compiler_params=pltpu.CompilerParams(vmem_limit_bytes=2 * 1024 * 1024),
        name='place_weights',
    )(board, other)
    rows = SIDE ** 3 * ROWS
    return (
        outs[0].reshape(rows, 2 * UNITS_OF[1] * WIDTH),
        outs[1].reshape(2 * SIDE ** 3 * UNITS_OF[2] * ROWS, WIDTH),
        outs[2].reshape(rows, 2 * UNITS_OF[3] * WIDTH),
        outs[3].reshape(2 * SIDE ** 3 * UNITS_OF[4] * ROWS, WIDTH),
    )


def sync_and_update(grads, masters, moms, variances, learn_rate, clip_max):
    shard = reduce_grads(*grads)
    results = adam_update(learn_rate, clip_max, shard, masters, moms, variances)
    new_masters, new_moms, new_vars = results[0:4], results[4:8], results[8:12]
    two_rows, four_rows, grad_norm, one_rows, three_rows = results[12:17]
    board, other = gather_rows(one_rows, three_rows, two_rows, four_rows)
    new_weights = place_weights(board, other)
    return tuple(new_weights) + tuple(new_masters) + tuple(new_moms) + tuple(new_vars) + (grad_norm.reshape(()),)


def solution(mesh):
    row_spec = P('dp', None)
    rep_spec = P()

    def per_device(x_rows, dy_rows, w_one, w_two, w_three, w_four, master_one, master_two, master_three, master_four, m_one, m_two, m_three, m_four, v_one, v_two, v_three, v_four, learn_rate, clip_max):
        grads = local_grads(x_rows, dy_rows, w_one, w_two, w_three, w_four)
        return sync_and_update(grads, (master_one, master_two, master_three, master_four), (m_one, m_two, m_three, m_four), (v_one, v_two, v_three, v_four), learn_rate, clip_max)

    in_specs = (row_spec, row_spec) + (rep_spec,) * 4 + (row_spec,) * 12 + (rep_spec, rep_spec)
    out_specs = (rep_spec,) * 4 + (row_spec,) * 12 + (rep_spec,)
    return jax.shard_map(per_device, mesh=mesh, in_specs=in_specs, out_specs=out_specs, check_vma=False)
```

```python
import functools

import jax
import jax.numpy as jnp
from jax import lax
from jax.experimental import pallas as pl
from jax.experimental.pallas import tpu as pltpu
from jax.sharding import PartitionSpec as P

ADAM_STEP = 10
BETA_ONE = 0.9
BETA_TWO = 0.95
ADAM_EPS = 1e-8
NORM_EPS = 1e-6
BIAS_ONE = 1.0 - BETA_ONE ** ADAM_STEP
BIAS_TWO = 1.0 - BETA_TWO ** ADAM_STEP
INV_SQRT2 = 0.7071067811865476
INV_SQRT2PI = 0.3989422804014327

WIDTH = 512
SIDE = 4
ROWS = 8
UNITS_OF = {3: 2, 4: 2, 2: 8, 1: 8}
MESH_ID = pl.DeviceIdType.MESH
BY_COLUMNS = (((1,), (1,)), ((), ()))
BY_ROWS = (((0,), (0,)), ((), ()))
VMEM_BYTES = 62 * 1024 * 1024
ADAM_VMEM = 8 * 1024 * 1024
WIDE_DEEP = 4


def unit_list():
    return [(mat, piece) for mat in (4, 2, 3, 1) for piece in range(UNITS_OF[mat])]


def first_unit(mat):
    return unit_list().index((mat, 0))


def gelu_value(pre_act):
    pre_wide = pre_act.astype(jnp.float32)
    return 0.5 * pre_wide * (1.0 + lax.erf(pre_wide * INV_SQRT2))


def gelu_slope(pre_act):
    pre_wide = pre_act.astype(jnp.float32)
    return 0.5 * (1.0 + lax.erf(pre_wide * INV_SQRT2)) + pre_wide * INV_SQRT2PI * jnp.exp(-0.5 * pre_wide * pre_wide)


WIDE_STEPS = 8
NARROW_STEPS = 4
TALL_STEPS = 8
NARROW_FROM = WIDE_STEPS
TALL_FROM = WIDE_STEPS + NARROW_STEPS


def local_kernel(x_ref, dy_ref, w_one, w_two, w_three, w_four, z_out, x_turned, g_three, g_four, g_two, dh_out, total, held, h_turned, a_turned):
    step = pl.program_id(0)
    f32, bf16 = jnp.float32, jnp.bfloat16

    @pl.when(step == 0)
    def _():
        total[...] = jnp.zeros_like(total)
        x_turned[...] = x_ref[...].T

    @pl.when(step < NARROW_FROM)
    def _():
        z_one = jnp.dot(x_ref[...], w_one[...], preferred_element_type=f32).astype(bf16)
        z_out[...] = z_one
        a_one = gelu_value(z_one).astype(bf16)
        a_turned[step] = a_one.T
        total[...] += jnp.dot(a_one, w_two[...], preferred_element_type=f32)

    @pl.when(step == NARROW_FROM - 1)
    def _():
        h_two = total[...].astype(bf16)
        held[...] = h_two
        h_turned[...] = h_two.T
        total[...] = jnp.zeros_like(total)

    @pl.when((step >= NARROW_FROM) & (step < TALL_FROM))
    def _():
        z_three = jnp.dot(held[...], w_three[...], preferred_element_type=f32).astype(bf16)
        a_three = gelu_value(z_three).astype(bf16)
        da_three = lax.dot_general(dy_ref[...], w_four[...], BY_COLUMNS, preferred_element_type=f32).astype(bf16)
        dz_three = (da_three.astype(f32) * gelu_slope(z_three)).astype(bf16)
        g_four[...] = lax.dot_general(a_three, dy_ref[...], BY_ROWS, preferred_element_type=f32)
        g_three[...] = jnp.dot(h_turned[...], dz_three, preferred_element_type=f32)
        total[...] += lax.dot_general(dz_three, w_three[...], BY_COLUMNS, preferred_element_type=f32)

    @pl.when(step == TALL_FROM - 1)
    def _():
        dh_out[...] = total[...].astype(bf16)

    @pl.when(step >= TALL_FROM)
    def _():
        g_two[...] = jnp.dot(a_turned[step - TALL_FROM], dh_out[...], preferred_element_type=f32)


def whole_at(step):
    return 0, 0


def held_step(step, first, count):
    return jnp.clip(step - first, 0, count - 1)


def wide_across(step):
    return 0, held_step(step, 0, WIDE_STEPS)


def wide_down(step):
    return held_step(step, 0, WIDE_STEPS), 0


def narrow_across(step):
    return 0, held_step(step, NARROW_FROM, NARROW_STEPS)


def narrow_down(step):
    return held_step(step, NARROW_FROM, NARROW_STEPS), 0


def tall_down(step):
    return held_step(step, TALL_FROM, TALL_STEPS), 0


def local_grads(x_rows, dy_rows, w_one, w_two, w_three, w_four):
    rows, dim = x_rows.shape
    wide, narrow = w_one.shape[1], w_three.shape[1]
    f32, bf16 = jnp.float32, jnp.bfloat16
    whole = pl.BlockSpec((rows, dim), whole_at)
    slab, thin, tall = wide // WIDE_STEPS, narrow // NARROW_STEPS, wide // TALL_STEPS
    z_one, x_turned, g_three, g_four, g_two, dh_two = pl.pallas_call(
        local_kernel,
        grid=(TALL_FROM + TALL_STEPS,),
        out_shape=(
            jax.ShapeDtypeStruct((rows, wide), bf16),
            jax.ShapeDtypeStruct((dim, rows), bf16),
            jax.ShapeDtypeStruct((dim, narrow), f32),
            jax.ShapeDtypeStruct((narrow, dim), f32),
            jax.ShapeDtypeStruct((wide, dim), f32),
            jax.ShapeDtypeStruct((rows, dim), bf16),
        ),
        in_specs=[
            whole, whole,
            pl.BlockSpec((dim, slab), wide_across), pl.BlockSpec((slab, dim), wide_down),
            pl.BlockSpec((dim, thin), narrow_across), pl.BlockSpec((thin, dim), narrow_down),
        ],
        out_specs=(
            pl.BlockSpec((rows, slab), wide_across),
            pl.BlockSpec((dim, rows), whole_at),
            pl.BlockSpec((dim, thin), narrow_across),
            pl.BlockSpec((thin, dim), narrow_down),
            pl.BlockSpec((tall, dim), tall_down),
            whole,
        ),
        scratch_shapes=[pltpu.VMEM((rows, dim), f32), pltpu.VMEM((rows, dim), bf16), pltpu.VMEM((dim, rows), bf16), pltpu.VMEM((WIDE_STEPS, slab, rows), bf16)],
        compiler_params=pltpu.CompilerParams(vmem_limit_bytes=VMEM_BYTES),
        name='local_grads',
    )(x_rows, dy_rows, w_one, w_two, w_three, w_four)
    return (x_turned, dh_two, z_one, w_two), g_two, g_three, g_four


class Place:
    def __init__(self):
        me = lax.axis_index('dp')
        self.core = lax.rem(me, 2)
        self.coords = [lax.div(me, 2 * SIDE * SIDE), lax.rem(lax.div(me, 2 * SIDE), SIDE), lax.rem(lax.div(me, 2), SIDE)]

    def step(self, axis, by):
        return lax.rem(self.coords[axis] + by, SIDE)

    def device(self, moves=None, other_core=False):
        pos = list(self.coords)
        for axis, by in (moves or {}).items():
            pos[axis] = self.step(axis, by)
        core = 1 - self.core if other_core else self.core
        return (((pos[0] * SIDE + pos[1]) * SIDE + pos[2]) * 2 + core,)

    def neighbours(self):
        found = [self.device(other_core=True)]
        for axis in range(3):
            found += [self.device({axis: 1}), self.device({axis: SIDE - 1})]
        return found


def enter(peers):
    barrier = pltpu.get_barrier_semaphore()
    for peer in peers:
        pl.semaphore_signal(barrier, inc=1, device_id=peer, device_id_type=MESH_ID)
    pl.semaphore_wait(barrier, len(peers))


def send(src, dst, send_sem, recv_sem, peer):
    pltpu.make_async_remote_copy(src_ref=src, dst_ref=dst, send_sem=send_sem, recv_sem=recv_sem, device_id=peer, device_id_type=MESH_ID).start()


def await_bytes(ref, sem):
    pltpu.make_async_copy(ref, ref, sem).wait()


def spot(lead, dims, fixed, cols):
    return tuple(lead) + tuple(fixed.get(axis, slice(None)) for axis in dims) + (slice(None), cols)


LEFT = pl.ds(0, WIDTH // 2)
RIGHT = pl.ds(WIDTH // 2, WIDTH // 2)
ALL = slice(None)


class RingSum:
    def __init__(self, place, dims, axis, relay, final, relay_sem, final_sem, send_sem):
        self.place, self.dims, self.axis = place, dims, axis
        self.relay, self.final = relay, final
        self.relay_sem, self.final_sem, self.send_sem = relay_sem, final_sem, send_sem
        self.own = place.coords[axis]
        self.up, self.down, self.far = place.step(axis, 1), place.step(axis, SIDE - 1), place.step(axis, 2)
        self.up_dev, self.down_dev = place.device({axis: 1}), place.device({axis: SIDE - 1})
        self.rest = [dim for dim in dims if dim != axis]

    def start(self, src, lead, unit):
        s = self
        send(src.at[spot(lead, s.dims, {s.axis: s.far}, LEFT)], s.relay.at[unit, 0], s.send_sem.at[unit], s.relay_sem.at[unit], s.up_dev)
        send(src.at[spot(lead, s.dims, {s.axis: s.far}, RIGHT)], s.relay.at[unit, 1], s.send_sem.at[unit], s.relay_sem.at[unit], s.down_dev)
        send(src.at[spot(lead, s.dims, {s.axis: s.up}, RIGHT)], s.final.at[spot((unit, 0), s.rest, {}, RIGHT)], s.send_sem.at[unit], s.final_sem.at[unit], s.up_dev)
        send(src.at[spot(lead, s.dims, {s.axis: s.down}, LEFT)], s.final.at[spot((unit, 1), s.rest, {}, LEFT)], s.send_sem.at[unit], s.final_sem.at[unit], s.down_dev)

    def pass_on(self, src, lead, unit):
        s = self
        await_bytes(s.relay.at[unit], s.relay_sem.at[unit])
        up_spot = spot(lead, s.dims, {s.axis: s.up}, LEFT)
        src[up_spot] = src[up_spot] + s.relay[unit, 0]
        send(src.at[up_spot], s.final.at[spot((unit, 0), s.rest, {}, LEFT)], s.send_sem.at[unit], s.final_sem.at[unit], s.up_dev)
        down_spot = spot(lead, s.dims, {s.axis: s.down}, RIGHT)
        src[down_spot] = src[down_spot] + s.relay[unit, 1]
        send(src.at[down_spot], s.final.at[spot((unit, 1), s.rest, {}, RIGHT)], s.send_sem.at[unit], s.final_sem.at[unit], s.down_dev)

    def finish(self, src, lead, unit):
        s = self
        await_bytes(s.final.at[unit], s.final_sem.at[unit])
        return src[spot(lead, s.dims, {s.axis: s.own}, ALL)] + s.final[unit, 0] + s.final[unit, 1]

    def drain(self, unit):
        await_bytes(self.relay.at[unit], self.send_sem.at[unit])
        await_bytes(self.final.at[unit], self.send_sem.at[unit])


BLOCK = 256
BLOCKS_PER_UNIT = 2 * (WIDTH // BLOCK)
BLOCKS_AFTER = (2, 2, 1)


def reduce_kernel(x_turned, dh_two, z_one, w_two, g_two, g_three, g_four, shard, own, wide_own, part, relay1, final1, relay2, final2, relay3, final3, norm_own, norm_a, norm_b, norm_c, x_buf, dh_buf, z_buf, w_buf, out_buf, load_sem, part_send, part_recv, ring_sems, swap_sems, norm_sems, fetch_sems, out_sems):
    place = Place()
    units = unit_list()
    chunks = -(-len(units) // 3)
    counts = [len(range(order, len(units), 3)) for order in range(3)]
    wide_base = first_unit(1)
    wide_units = UNITS_OF[1]
    wide_half = wide_units * WIDTH
    pieces = WIDTH // BLOCK
    blocks = wide_units * BLOCKS_PER_UNIT
    partner = place.device(other_core=True)
    group_x = [(place.device({2: by}, other_core=swap)) for by in range(SIDE) for swap in (False, True) if by or swap]
    group_y = [place.device({1: by}) for by in range(1, SIDE)]
    group_z = [place.device({0: by}) for by in range(1, SIDE)]

    def block_start(block):
        unit = lax.div(block, BLOCKS_PER_UNIT)
        mine = lax.rem(lax.div(block, pieces), 2)
        owner = lax.rem(place.core + 1 + mine, 2)
        start = owner * wide_half + unit * WIDTH + lax.rem(block, pieces) * BLOCK
        return pl.multiple_of(start, BLOCK)

    def fetch(block):
        slot = lax.rem(block, WIDE_DEEP)
        start = block_start(block)
        return (
            pltpu.make_async_copy(z_one.at[:, pl.ds(start, BLOCK)], z_buf.at[slot], fetch_sems.at[0, slot]),
            pltpu.make_async_copy(w_two.at[pl.ds(start, BLOCK), :], w_buf.at[slot], fetch_sems.at[1, slot]),
        )

    steady = (pltpu.make_async_copy(x_turned, x_buf, fetch_sems.at[2, 0]), pltpu.make_async_copy(dh_two, dh_buf, fetch_sems.at[2, 1]))
    for copy in steady:
        copy.start()
    for block in range(WIDE_DEEP - 1):
        for copy in fetch(block):
            copy.start()
    enter(group_x + group_y + group_z)

    def source(mat, piece, core):
        if mat == 3:
            start = core * (UNITS_OF[mat] * WIDTH) + piece * WIDTH
            return g_three.at[:, :, :, :, pl.ds(pl.multiple_of(start, WIDTH), WIDTH)]
        ref = g_two if mat == 2 else g_four
        return ref.at[:, :, :, core, pl.ds(piece * ROWS, ROWS), :]

    def sems_of(level):
        return [ring_sems.at[level, kind] for kind in range(3)]

    rings = []
    for order in range(3):
        a, b = order, (order + 1) % 3
        c = (order + 2) % 3
        first = RingSum(place, [0, 1, 2], a, relay1, final1, *sems_of(0))
        second = RingSum(place, first.rest, b, relay2, final2, *sems_of(1))
        third = RingSum(place, second.rest, c, relay3, final3, *sems_of(2))
        rings.append((first, second, third))

    def load(chunk):
        for order in range(3):
            unit = 3 * chunk + order
            if unit >= wide_base:
                continue
            mat, piece = units[unit]
            send(source(mat, piece, 1 - place.core), part.at[unit], part_send.at[unit], part_recv.at[unit], partner)
            pltpu.make_async_copy(source(mat, piece, place.core), own.at[order], load_sem.at[unit]).start()

    def wide_block(block, carry):
        slot = lax.rem(block, WIDE_DEEP)

        @pl.when(block + WIDE_DEEP - 1 < blocks)
        def _():
            for copy in fetch(block + WIDE_DEEP - 1):
                copy.start()

        for copy in fetch(block):
            copy.wait()
        da_one = lax.dot_general(dh_buf[...], w_buf[slot], BY_COLUMNS, preferred_element_type=jnp.float32).astype(jnp.bfloat16)
        dz_one = (da_one.astype(jnp.float32) * gelu_slope(z_buf[slot])).astype(jnp.bfloat16)
        grad = jnp.dot(x_buf[...], dz_one, preferred_element_type=jnp.float32)
        grad = grad.reshape(SIDE, SIDE, SIDE, ROWS, BLOCK)
        unit = lax.div(block, BLOCKS_PER_UNIT)
        piece = lax.rem(block, pieces)
        mine = lax.rem(lax.div(block, pieces), 2)
        cols = pl.ds(pl.multiple_of(piece * BLOCK, BLOCK), BLOCK)

        @pl.when(mine == 1)
        def _():
            wide_own[unit, :, :, :, :, cols] = grad

        @pl.when(mine == 0)
        def _():
            @pl.when(unit > 0)
            def _():
                await_bytes(out_buf.at[piece], out_sems.at[piece])
            out_buf[piece] = grad
            send(out_buf.at[piece], part.at[wide_base + unit, :, :, :, :, cols], out_sems.at[piece], part_recv.at[wide_base + unit], partner)
        return carry

    def stage_b(order, chunk, unit):
        await_bytes(part.at[unit], part_recv.at[unit])

        @pl.when(unit < wide_base)
        def _():
            await_bytes(own.at[order], load_sem.at[unit])
            part[unit] = part[unit] + own[order]

        @pl.when(unit >= wide_base)
        def _():
            part[unit] = part[unit] + wide_own[unit - wide_base]
        rings[order][0].start(part, (unit,), unit)

    def stage_c(order, chunk, unit):
        rings[order][0].pass_on(part, (unit,), unit)

    def stage_d(order, chunk, unit):
        final1[unit, 0] = rings[order][0].finish(part, (unit,), unit)
        rings[order][1].start(final1, (unit, 0), unit)

    def stage_e(order, chunk, unit):
        rings[order][1].pass_on(final1, (unit, 0), unit)

    def stage_f(order, chunk, unit):
        final2[unit, 0] = rings[order][1].finish(final1, (unit, 0), unit)
        rings[order][2].start(final2, (unit, 0), unit)

    def stage_g(order, chunk, unit):
        rings[order][2].pass_on(final2, (unit, 0), unit)

    def stage_h(order, chunk, unit):
        shard[unit] = rings[order][2].finish(final2, (unit, 0), unit) * (1.0 / (2 * SIDE ** 3))

    stages = (stage_b, stage_c, stage_d, stage_e, stage_f, stage_g, stage_h)

    def run(now, lag):
        chunk = now - lag - 1
        for order in range(3):
            @pl.when((chunk >= 0) & (chunk < counts[order]))
            def _(order=order):
                stages[lag](order, chunk, 3 * chunk + order)

    def wide_blocks(low, count):
        lax.fori_loop(lax.min(low, blocks), lax.min(low + count, blocks), wide_block, 0)

    load(0)
    for copy in steady:
        copy.wait()
    first_blocks = 2
    wide_blocks(0, first_blocks)

    def turn(now, carry):
        run(now, 0)
        for chunk in range(1, chunks):
            if 3 * chunk < wide_base:
                @pl.when(now == chunk)
                def _(chunk=chunk):
                    load(chunk)
        done = first_blocks + (now - 1) * sum(BLOCKS_AFTER)
        for lag in range(1, len(stages)):
            if lag <= len(BLOCKS_AFTER):
                wide_blocks(done, BLOCKS_AFTER[lag - 1])
                done = done + BLOCKS_AFTER[lag - 1]
            run(now, lag)
        return carry

    lax.fori_loop(1, chunks + len(stages), turn, 0)

    swap_count = UNITS_OF[3] + wide_units
    swapped = shard.at[pl.ds(len(units), swap_count)]
    send(shard.at[pl.ds(first_unit(3), swap_count)], swapped, swap_sems.at[0], swap_sems.at[1], partner)

    def fold(unit, total):
        value = shard[unit]
        return total + value * value

    squares = lax.fori_loop(0, len(units), fold, jnp.zeros((ROWS, WIDTH), jnp.float32))
    total = squares[:, 0:128]
    for col in range(1, WIDTH // 128):
        total = total + squares[:, col * 128:(col + 1) * 128]
    levels = ((norm_a, group_x, place.coords[2] * 2 + place.core), (norm_b, group_y, place.coords[1]), (norm_c, group_z, place.coords[0]))
    for level, (board, group, seat) in enumerate(levels):
        norm_own[level] = total
        board[seat] = total
        for peer in group:
            send(norm_own.at[level], board.at[seat], norm_sems.at[0, level], norm_sems.at[1, level], peer)
        await_bytes(board.at[pl.ds(0, len(group))], norm_sems.at[1, level])
        total = board[0]
        for row in range(1, len(group) + 1):
            total = total + board[row]
    shard[len(units) + swap_count] = jnp.concatenate([total] * (WIDTH // 128), axis=1)

    await_bytes(swapped, swap_sems.at[0])
    await_bytes(swapped, swap_sems.at[1])
    for level, (board, group, seat) in enumerate(levels):
        await_bytes(board.at[pl.ds(0, len(group))], norm_sems.at[0, level])
    for piece in range(pieces):
        await_bytes(out_buf.at[piece], out_sems.at[piece])
    for order in range(3):
        def tidy(chunk, carry, order=order):
            unit = 3 * chunk + order
            for ring in rings[order]:
                ring.drain(unit)

            @pl.when(unit < wide_base)
            def _():
                await_bytes(part.at[unit], part_send.at[unit])
            return carry

        lax.fori_loop(0, counts[order], tidy, 0)


def reduce_grads(wide_parts, g_two, g_three, g_four):
    n = len(unit_list())
    cube = (SIDE, SIDE, SIDE)
    args = tuple(wide_parts) + (
        g_two.reshape(cube + (2, UNITS_OF[2] * ROWS, WIDTH)),
        g_three.reshape(cube + (ROWS, 2 * UNITS_OF[3] * WIDTH)),
        g_four.reshape(cube + (2, UNITS_OF[4] * ROWS, WIDTH)),
    )
    f32, bf16 = jnp.float32, jnp.bfloat16
    dma = pltpu.SemaphoreType.DMA
    dim, rows = wide_parts[0].shape
    model = wide_parts[1].shape[1]
    scratch = [
        pltpu.VMEM((3,) + cube + (ROWS, WIDTH), f32),
        pltpu.VMEM((UNITS_OF[1],) + cube + (ROWS, WIDTH), f32),
        pltpu.VMEM((n,) + cube + (ROWS, WIDTH), f32),
        pltpu.VMEM((n, 2, SIDE, SIDE, ROWS, WIDTH // 2), f32),
        pltpu.VMEM((n, 2, SIDE, SIDE, ROWS, WIDTH), f32),
        pltpu.VMEM((n, 2, SIDE, ROWS, WIDTH // 2), f32),
        pltpu.VMEM((n, 2, SIDE, ROWS, WIDTH), f32),
        pltpu.VMEM((n, 2, ROWS, WIDTH // 2), f32),
        pltpu.VMEM((n, 2, ROWS, WIDTH), f32),
        pltpu.VMEM((3, ROWS, 128), f32),
        pltpu.VMEM((2 * SIDE, ROWS, 128), f32),
        pltpu.VMEM((SIDE, ROWS, 128), f32),
        pltpu.VMEM((SIDE, ROWS, 128), f32),
        pltpu.VMEM((dim, rows), bf16),
        pltpu.VMEM((rows, model), bf16),
        pltpu.VMEM((WIDE_DEEP, rows, BLOCK), bf16),
        pltpu.VMEM((WIDE_DEEP, BLOCK, model), bf16),
        pltpu.VMEM((WIDTH // BLOCK,) + cube + (ROWS, BLOCK), f32),
        dma((n,)), dma((n,)), dma((n,)), dma((3, 3, n)), dma((2,)), dma((2, 3)), dma((3, WIDE_DEEP)), dma((WIDTH // BLOCK,)),
    ]
    any_spec = pl.BlockSpec(memory_space=pl.ANY)
    vmem_spec = pl.BlockSpec(memory_space=pltpu.VMEM)
    return pl.pallas_call(
        reduce_kernel,
        out_shape=jax.ShapeDtypeStruct((n + UNITS_OF[3] + UNITS_OF[1] + 1, ROWS, WIDTH), f32),
        in_specs=[any_spec] * len(args),
        out_specs=vmem_spec,
        scratch_shapes=scratch,
        compiler_params=pltpu.CompilerParams(collective_id=0, has_side_effects=True, vmem_limit_bytes=VMEM_BYTES),
        name='reduce_grads',
    )(*args)


def adam_kernel(lr_ref, clip_ref, shard, *refs):
    masters, moms, variances = refs[0:4], refs[4:8], refs[8:12]
    new_masters, new_moms, new_vars = refs[12:16], refs[16:20], refs[20:24]
    two_rows, four_rows, norm_ref, one_rows, three_rows = refs[24:29]
    spread = {1: one_rows, 3: three_rows}
    units = len(unit_list())
    norm_tile = shard[units + UNITS_OF[3] + UNITS_OF[1]][:, 0:128]
    core = lax.rem(lax.axis_index('dp'), 2)
    grad_norm = jnp.sqrt(jnp.sum(jnp.sum(norm_tile, axis=1, keepdims=True), axis=0, keepdims=True))
    norm_ref[...] = grad_norm
    clip_scale = jnp.minimum(1.0, clip_ref[...] / (grad_norm + NORM_EPS))
    learn_rate = lr_ref[...]

    def update(mat, where, grad):
        scaled = clip_scale * grad
        mom_new = BETA_ONE * moms[mat][where] + (1.0 - BETA_ONE) * scaled
        var_new = BETA_TWO * variances[mat][where] + (1.0 - BETA_TWO) * scaled * scaled
        master_new = masters[mat][where] - learn_rate * (mom_new / BIAS_ONE) / (jnp.sqrt(var_new / BIAS_TWO) + ADAM_EPS)
        new_moms[mat][where] = mom_new
        new_vars[mat][where] = var_new
        new_masters[mat][where] = master_new
        return master_new

    for mat, rows_out in ((2, two_rows), (4, four_rows)):
        for piece in range(UNITS_OF[mat]):
            where = (slice(piece * ROWS, (piece + 1) * ROWS), slice(None))
            rows_out[piece] = update(mat - 1, where, shard[first_unit(mat) + piece]).astype(jnp.bfloat16)
    for mat, base in ((3, 0), (1, UNITS_OF[3])):
        for half in range(2):
            for piece in range(UNITS_OF[mat]):
                col = (half * UNITS_OF[mat] + piece) * WIDTH
                where = (slice(None), slice(col, col + WIDTH))
                block = jnp.where(core == half, shard[first_unit(mat) + piece], shard[units + base + piece])
                spread[mat][where] = update(mat - 1, where, jnp.where(core == 0, block[0:ROWS // 2], block[ROWS // 2:ROWS]))


def adam_update(learn_rate, clip_max, shard, masters, moms, variances):
    state = list(masters) + list(moms) + list(variances)
    f32, bf16 = jnp.float32, jnp.bfloat16
    vmem_spec = pl.BlockSpec(memory_space=pltpu.VMEM)
    out_shape = [jax.ShapeDtypeStruct(part.shape, f32) for part in state]
    out_shape += [
        jax.ShapeDtypeStruct((UNITS_OF[2], ROWS, WIDTH), bf16),
        jax.ShapeDtypeStruct((UNITS_OF[4], ROWS, WIDTH), bf16),
        jax.ShapeDtypeStruct((1, 1), f32),
        jax.ShapeDtypeStruct(masters[0].shape, f32),
        jax.ShapeDtypeStruct(masters[2].shape, f32),
    ]
    args = [learn_rate.reshape(1, 1), clip_max.reshape(1, 1), shard] + state
    return pl.pallas_call(
        adam_kernel,
        out_shape=out_shape,
        in_specs=[vmem_spec] * len(args),
        out_specs=[vmem_spec] * len(out_shape),
        compiler_params=pltpu.CompilerParams(vmem_limit_bytes=ADAM_VMEM),
        name='adam_update',
    )(*args)


class RingSpread:
    def __init__(self, place, axis, known, board, near_sem, far_sem, send_sem):
        self.place, self.axis, self.known, self.board = place, axis, known, board
        self.near_sem, self.far_sem, self.send_sem = near_sem, far_sem, send_sem
        self.up_dev, self.down_dev = place.device({axis: 1}), place.device({axis: SIDE - 1})

    def block(self, unit, by, cols):
        fixed = {dim: self.place.coords[dim] for dim in range(3) if dim not in self.known}
        fixed[self.axis] = self.place.step(self.axis, by)
        return self.board.at[spot((unit,), [0, 1, 2], fixed, cols)]

    def blocks(self, unit, count):
        return self.board.at[(unit,) + (0,) * (2 - len(self.known)) + (pl.ds(0, count),)]

    def start(self, unit):
        s = self
        mine = s.block(unit, 0, ALL)
        send(mine, mine, s.send_sem.at[unit], s.near_sem.at[unit], s.up_dev)
        send(mine, mine, s.send_sem.at[unit], s.near_sem.at[unit], s.down_dev)

    def pass_on(self, unit):
        s = self
        await_bytes(s.blocks(unit, 2), s.near_sem.at[unit])
        from_down, from_up = s.block(unit, SIDE - 1, LEFT), s.block(unit, 1, RIGHT)
        send(from_down, from_down, s.send_sem.at[unit], s.far_sem.at[unit], s.up_dev)
        send(from_up, from_up, s.send_sem.at[unit], s.far_sem.at[unit], s.down_dev)

    def finish(self, unit):
        await_bytes(self.block(unit, 0, ALL), self.far_sem.at[unit])

    def drain(self, unit):
        await_bytes(self.blocks(unit, 3), self.send_sem.at[unit])


def gather_kernel(one_rows, three_rows, two_rows, four_rows, board, other, own_one, own_three, swap_one, swap_three, ring_sems, pair_sems, swap_sems, load_sems):
    place = Place()
    units = unit_list()
    chunks = -(-len(units) // 3)
    counts = [len(range(order, len(units), 3)) for order in range(3)]
    partner = place.device(other_core=True)
    here = tuple(place.coords)
    splits = ((1, one_rows, own_one, swap_one), (3, three_rows, own_three, swap_three))
    loads = []
    for index, (mat, rows, mine, landing) in enumerate(splits):
        span = UNITS_OF[mat] * WIDTH
        loads.append(pltpu.make_async_copy(rows.at[:, pl.ds(pl.multiple_of(place.core * span, WIDTH), span)], mine, load_sems.at[index]))
    for index, (mat, rows) in enumerate(((2, two_rows), (4, four_rows))):
        loads.append(pltpu.make_async_copy(rows, board.at[(pl.ds(first_unit(mat), UNITS_OF[mat]),) + here], load_sems.at[2 + index]))
    for copy in loads:
        copy.start()
    enter(place.neighbours())
    for index, (mat, rows, mine, landing) in enumerate(splits):
        span = UNITS_OF[mat] * WIDTH
        theirs = rows.at[:, pl.ds(pl.multiple_of((1 - place.core) * span, WIDTH), span)]
        send(theirs, landing, swap_sems.at[0, index], swap_sems.at[1, index], partner)
    for copy in loads:
        copy.wait()

    def assemble():
        for index, (mat, rows, mine, landing) in enumerate(splits):
            await_bytes(landing, swap_sems.at[1, index])
            for piece in range(UNITS_OF[mat]):
                cols = slice(piece * WIDTH, (piece + 1) * WIDTH)
                top = jnp.where(place.core == 0, mine[:, cols], landing[:, cols])
                bottom = jnp.where(place.core == 0, landing[:, cols], mine[:, cols])
                board[(first_unit(mat) + piece,) + here] = jnp.concatenate([top, bottom], axis=0).astype(board.dtype)

    rings = []
    for order in range(3):
        axes = (order + 2) % 3, (order + 1) % 3, order
        rings.append([RingSpread(place, axis, axes[:level], board, *[ring_sems.at[level, kind] for kind in range(3)]) for level, axis in enumerate(axes)])

    def begin(order, unit, level):
        if level:
            rings[order][level - 1].finish(unit)
        rings[order][level].start(unit)

    def pass_on(order, unit, level):
        rings[order][level].pass_on(unit)

    def hand_over(order, unit, level):
        rings[order][level].finish(unit)
        send(board.at[unit], other.at[unit], pair_sems.at[0, unit], pair_sems.at[1, unit], partner)

    def tidy(order, unit, level):
        await_bytes(other.at[unit], pair_sems.at[1, unit])
        await_bytes(board.at[unit], pair_sems.at[0, unit])
        for ring in rings[order]:
            ring.drain(unit)

    stages = ((begin, 0), (pass_on, 0), (begin, 1), (pass_on, 1), (begin, 2), (pass_on, 2), (hand_over, 2), (tidy, 2))

    early = 4
    ready = -(-(first_unit(3) // 3) // 2)

    def turn(now, carry):
        @pl.when(now == ready)
        def _():
            assemble()
        for lag, (stage, level) in enumerate(stages):
            entered = now - lag
            for chunk in (2 * entered - 1, 2 * entered) if lag < early else (entered,):
                for order in range(3):
                    @pl.when((chunk >= 0) & (chunk < counts[order]))
                    def _(stage=stage, level=level, chunk=chunk, order=order):
                        stage(order, 3 * chunk + order, level)
        return carry

    lax.fori_loop(0, chunks + len(stages) - 1, turn, 0)
    for index, (mat, rows, mine, landing) in enumerate(splits):
        await_bytes(landing, swap_sems.at[0, index])


def gather_rows(one_rows, three_rows, two_rows, four_rows):
    n = len(unit_list())
    cube = (SIDE, SIDE, SIDE)
    bf16, f32 = jnp.bfloat16, jnp.float32
    dma = pltpu.SemaphoreType.DMA
    vmem_spec = pl.BlockSpec(memory_space=pltpu.VMEM)
    full = jax.ShapeDtypeStruct((n,) + cube + (ROWS, WIDTH), bf16)
    return pl.pallas_call(
        gather_kernel,
        out_shape=(full, full),
        in_specs=[pl.BlockSpec(memory_space=pltpu.HBM)] * 4,
        out_specs=(vmem_spec, vmem_spec),
        scratch_shapes=[
            pltpu.VMEM((ROWS // 2, UNITS_OF[1] * WIDTH), f32),
            pltpu.VMEM((ROWS // 2, UNITS_OF[3] * WIDTH), f32),
            pltpu.VMEM((ROWS // 2, UNITS_OF[1] * WIDTH), f32),
            pltpu.VMEM((ROWS // 2, UNITS_OF[3] * WIDTH), f32),
            dma((3, 3, n)), dma((2, n)), dma((2, 2)), dma((4,)),
        ],
        compiler_params=pltpu.CompilerParams(collective_id=1, has_side_effects=True, vmem_limit_bytes=32 * 1024 * 1024),
        name='gather_rows',
    )(one_rows, three_rows, two_rows, four_rows)


def place_kernel(board, other, w_one, w_two, w_three, w_four, sems):
    core = lax.rem(lax.axis_index('dp'), 2)
    outs = {1: w_one, 2: w_two, 3: w_three, 4: w_four}
    copies = []
    for unit, (mat, piece) in enumerate(unit_list()):
        for index, (source, owner) in enumerate(((board, core), (other, 1 - core))):
            if mat in (1, 3):
                start = owner * (UNITS_OF[mat] * WIDTH) + piece * WIDTH
                target = outs[mat].at[:, :, :, :, pl.ds(pl.multiple_of(start, WIDTH), WIDTH)]
            else:
                target = outs[mat].at[:, :, :, owner, pl.ds(piece * ROWS, ROWS), :]
            copies.append(pltpu.make_async_copy(source.at[unit], target, sems.at[index, unit]))
    for copy in copies:
        copy.start()
    for copy in copies:
        copy.wait()


def place_weights(board, other):
    n = len(unit_list())
    cube = (SIDE, SIDE, SIDE)
    bf16 = jnp.bfloat16
    vmem_spec = pl.BlockSpec(memory_space=pltpu.VMEM)
    any_spec = pl.BlockSpec(memory_space=pl.ANY)
    outs = pl.pallas_call(
        place_kernel,
        out_shape=(
            jax.ShapeDtypeStruct(cube + (ROWS, 2 * UNITS_OF[1] * WIDTH), bf16),
            jax.ShapeDtypeStruct(cube + (2, UNITS_OF[2] * ROWS, WIDTH), bf16),
            jax.ShapeDtypeStruct(cube + (ROWS, 2 * UNITS_OF[3] * WIDTH), bf16),
            jax.ShapeDtypeStruct(cube + (2, UNITS_OF[4] * ROWS, WIDTH), bf16),
        ),
        in_specs=[vmem_spec] * 2,
        out_specs=(any_spec,) * 4,
        scratch_shapes=[pltpu.SemaphoreType.DMA((2, n))],
        compiler_params=pltpu.CompilerParams(vmem_limit_bytes=2 * 1024 * 1024),
        name='place_weights',
    )(board, other)
    rows = SIDE ** 3 * ROWS
    return (
        outs[0].reshape(rows, 2 * UNITS_OF[1] * WIDTH),
        outs[1].reshape(2 * SIDE ** 3 * UNITS_OF[2] * ROWS, WIDTH),
        outs[2].reshape(rows, 2 * UNITS_OF[3] * WIDTH),
        outs[3].reshape(2 * SIDE ** 3 * UNITS_OF[4] * ROWS, WIDTH),
    )


def sync_and_update(grads, masters, moms, variances, learn_rate, clip_max):
    shard = reduce_grads(*grads)
    results = adam_update(learn_rate, clip_max, shard, masters, moms, variances)
    new_masters, new_moms, new_vars = results[0:4], results[4:8], results[8:12]
    two_rows, four_rows, grad_norm, one_rows, three_rows = results[12:17]
    board, other = gather_rows(one_rows, three_rows, two_rows, four_rows)
    new_weights = place_weights(board, other)
    return tuple(new_weights) + tuple(new_masters) + tuple(new_moms) + tuple(new_vars) + (grad_norm.reshape(()),)


def solution(mesh):
    row_spec = P('dp', None)
    rep_spec = P()

    def per_device(x_rows, dy_rows, w_one, w_two, w_three, w_four, master_one, master_two, master_three, master_four, m_one, m_two, m_three, m_four, v_one, v_two, v_three, v_four, learn_rate, clip_max):
        grads = local_grads(x_rows, dy_rows, w_one, w_two, w_three, w_four)
        return sync_and_update(grads, (master_one, master_two, master_three, master_four), (m_one, m_two, m_three, m_four), (v_one, v_two, v_three, v_four), learn_rate, clip_max)

    in_specs = (row_spec, row_spec) + (rep_spec,) * 4 + (row_spec,) * 12 + (rep_spec, rep_spec)
    out_specs = (rep_spec,) * 4 + (row_spec,) * 12 + (rep_spec,)
    return jax.shard_map(per_device, mesh=mesh, in_specs=in_specs, out_specs=out_specs, check_vma=False)
```
